128 devices in a mesh: gx: 2 (over core), gy: 4 (over x), gz: 16 (over z, y).
Axes of the slice: x: 4, y: 4, z: 4, core: 2. Of those that a mesh axis runs over, the one named last changes fastest.
Arguments:
- right_side: float32 [96, 192, 768], P('gx', 'gy', 'gz'), may hold values from -6 to 6
- start_guess: float32 [96, 192, 768], P('gx', 'gy', 'gz'), may hold values from -3 to 3
- reaction: float32 [96, 192, 768], P('gx', 'gy', 'gz'), may hold values from 0.0005 to 0.005
Outputs:
- solution_field: float32 [96, 192, 768], P('gx', 'gy', 'gz')
- residual: float32 [96, 192, 768], P('gx', 'gy', 'gz')
The draws below stay inside these ranges and needn't reach their ends.
All inputs are finite; a program needn't handle non-finite values.
Results may differ from the reference program's by a relative error of at most 0.0003.
Values sent between devices are 32-bit elements.
A program may use at most 128 MiB of HBM per device.

```python
import math
import jax
import jax.numpy as jnp

LEVELS = 5
BOTTOM_ITERS = 6
NX = 96
NY = 192
NZ = 768


def block_scale(rng, shape, cuts, low, largest):
    def one(axis_at, parts):
        heights = jax.random.uniform(jax.random.fold_in(jax.random.fold_in(rng, 6), axis_at), (parts,), jnp.float32, low / len(cuts), largest / len(cuts))
        return jnp.repeat(jnp.exp(heights), shape[axis_at] // parts).reshape((-1,) + (1,) * (len(shape) - axis_at - 1))

    gain = one(*cuts[0])
    for cut in cuts[1:]:
        gain = gain * one(*cut)
    return gain


def scatter_about(own_key, extent, scale, bound, shards=(), dtype=jnp.bfloat16):
    values = jax.random.normal(own_key, extent, jnp.float32) * scale
    if len(shards) > 0:
        values = block_scale(own_key, extent, shards, -0.22, 0.18) * values
    return jnp.clip(values, min=-bound, max=bound).astype(dtype)


def setup_inputs(seed: int = 0) -> dict:
    key_list = jax.random.split(jax.random.key(seed), 4)
    right_side = scatter_about(key_list[0], (NX, NY, NZ), 1.0, 6.0, ((0, 2), (1, 4), (2, 16)), jnp.float32)
    start_guess = scatter_about(key_list[1], (NX, NY, NZ), 0.2, 3.0, ((0, 2), (1, 4), (2, 16)), jnp.float32)
    reaction = jnp.clip(jnp.exp(math.log(0.005) - 2.30258502 * jax.random.uniform(key_list[2], (NX, NY, NZ), jnp.float32) ** block_scale(key_list[2], (NX, NY, NZ), ((0, 2), (1, 4), (2, 16)), -0.2, 0.2)), 0.0005, 0.005)
    return {"right_side": right_side, "start_guess": start_guess, "reaction": reaction}


damping = 6.0 / 7.0


def operate(values, shifted, factor):
    padded = jnp.pad(values, 1)
    beside = padded[2:, 1:-1, 1:-1] + padded[:-2, 1:-1, 1:-1]
    beside = beside + padded[1:-1, 2:, 1:-1] + padded[1:-1, :-2, 1:-1]
    beside = beside + padded[1:-1, 1:-1, 2:] + padded[1:-1, 1:-1, :-2]
    return factor * (6.0 * values - beside) + shifted * values


def coarsen(values):
    size_x, size_y, size_z = values.shape
    blocks = values.reshape(size_x // 2, 2, size_y // 2, 2, size_z // 2, 2)
    return jnp.mean(blocks, axis=(1, 3, 5))


def refine(values):
    size_x, size_y, size_z = values.shape
    spread = jnp.broadcast_to(values[:, None, :, None, :, None], (size_x, 2, size_y, 2, size_z, 2))
    return spread.reshape(2 * size_x, 2 * size_y, 2 * size_z)


def smooth_once(estimate, source, shifted, factor):
    return estimate + damping * (source - operate(estimate, shifted, factor)) / (6.0 * factor + shifted)


def bottom(source, shifted, factor):
    estimate = jnp.zeros_like(source)
    leftover = source
    direction = source
    norm_now = jnp.sum(leftover * leftover)
    for repeat_index in range(BOTTOM_ITERS):
        applied = operate(direction, shifted, factor)
        step_length = norm_now / jnp.sum(direction * applied)
        estimate = estimate + step_length * direction
        leftover = leftover - step_length * applied
        norm_next = jnp.sum(leftover * leftover)
        direction = leftover + (norm_next / norm_now) * direction
        norm_now = norm_next
    return estimate


def vcycle_level(source, shifts, depth_index):
    factor = 0.25 ** depth_index
    shifted = shifts[depth_index]
    if depth_index == LEVELS - 1:
        return bottom(source, shifted, factor)
    estimate = damping * source / (6.0 * factor + shifted)
    estimate = smooth_once(estimate, source, shifted, factor)
    leftover = source - operate(estimate, shifted, factor)
    estimate = estimate + refine(vcycle_level(coarsen(leftover), shifts, depth_index + 1))
    estimate = smooth_once(estimate, source, shifted, factor)
    estimate = smooth_once(estimate, source, shifted, factor)
    return estimate


def reference(right_side, start_guess, reaction):
    shifts = [reaction]
    for depth_index in range(LEVELS - 1):
        shifts.append(coarsen(shifts[-1]))
    start_residual = right_side - operate(start_guess, reaction, 1.0)
    precond = vcycle_level(start_residual, shifts, 0)
    upper = jnp.sum(start_residual * precond)
    applied = operate(precond, reaction, 1.0)
    step_length = upper / jnp.sum(precond * applied)
    solution_field = start_guess + step_length * precond
    residual = start_residual - step_length * applied
    return solution_field, residual
```

```python
import jax
import jax.numpy as jnp
from jax import lax
from jax.experimental import pallas as pl
from jax.experimental.pallas import tpu as pltpu
from jax.sharding import PartitionSpec as P

BOTTOM_ITERS = 6
AXES = ("gx", "gy", "gz")
MESH = pl.DeviceIdType.MESH
F32 = jnp.float32
BF16 = jnp.bfloat16
DAMPING = 6.0 / 7.0
KEEP = 1.0 / 7.0
SPLIT = 3
HALO = (4, 5, 5)


def loop(n, f, carry=0, unroll=4):
    while n % unroll:
        unroll -= 1

    def step(i, c):
        for k in range(unroll):
            c = f(i * unroll + k, c)
        return c

    return lax.fori_loop(0, n // unroll, step, carry)


def iota(shape, axis):
    return lax.broadcasted_iota(jnp.int32, shape, axis)


def roll(v, shift, axis=1):
    shift = shift % v.shape[axis] if isinstance(shift, int) else shift
    return v if isinstance(shift, int) and shift == 0 else pltpu.roll(v, shift, axis)


def halves(v):
    high = v.astype(BF16)
    low = (v - high.astype(F32)).astype(BF16)
    return high, low


def picked(v, table):
    high, low = halves(v)
    return jnp.dot(high, table, preferred_element_type=F32) + jnp.dot(low, table, preferred_element_type=F32)


def total(v):
    v = jnp.sum(v, axis=0, keepdims=True)
    return jnp.sum(v, axis=1, keepdims=True)


class Level:
    def __init__(self, k, block):
        self.k = k
        self.n = block >> k
        self.h = HALO[k]
        self.r = 1 << k
        self.q = 0.25**k
        self.tiles = -(-(self.n + 2 * self.h) // 8)
        self.rows = 8 * self.tiles
        self.slabs = self.n + self.h
        self.first = 8 + self.h
        self.shape = (self.slabs + 2, self.rows + 16, 128)


def make_kernel(sizes, block):
    nx, ny, nz = sizes
    B = block[0]
    levels = [Level(k, B) for k in range(SPLIT)]
    n3 = B >> SPLIT
    groups = n3 * n3
    planes = -(-groups * 8 // 128)
    q3, q4 = 0.25**3, 0.25**4
    line = nz
    plane = nx * ny

    scratch = {}
    for name in ("rsr", "sgr", "rer"):
        scratch[name] = pltpu.VMEM((B, B, B), F32)
    scratch["insem"] = pltpu.SemaphoreType.DMA((3,))
    exchanges = {}

    def add_exchange(name, k, field, t, wide):
        lv = levels[k]
        slabs = lv.slabs if wide else lv.n
        per = 128 // (t * lv.r)
        ex = dict(name=name, lv=lv, field=field, t=t, wide=wide, slabs=slabs, per=per,
                  pairs=-(-slabs // 2), groups=-(-slabs // per))
        for d in ("s", "r"):
            scratch[f"y{d}_{name}"] = pltpu.VMEM((2, ex["pairs"], t, 128), F32)
            scratch[f"z{d}_{name}"] = pltpu.VMEM((2, ex["groups"], lv.rows, 128), F32)
        scratch[f"send_{name}"] = pltpu.SemaphoreType.DMA((5,))
        scratch[f"recv_{name}"] = pltpu.SemaphoreType.DMA((5,))
        exchanges[name] = ex

    for lv in levels:
        k = lv.k
        for name in ("f", "s", "w", "e", "a", "b"):
            scratch[f"{name}{k}"] = pltpu.VMEM(lv.shape, F32)
        scratch[f"vm{k}"] = pltpu.VMEM((lv.rows, 128), F32)
        scratch[f"t{k}"] = pltpu.VMEM((lv.n // 2, lv.rows, 128), F32)
        scratch[f"u{k}"] = pltpu.VMEM((lv.slabs // 2 + 1, lv.rows + 16, 128), F32)
        add_exchange(f"f{k}", k, f"f{k}", lv.h, True)
        add_exchange(f"s{k}", k, f"s{k}", lv.h, True)
    scratch["sg"] = pltpu.VMEM(levels[0].shape, F32)
    add_exchange("sg", 0, "sg", 1, False)
    scratch["ap"] = pltpu.VMEM((B, levels[0].rows, 128), F32)
    scratch["own"] = pltpu.VMEM((levels[0].rows, 128), F32)
    for name, count in (("gs", planes), ("gf", planes), ("gr", 2)):
        scratch[f"{name}a"] = pltpu.VMEM((plane, count, 128), F32)
        scratch[f"{name}b"] = pltpu.VMEM((count, line, plane, 128), F32)
        for m, c in (("a", plane), ("b", line)):
            scratch[f"{name}{m}_send"] = pltpu.SemaphoreType.DMA((c,))
            scratch[f"{name}{m}_recv"] = pltpu.SemaphoreType.DMA((c,))
    scratch["l3"] = pltpu.VMEM((n3, 8, 128), F32)
    for name in ("s3", "f3", "w3", "e3"):
        scratch[name] = pltpu.VMEM((planes * 128, 128), F32)
    scratch["x3"] = pltpu.VMEM((planes, plane * line, 128), F32)
    scratch["lhs"] = pltpu.VMEM((3, (n3 + 2) * 16, planes * 128), F32)

    names = list(scratch)

    def kernel(rs_ref, sg_ref, re_ref, sol_ref, res_ref, *refs):
        R = dict(zip(names, refs))
        gx, gy, gz = (lax.axis_index(a) for a in AXES)
        mine = gx * ny + gy

        inputs = [
            pltpu.make_async_copy(src, R[dst], R["insem"].at[i])
            for i, (src, dst) in enumerate(((sg_ref, "sgr"), (re_ref, "rer"), (rs_ref, "rsr")))
        ]
        for copy in inputs:
            copy.start()

        def start_of(lv):
            return 1 + gx * lv.h

        for lv in levels:
            k = lv.k
            z8 = jnp.zeros((8, 128), F32)
            zs = jnp.zeros((lv.rows, 128), F32)
            fields = ["e", "a", "b"] + (["sg"] if k == 0 else [])
            fields = [R[f if f == "sg" else f"{f}{k}"] for f in fields]

            def guard(a, c, fields=fields, lv=lv, z8=z8):
                for ref in fields:
                    ref[a, 0:8, :] = z8
                    ref[a, 8 + lv.rows : 16 + lv.rows, :] = z8
                return c

            loop(lv.shape[0], guard, 0, 2)
            for ref in fields:
                ref[0, 8 : 8 + lv.rows, :] = zs
                ref[lv.slabs + 1, 8 : 8 + lv.rows, :] = zs

            def blank(a, c, k=k, lv=lv):
                for name in ("f", "s"):
                    ref = R[f"{name}{k}"]
                    ref[a, 8:16, :] = jnp.zeros((8, 128), F32)
                    low = (lv.first + lv.n) // 8 * 8
                    ref[a, low : 8 + lv.rows, :] = jnp.zeros((8 + lv.rows - low, 128), F32)
                if k == 0:
                    ref = R["sg"]
                    ref[a, 8:16, :] = jnp.zeros((8, 128), F32)
                    ref[a, low : 8 + lv.rows, :] = jnp.zeros((8 + lv.rows - low, 128), F32)
                return c

            loop(lv.shape[0], blank, 0, 2)
            lane, row = iota((lv.rows, 128), 1), iota((lv.rows, 128), 0)
            wd = lv.h * lv.r
            ok = (lane < B) | ((lane < B + wd) & (gz < nz - 1)) | ((lane >= 128 - wd) & (gz > 0))
            ok = ok & (row >= jnp.where(gy > 0, 0, lv.h))
            ok = ok & (row < lv.n + lv.h + jnp.where(gy < ny - 1, lv.h, 0))
            R[f"vm{k}"][...] = jnp.where(ok, 1.0, 0.0)
            if k == 0:
                own = (lane < B) & (row >= lv.h) & (row < lv.h + lv.n)
                R["own"][...] = jnp.where(own, 1.0, 0.0)
        for name, ex in exchanges.items():
            for m in ("y", "z"):
                ref = R[f"{m}r_{name}"]
                side, at = (gy, ny) if m == "y" else (gz, nz)

                @pl.when((side == 0) | (side == at - 1))
                def _(ref=ref):
                    ref[...] = jnp.zeros(ref.shape, F32)

        barrier = pltpu.get_barrier_semaphore()
        others = []
        for dx in range(nx):
            for dy in range(ny):
                if dx or dy:
                    others.append({"gx": lax.rem(gx + dx, nx), "gy": lax.rem(gy + dy, ny)})
        lines = [{"gz": lax.rem(gz + d, nz)} for d in range(1, nz)]
        for to in others + lines:
            pl.semaphore_signal(barrier, inc=1, device_id=to, device_id_type=MESH)

        def part(name, i):
            ex = exchanges[name]
            lv, t = ex["lv"], ex["t"]
            f = R[ex["field"]]
            src = jnp.where(gx == 0, 1 + lv.n - t, 1 + lv.h)
            dst = jnp.where(gx == 0, 1 + lv.h - t, 1 + lv.n)
            ys, yr, zs, zr = (R[f"{m}_{name}"] for m in ("ys", "yr", "zs", "zr"))
            pairs = (
                (f.at[pl.ds(src, t), 8 : 8 + lv.rows, :], f.at[pl.ds(dst, t), 8 : 8 + lv.rows, :],
                 {"gx": 1 - gx}, None, None),
                (ys.at[0], yr.at[1], {"gy": gy - 1}, gy > 0, gy < ny - 1),
                (ys.at[1], yr.at[0], {"gy": gy + 1}, gy < ny - 1, gy > 0),
                (zs.at[0], zr.at[1], {"gz": gz - 1}, gz > 0, gz < nz - 1),
                (zs.at[1], zr.at[0], {"gz": gz + 1}, gz < nz - 1, gz > 0),
            )
            s, d, to, sends, gets = pairs[i]
            copy = pltpu.make_async_remote_copy(
                src_ref=s, dst_ref=d, send_sem=R[f"send_{name}"].at[i], recv_sem=R[f"recv_{name}"].at[i],
                device_id=to, device_id_type=MESH)
            return copy, sends, gets

        at = {"x": (0,), "y": (1, 2), "z": (3, 4)}

        def doing(cond, f):
            if cond is None:
                f()
            else:
                pl.when(cond)(f)

        def send(name, axis):
            for i in at[axis]:
                copy, sends, _ = part(name, i)
                doing(sends, copy.start)

        def arrive(name, axis):
            for i in at[axis]:
                copy, _, gets = part(name, i)
                doing(gets, copy.wait_recv)

        def sent(name, axis):
            for i in at[axis]:
                copy, sends, _ = part(name, i)
                doing(sends, copy.wait_send)

        def base(ex):
            return 1 if ex["wide"] else start_of(ex["lv"])

        def y_pack(name):
            ex = exchanges[name]
            lv, t, m = ex["lv"], ex["t"], ex["pairs"]
            f, a = R[ex["field"]], base(ex)
            lane = iota((t, 128), 1)
            for side, row in ((0, lv.first), (1, lv.first + lv.n - t)):
                for i in range(m):
                    v = f[a + i, row : row + t, :]
                    if i + m < ex["slabs"]:
                        v = jnp.where(lane < 64, v, roll(f[a + i + m, row : row + t, :], 64))
                    R[f"ys_{name}"][side, i] = v

        def y_unpack(name):
            ex = exchanges[name]
            lv, t, m = ex["lv"], ex["t"], ex["pairs"]
            f, a = R[ex["field"]], base(ex)
            lane = iota((t, 128), 1)
            for side, row in ((0, lv.first - t), (1, lv.first + lv.n)):
                for i in range(m):
                    v = R[f"yr_{name}"][side, i]
                    f[a + i, row : row + t, :] = jnp.where(lane < B, v, 0.0)
                    if i + m < ex["slabs"]:
                        f[a + i + m, row : row + t, :] = jnp.where(lane < B, roll(v, 64), 0.0)

        def z_pack(name):
            ex = exchanges[name]
            lv, per = ex["lv"], ex["per"]
            wd = ex["t"] * lv.r
            f, a = R[ex["field"]], base(ex)
            lane = iota((lv.rows, 128), 1)
            for g in range(ex["groups"]):
                low = high = None
                count = min(per, ex["slabs"] - g * per)
                for j in reversed(range(count)):
                    v = f[a + g * per + j, 8 : 8 + lv.rows, :]
                    c = j * wd
                    one, two = roll(v, c), roll(v, c - (B - wd))
                    low = one if low is None else jnp.where(lane < c + wd, one, low)
                    high = two if high is None else jnp.where(lane < c + wd, two, high)
                R[f"zs_{name}"][0, g] = low
                R[f"zs_{name}"][1, g] = high

        def z_unpacked(name, use):
            ex = exchanges[name]
            lv, per = ex["lv"], ex["per"]
            wd = ex["t"] * lv.r
            f, a = R[ex["field"]], base(ex)
            lane = iota((lv.rows, 128), 1)
            for g in range(ex["groups"]):
                count = min(per, ex["slabs"] - g * per)
                for j in range(count):
                    i = a + g * per + j
                    c = j * wd
                    below = roll(R[f"zr_{name}"][0, g], -wd - c)
                    above = roll(R[f"zr_{name}"][1, g], B - c)
                    v = jnp.where(lane < B + wd, above, jnp.where(lane >= 128 - wd, below, 0.0))
                    use(i, jnp.where(lane < B, f[i, 8 : 8 + lv.rows, :], v))

        def beside_of(lv, ref, a):
            rows = lv.rows
            c = ref[a, 8 : 8 + rows, :]
            v = ref[a + 1, 8 : 8 + rows, :] + ref[a - 1, 8 : 8 + rows, :]
            v = v + (ref[a, 9 : 9 + rows, :] + ref[a, 7 : 7 + rows, :])
            return c, v + (roll(c, lv.r) + roll(c, -lv.r))

        def span(lv, far):
            return lv.n + far, 1 + gx * (lv.h - far)

        def relax(lv, src, dst, far, unroll=2):
            k = lv.k
            count, a0 = span(lv, far)

            def one(i, carry):
                a = a0 + i
                c, v = beside_of(lv, R[f"{src}{k}"], a)
                w = R[f"w{k}"][a, 8 : 8 + lv.rows, :]
                e = R[f"e{k}"][a, 8 : 8 + lv.rows, :]
                R[f"{dst}{k}"][a, 8 : 8 + lv.rows, :] = c * KEEP + (e + w * v)
                return carry

            loop(count, one, 0, unroll)

        def weigh(lv):
            k = lv.k
            vm = R[f"vm{k}"]

            def use(i, s):
                R[f"w{k}"][i, 8 : 8 + lv.rows, :] = vm[...] * ((DAMPING * lv.q) / (6.0 * lv.q + s))

            z_unpacked(f"s{k}", use)

        def begin(lv):
            k = lv.k
            scale = 1.0 / lv.q

            def use(i, f):
                w = R[f"w{k}"][i, 8 : 8 + lv.rows, :]
                R[f"e{k}"][i, 8 : 8 + lv.rows, :] = (w * scale) * f if k else w * f

            z_unpacked(f"f{k}", use)

        def restrict(lv, of, name):
            k = lv.k
            a0 = start_of(lv)
            half = lv.n // 2
            lane = iota((lv.rows, 128), 1)
            t = R[f"t{k}"]

            def one(j, c):
                v = of(a0 + 2 * j) + of(a0 + 2 * j + 1)
                v = v + jnp.where((lane & lv.r) == 0, roll(v, -lv.r), roll(v, lv.r))
                t[j] = v
                return c

            loop(half, one, 0, 2)
            wide = iota((half, 128), 1) < B

            def two(j, c):
                v = t[j, pl.ds(lv.h, half, stride=2), :] + t[j, pl.ds(lv.h + 1, half, stride=2), :]
                v = jnp.where(wide, 0.125 * v, 0.0)
                if k + 1 < SPLIT:
                    nxt = levels[k + 1]
                    R[f"{name}{k + 1}"][start_of(nxt) + j, nxt.first : nxt.first + half, :] = v
                else:
                    R["l3"][j, 0:half, :] = v
                return c

            loop(half, two, 0, 2)

        def left_of(lv, src):
            k = lv.k

            def f(a):
                c, v = beside_of(lv, R[f"{src}{k}"], a)
                s = R[f"s{k}"][a, 8 : 8 + lv.rows, :]
                return R[f"f{k}"][a, 8 : 8 + lv.rows, :] - ((6.0 * lv.q + s) * c - lv.q * v)

            return f

        def coefficient(lv):
            return lambda a: R[f"s{lv.k}"][a, 8 : 8 + lv.rows, :]

        def prolong(lv, coarse_rows):
            k = lv.k
            nxt_far = 2
            half = lv.n // 2
            m = half + 2 * nxt_far
            shift = lv.h - 2 * nxt_far
            u = R[f"u{k}"]

            def put(j, c):
                v = coarse_rows(j, m)
                u[j, pl.ds(shift, m, stride=2), :] = v
                u[j, pl.ds(shift + 1, m, stride=2), :] = v
                return c

            loop(half + nxt_far, put, 0, 2)

        def add_up(lv):
            k = lv.k
            a0 = 1 + gx * (lv.h - 4)

            def one(j, c):
                p = R[f"u{k}"][j, 0 : lv.rows, :]
                if k:
                    row = iota((lv.rows, 128), 0)
                    p = jnp.where((row >= lv.h - 4) & (row < lv.h + lv.n + 4), p, 0.0)
                if k == SPLIT - 1:
                    p = jnp.where(R[f"vm{k}"][...] > 0.0, p, 0.0)
                for d in range(2):
                    a = a0 + 2 * j + d
                    R[f"b{k}"][a, 8 : 8 + lv.rows, :] = R[f"a{k}"][a, 8 : 8 + lv.rows, :] + p
                return c

            loop((lv.n + 4) // 2, one, 0, 2)

        def gather_a(name):
            a = R[f"{name}a"]
            out = []
            for d, to in enumerate(others):
                out.append(pltpu.make_async_remote_copy(
                    src_ref=a.at[mine], dst_ref=a.at[mine], send_sem=R[f"{name}a_send"].at[d],
                    recv_sem=R[f"{name}a_recv"].at[d], device_id=to, device_id_type=MESH))
            return out

        def gather_b(name):
            b = R[f"{name}b"]
            out = []
            for d, to in enumerate(lines):
                out.append(pltpu.make_async_remote_copy(
                    src_ref=b.at[:, gz], dst_ref=b.at[:, gz], send_sem=R[f"{name}b_send"].at[d],
                    recv_sem=R[f"{name}b_recv"].at[d], device_id=to, device_id_type=MESH))
            return out

        def gather_start(name, rows):
            for p, v in enumerate(rows):
                R[f"{name}a"][mine, p : p + 1, :] = v
            for copy in gather_a(name):
                copy.start()

        def gather_middle(name, count):
            for copy in gather_a(name):
                copy.wait_recv()
            for p in range(count):
                for j in range(plane):
                    R[f"{name}b"][p, gz, j : j + 1, :] = R[f"{name}a"][j, p : p + 1, :]
            for copy in gather_b(name):
                copy.start()

        def gather_end(name):
            for copy in gather_b(name):
                copy.wait_recv()

        def gather_sent(name):
            for copy in gather_a(name) + gather_b(name):
                copy.wait_send()

        def local_vector():
            wide = planes * 128
            v = R["l3"][...].reshape(n3 * 8, 128)
            l, c = iota((128, wide), 0), iota((128, wide), 1)
            table = jnp.where((l == (c & 7) * (1 << SPLIT)) & ((c & 7) < n3) & (c < groups * 8), 1.0, 0.0).astype(BF16)
            v = picked(v, table)
            row, c = iota((n3 * 8, wide), 0), iota((n3 * 8, wide), 1)
            keep = ((row & 7) < n3) & ((c >> 3) == (row >> 3) * n3 + (row & 7))
            v = jnp.sum(jnp.where(keep, v, 0.0), axis=0, keepdims=True)
            return [v[:, 128 * p : 128 * p + 128] for p in range(planes)]

        def by_device(name, dst):
            for p in range(planes):
                v = R[f"{name}b"][p].reshape(plane * line, 128)
                R[dst][128 * p : 128 * p + 128, :] = v.T

        lv0, lv1, lv2 = levels
        inside = jnp.zeros((B, 128 - B), F32)

        def take(raw, dst):
            def one(x, c):
                v = jnp.concatenate([R[raw][x], inside], axis=1)
                R[dst][start_of(lv0) + x, lv0.first : lv0.first + B, :] = v
                return c

            loop(B, one, 0, 4)

        R["l3"][...] = jnp.zeros((n3, 8, 128), F32)
        inputs[0].wait()
        take("sgr", "sg")
        y_pack("sg")
        z_pack("sg")
        pl.semaphore_wait(barrier, len(others) + len(lines))
        for axis in "xyz":
            send("sg", axis)
        inputs[1].wait()
        take("rer", "s0")
        send("s0", "x")
        inputs[2].wait()
        take("rsr", "f0")
        restrict(lv0, coefficient(lv0), "s")
        send("s1", "x")
        restrict(lv1, coefficient(lv1), "s")
        send("s2", "x")
        restrict(lv2, coefficient(lv2), "s")
        gather_start("gs", local_vector())
        arrive("s0", "x")
        y_pack("s0")
        send("s0", "y")

        for axis in "xyz":
            arrive("sg", axis)
        sent("sg", "x")
        y_unpack("sg")

        def keep_guess(i, v):
            R["sg"][i, 8 : 8 + lv0.rows, :] = v

        z_unpacked("sg", keep_guess)

        def first_residual(x, carry):
            a = start_of(lv0) + x
            c, v = beside_of(lv0, R["sg"], a)
            s = R["s0"][a, 8 : 8 + lv0.rows, :]
            f = R["f0"][a, 8 : 8 + lv0.rows, :] - ((6.0 + s) * c - v)
            R["f0"][a, 8 : 8 + lv0.rows, :] = jnp.where(R["own"][...] > 0.0, f, 0.0)
            return carry

        loop(B, first_residual, 0, 2)
        send("f0", "x")
        for k in (1, 2):
            arrive(f"s{k}", "x")
            y_pack(f"s{k}")
            send(f"s{k}", "y")
        arrive("s0", "y")
        sent("s0", "x")
        y_unpack("s0")
        z_pack("s0")
        arrive("f0", "x")
        y_pack("f0")
        send("f0", "y")
        send("s0", "z")
        gather_middle("gs", planes)
        arrive("f0", "y")
        sent("f0", "x")
        y_unpack("f0")
        z_pack("f0")
        send("f0", "z")
        for k in (1, 2):
            arrive(f"s{k}", "y")
            sent(f"s{k}", "x")
            y_unpack(f"s{k}")
            z_pack(f"s{k}")
            send(f"s{k}", "z")
        arrive("s0", "z")
        weigh(lv0)
        arrive("f0", "z")

        begin(lv0)

        def first_relax(lv):
            k = lv.k
            count, a0 = span(lv, 4)

            def one(i, carry):
                a = a0 + i
                c, v = beside_of(lv, R[f"e{k}"], a)
                w = R[f"w{k}"][a, 8 : 8 + lv.rows, :]
                R[f"a{k}"][a, 8 : 8 + lv.rows, :] = c * (1.0 + KEEP) + w * v
                return carry

            loop(count, one, 0, 2)

        first_relax(lv0)
        restrict(lv0, left_of(lv0, "a"), "f")

        def deeper(lv, fill):
            k = lv.k
            name = f"f{k}"
            send(name, "x")
            fill()
            arrive(name, "x")
            y_pack(name)
            send(name, "y")
            arrive(name, "y")
            sent(name, "x")
            y_unpack(name)
            z_pack(name)
            send(name, "z")
            arrive(f"s{k}", "z")
            weigh(lv)
            arrive(name, "z")
            begin(lv)
            first_relax(lv)
            restrict(lv, left_of(lv, "a"), "f")

        deeper(lv1, lambda: None)
        deeper(lv2, lambda: None)
        gather_start("gf", local_vector())

        gather_end("gs")
        by_device("gs", "s3")
        lane8, row8 = iota((8, 128), 1), iota((8, 128), 0)
        dev_y, dev_x, dev_z = lane8 & (ny - 1), (lane8 >> 2) & 1, lane8 >> 3
        step_x, step_z = ny, plane
        has = {
            ("y", 1): dev_y < ny - 1, ("y", -1): dev_y > 0, ("x", 1): dev_x < nx - 1, ("x", -1): dev_x > 0,
            ("z", 1): dev_z < nz - 1, ("z", -1): dev_z > 0,
        }
        strides = {"y": 1, "x": step_x, "z": step_z}

        def across(v, axis, way):
            return jnp.where(has[axis, way], roll(v, -way * strides[axis]), 0.0)

        def around(get, m):
            def one(x, y):
                c = get(x, y)
                r = n3 // m
                up = jnp.where(row8 >= n3 - r, roll(across(c, "z", 1), n3 - r, 0), roll(c, -r, 0))
                dn = jnp.where(row8 < r, roll(across(c, "z", -1), r - n3, 0), roll(c, r, 0))
                v = up + dn
                v = v + (get(x + 1, y) if x + 1 < m else across(get(0, y), "x", 1))
                v = v + (get(x - 1, y) if x else across(get(m - 1, y), "x", -1))
                v = v + (get(x, y + 1) if y + 1 < m else across(get(x, 0), "y", 1))
                v = v + (get(x, y - 1) if y else across(get(x, m - 1), "y", -1))
                return c, v

            return one

        cells = [(x, y) for x in range(n3) for y in range(n3)]
        m4 = n3 // 2
        cells4 = [(x, y) for x in range(m4) for y in range(m4)]
        live = row8 < n3

        def tile(name, x, y):
            g = x * n3 + y
            return R[name][8 * g : 8 * g + 8, :]

        for x, y in cells:
            R["w3"][8 * (x * n3 + y) : 8 * (x * n3 + y) + 8, :] = jnp.where(
                live, (DAMPING * q3) / (6.0 * q3 + tile("s3", x, y)), 0.0)

        def coarser(get):
            out = {}
            for x, y in cells4:
                v = (get(2 * x, 2 * y) + get(2 * x, 2 * y + 1)) + (get(2 * x + 1, 2 * y) + get(2 * x + 1, 2 * y + 1))
                v = v + jnp.where((row8 & 1) == 0, roll(v, -1, 0), roll(v, 1, 0))
                out[x, y] = jnp.where(live, 0.125 * v, 0.0)
            return out

        s4 = coarser(lambda x, y: tile("s3", x, y))
        gather_middle("gf", planes)
        gather_end("gf")
        by_device("gf", "f3")
        e = {}
        e0 = {}
        for c in cells:
            e0[c] = (tile("w3", *c) * (1.0 / q3)) * tile("f3", *c)
        op = around(lambda x, y: e0[x, y], n3)
        for c in cells:
            u, v = op(*c)
            e[c] = u * (1.0 + KEEP) + tile("w3", *c) * v
        op = around(lambda x, y: e[x, y], n3)
        rest = {}
        for c in cells:
            u, v = op(*c)
            rest[c] = jnp.where(live, tile("f3", *c) - ((6.0 * q3 + tile("s3", *c)) * u - q3 * v), 0.0)
        f4 = coarser(lambda x, y: rest[x, y])

        def inner(u, v):
            s = None
            for c in cells4:
                s = u[c] * v[c] if s is None else s + u[c] * v[c]
            return total(s)

        r4 = dict(f4)
        p4 = dict(f4)
        e4 = {c: jnp.zeros((8, 128), F32) for c in cells4}
        rr = inner(r4, r4)
        for _ in range(BOTTOM_ITERS):
            op = around(lambda x, y: p4[x, y], m4)
            q = {}
            for c in cells4:
                u, v = op(*c)
                q[c] = jnp.where(live, (6.0 * q4 + s4[c]) * u - q4 * v, 0.0)
            a = rr / inner(p4, q)
            e4 = {c: e4[c] + a * p4[c] for c in cells4}
            r4 = {c: r4[c] - a * q[c] for c in cells4}
            new = inner(r4, r4)
            ratio = new / rr
            p4 = {c: r4[c] + ratio * p4[c] for c in cells4}
            rr = new
        e = {(x, y): e[x, y] + e4[x // 2, y // 2] for x, y in cells}
        for _ in range(2):
            op = around(lambda x, y: e[x, y], n3)
            nxt = {}
            for c in cells:
                u, v = op(*c)
                nxt[c] = u * KEEP + (e0[c] + tile("w3", *c) * v)
            e = nxt
        for x, y in cells:
            g = x * n3 + y
            R["e3"][8 * g : 8 * g + 8, :] = e[x, y]
        R["e3"][groups * 8 :, :] = jnp.zeros((planes * 128 - groups * 8, 128), F32)
        for p in range(planes):
            R["x3"][p] = R["e3"][128 * p : 128 * p + 128, :].T

        wide = planes * 128
        slabs3 = n3 + 2
        lane_w = iota((8, wide), 1) >> 3
        row_w = iota((8, wide), 0)
        lo_rows = jnp.where(row_w < 2, n3 - 2 + row_w, -1000)
        mid_rows = jnp.where(row_w < 2, -1000, row_w - 2)
        hi_rows = jnp.where(row_w < 2, row_w, -1000)
        y_below, y_above = jnp.maximum(gy - 1, 0), jnp.minimum(gy + 1, ny - 1)
        z_at = [jnp.maximum(gz - 1, 0), gz, jnp.minimum(gz + 1, nz - 1)]

        def vector(dev):
            return jnp.concatenate([R["x3"][p, pl.ds(dev, 1), :] for p in range(planes)], axis=1)

        for i in range(slabs3):
            partner = jnp.where(gx == 0, i >= n3, i < 2)
            px = jnp.where(partner, 1 - gx, gx)
            xx = jnp.where(gx == 0, i - jnp.where(i >= n3, n3, 0), i - 2 + jnp.where(i < 2, n3, 0))
            lo, mid, hi = (lane_w == xx * n3 + rows for rows in (lo_rows, mid_rows, hi_rows))
            for d in range(3):
                at_y = lambda g: vector(z_at[d] * plane + px * ny + g)
                first = jnp.where(mid, at_y(gy), jnp.where(lo, at_y(y_below), 0.0))
                second = jnp.where(hi, at_y(y_above), 0.0)
                R["lhs"][d, 16 * i : 16 * i + 8, :] = first
                R["lhs"][d, 16 * i + 8 : 16 * i + 16, :] = second
        l, c = iota((wide, 128), 1), iota((wide, 128), 0)
        table = jnp.where((l < B) & ((c & 7) == (l >> SPLIT)) & (c < groups * 8), 1.0, 0.0).astype(BF16)
        v = picked(R["lhs"][...].reshape(3 * slabs3 * 16, wide), table).reshape(3, slabs3, 16, 128)
        v = v[1] + roll(v[2].reshape(slabs3 * 16, 128), B).reshape(slabs3, 16, 128) + roll(
            v[0].reshape(slabs3 * 16, 128), -B).reshape(slabs3, 16, 128)
        u = R["u2"]
        shift = lv2.h - 4
        for i in range(slabs3):
            m = n3 + 4
            u[i, pl.ds(shift, m, stride=2), :] = v[i, 0:m]
            u[i, pl.ds(shift + 1, m, stride=2), :] = v[i, 0:m]

        add_up(lv2)
        relax(lv2, "b", "a", 4)
        relax(lv2, "a", "b", 2)

        def coarse_of(nxt, ref):
            a0 = 1 + gx * (nxt.h - 2)
            return lambda j, m: R[ref][a0 + j, nxt.first - 2 : nxt.first - 2 + m, :]

        prolong(lv1, coarse_of(lv2, "b2"))
        add_up(lv1)
        relax(lv1, "b", "a", 4)
        relax(lv1, "a", "b", 2)
        prolong(lv0, coarse_of(lv1, "b1"))
        add_up(lv0)
        relax(lv0, "b", "a", 4)
        relax(lv0, "a", "b", 2)

        def image(x, sums):
            upper, lower = sums
            a = start_of(lv0) + x
            c, v = beside_of(lv0, R["b0"], a)
            s = R["s0"][a, 8 : 8 + lv0.rows, :]
            ap = (6.0 + s) * c - v
            R["ap"][x] = ap
            c = jnp.where(R["own"][...] > 0.0, c, 0.0)
            return upper + R["f0"][a, 8 : 8 + lv0.rows, :] * c, lower + ap * c

        zero = jnp.zeros((lv0.rows, 128), F32)
        upper, lower = loop(B, image, (zero, zero), 2)
        gather_start("gr", [jnp.sum(v, axis=0, keepdims=True) for v in (upper, lower)])
        gather_middle("gr", 2)
        gather_end("gr")
        sums = [total(jnp.sum(R["grb"][p], axis=0)) for p in range(2)]
        step_length = sums[0] / sums[1]

        def finish(x, c):
            a = start_of(lv0) + x
            p = R["b0"][a, lv0.first : lv0.first + B, :]
            f = R["f0"][a, lv0.first : lv0.first + B, :]
            q = R["ap"][x, lv0.h : lv0.h + B, :]
            sol_ref[x] = R["sgr"][x] + (step_length * p)[:, 0:B]
            res_ref[x] = (f - step_length * q)[:, 0:B]
            return c

        loop(B, finish, 0, 2)
        for name in exchanges:
            for axis in "yz":
                sent(name, axis)
        for name in ("gs", "gf", "gr"):
            gather_sent(name)

    return kernel, list(scratch.values())


def solution(mesh):
    sizes = tuple(mesh.shape[a] for a in AXES)

    def body(right_side, start_guess, reaction):
        kernel, scratch = make_kernel(sizes, right_side.shape)
        out = jax.ShapeDtypeStruct(right_side.shape, F32)
        return tuple(
            pl.pallas_call(
                kernel,
                out_shape=(out, out),
                in_specs=[pl.BlockSpec(memory_space=pl.ANY)] * 3,
                out_specs=(pl.BlockSpec(memory_space=pltpu.VMEM),) * 2,
                scratch_shapes=scratch,
                compiler_params=pltpu.CompilerParams(
                    collective_id=0, has_side_effects=True, vmem_limit_bytes=60 * 2**20
                ),
                name="cg_step",
            )(right_side, start_guess, reaction)
        )

    placed = P(*AXES)
    return jax.shard_map(
        body, mesh=mesh, in_specs=(placed,) * 3, out_specs=(placed,) * 2, check_vma=False
    )
```

```python
import jax
import jax.numpy as jnp
from jax import lax
from jax.experimental import pallas as pl
from jax.experimental.pallas import tpu as pltpu
from jax.sharding import PartitionSpec as P

BOTTOM_ITERS = 6
AXES = ("gx", "gy", "gz")
MESH = pl.DeviceIdType.MESH
F32 = jnp.float32
BF16 = jnp.bfloat16
DAMPING = 6.0 / 7.0
KEEP = 1.0 / 7.0
SPLIT = 3
HALO = (4, 5, 5)


def loop(n, f, carry=0, unroll=4):
    unroll = min(unroll, n)
    while n % unroll:
        unroll -= 1

    def step(i, c):
        for k in range(unroll):
            c = f(i * unroll + k, c)
        return c

    return lax.fori_loop(0, n // unroll, step, carry)


def iota(shape, axis):
    return lax.broadcasted_iota(jnp.int32, shape, axis)


def roll(v, shift, axis=1):
    shift = shift % v.shape[axis] if isinstance(shift, int) else shift
    return v if isinstance(shift, int) and shift == 0 else pltpu.roll(v, shift, axis)


def halves(v):
    high = v.astype(BF16)
    low = (v - high.astype(F32)).astype(BF16)
    return high, low


def picked(v, table):
    high, low = halves(v)
    return jnp.dot(high, table, preferred_element_type=F32) + jnp.dot(low, table, preferred_element_type=F32)


def total(v):
    v = jnp.sum(v, axis=0, keepdims=True)
    return jnp.sum(v, axis=1, keepdims=True)


class Level:
    def __init__(self, k, block):
        self.k = k
        self.n = block >> k
        self.h = HALO[k]
        self.r = 1 << k
        self.q = 0.25**k
        self.tiles = -(-(self.n + 2 * self.h) // 8)
        self.rows = 8 * self.tiles
        self.slabs = self.n + self.h
        self.first = 8 + self.h
        self.unroll = 14 if k == 0 else 28
        self.shape = (self.slabs + 2, self.rows + 16, 128)


def make_kernel(sizes, block):
    nx, ny, nz = sizes
    B = block[0]
    levels = [Level(k, B) for k in range(SPLIT)]
    n3 = B >> SPLIT
    groups = n3 * n3
    planes = -(-groups * 8 // 128)
    q3, q4 = 0.25**3, 0.25**4
    line = nz
    plane = nx * ny

    scratch = {}
    for name in ("rsr", "sgr", "rer"):
        scratch[name] = pltpu.VMEM((B, B, B), F32)
    scratch["insem"] = pltpu.SemaphoreType.DMA((3,))
    exchanges = {}

    def add_exchange(name, k, field, t, wide):
        lv = levels[k]
        per = 128 // (t * lv.r)
        ex = dict(lv=lv, field=field, t=t, wide=wide, per=per, pairs=lv.n // 2, groups=-(-lv.n // per))
        for d in ("s", "r"):
            scratch[f"y{d}_{name}"] = pltpu.VMEM((2, ex["pairs"], t, 128), F32)
            scratch[f"z{d}_{name}"] = pltpu.VMEM((2, ex["groups"], lv.rows, 128), F32)
        if wide:
            scratch[f"yx_{name}"] = pltpu.VMEM((2, t, t, 128), F32)
            scratch[f"zx_{name}"] = pltpu.VMEM((2, lv.rows, 128), F32)
        count = 17 if wide else 5
        scratch[f"send_{name}"] = pltpu.SemaphoreType.DMA((count,))
        scratch[f"recv_{name}"] = pltpu.SemaphoreType.DMA((count,))
        exchanges[name] = ex

    for lv in levels:
        k = lv.k
        for name in ("f", "s", "w", "e", "a", "b"):
            scratch[f"{name}{k}"] = pltpu.VMEM(lv.shape, F32)
        scratch[f"vm{k}"] = pltpu.VMEM((lv.rows, 128), F32)
        scratch[f"t{k}"] = pltpu.VMEM((lv.n // 2, lv.rows, 128), F32)
        scratch[f"u{k}"] = pltpu.VMEM((lv.slabs // 2 + 1, lv.rows + 16, 128), F32)
        add_exchange(f"f{k}", k, f"f{k}", lv.h, True)
        add_exchange(f"s{k}", k, f"s{k}", lv.h, True)
    scratch["sg"] = pltpu.VMEM(levels[0].shape, F32)
    add_exchange("sg", 0, "sg", 1, False)
    scratch["ap"] = pltpu.VMEM((B, levels[0].rows, 128), F32)
    scratch["own"] = pltpu.VMEM((levels[0].rows, 128), F32)
    for name, count in (("gs", planes), ("gf", planes), ("gr", 2)):
        scratch[name] = pltpu.VMEM((count, line, plane, 128), F32)
        scratch[f"{name}_send"] = pltpu.SemaphoreType.DMA((line,))
        scratch[f"{name}_recv"] = pltpu.SemaphoreType.DMA((line,))
    scratch["l3"] = pltpu.VMEM((n3, 8, 128), F32)
    for name in ("s3", "f3", "w3", "e3"):
        scratch[name] = pltpu.VMEM((planes * 128, 128), F32)
    scratch["x3"] = pltpu.VMEM((planes, plane * line, 128), F32)
    scratch["lhs"] = pltpu.VMEM((3, (n3 + 2) * 16, planes * 128), F32)

    names = list(scratch)

    def kernel(rs_ref, sg_ref, re_ref, sol_ref, res_ref, *refs):
        R = dict(zip(names, refs))
        gx, gy, gz = (lax.axis_index(a) for a in AXES)
        mine = gx * ny + gy

        inputs = [
            pltpu.make_async_copy(src, R[dst], R["insem"].at[i])
            for i, (src, dst) in enumerate(((sg_ref, "sgr"), (re_ref, "rer"), (rs_ref, "rsr")))
        ]
        for copy in inputs:
            copy.start()

        def start_of(lv):
            return 1 + gx * lv.h

        for lv in levels:
            k = lv.k
            z8 = jnp.zeros((8, 128), F32)
            zs = jnp.zeros((lv.rows, 128), F32)
            fields = ["e", "a", "b"] + (["sg"] if k == 0 else [])
            fields = [R[f if f == "sg" else f"{f}{k}"] for f in fields]

            def guard(a, c, fields=fields, lv=lv, z8=z8):
                for ref in fields:
                    ref[a, 0:8, :] = z8
                    ref[a, 8 + lv.rows : 16 + lv.rows, :] = z8
                return c

            loop(lv.shape[0], guard, 0, 2)
            for ref in fields:
                ref[0, 8 : 8 + lv.rows, :] = zs
                ref[lv.slabs + 1, 8 : 8 + lv.rows, :] = zs

            def blank(a, c, k=k, lv=lv):
                for name in ("f", "s"):
                    ref = R[f"{name}{k}"]
                    ref[a, 8:16, :] = jnp.zeros((8, 128), F32)
                    low = (lv.first + lv.n) // 8 * 8
                    ref[a, low : 8 + lv.rows, :] = jnp.zeros((8 + lv.rows - low, 128), F32)
                if k == 0:
                    ref = R["sg"]
                    ref[a, 8:16, :] = jnp.zeros((8, 128), F32)
                    ref[a, low : 8 + lv.rows, :] = jnp.zeros((8 + lv.rows - low, 128), F32)
                return c

            loop(lv.shape[0], blank, 0, 2)
            lane, row = iota((lv.rows, 128), 1), iota((lv.rows, 128), 0)
            wd = lv.h * lv.r
            ok = (lane < B) | ((lane < B + wd) & (gz < nz - 1)) | ((lane >= 128 - wd) & (gz > 0))
            ok = ok & (row >= jnp.where(gy > 0, 0, lv.h))
            ok = ok & (row < lv.n + lv.h + jnp.where(gy < ny - 1, lv.h, 0))
            R[f"vm{k}"][...] = jnp.where(ok, 1.0, 0.0)
            if k == 0:
                own = (lane < B) & (row >= lv.h) & (row < lv.h + lv.n)
                R["own"][...] = jnp.where(own, 1.0, 0.0)
        for name, ex in exchanges.items():
            for m in ("yr", "zr") + (("yx", "zx") if ex["wide"] else ()):
                ref = R[f"{m}_{name}"]
                ref[...] = jnp.zeros(ref.shape, F32)

        barrier = pltpu.get_barrier_semaphore()
        others = []
        for dz in range(nz):
            for dx in range(nx):
                for dy in range(ny):
                    if dx or dy or dz:
                        others.append((dx, dy, dz))

        def device(dx, dy, dz):
            return {"gx": lax.rem(gx + dx, nx), "gy": lax.rem(gy + dy, ny), "gz": lax.rem(gz + dz, nz)}

        for to in others:
            pl.semaphore_signal(barrier, inc=1, device_id=device(*to), device_id_type=MESH)

        def exists(at, n, way):
            return at > 0 if way < 0 else at < n - 1

        def messages(name):
            ex = exchanges[name]
            lv, t, m = ex["lv"], ex["t"], ex["pairs"]
            f = R[ex["field"]]
            src = jnp.where(gx == 0, 1 + lv.n - t, 1 + lv.h)
            dst = jnp.where(gx == 0, 1 + lv.h - t, 1 + lv.n)
            rows = pl.ds(lv.first, lv.n)
            own = pl.ds(lv.h, lv.n)
            ys, yr, zs, zr = (R[f"{c}_{name}"] for c in ("ys", "yr", "zs", "zr"))
            out = [(f.at[pl.ds(src, t), rows, :], f.at[pl.ds(dst, t), rows, :], 1, 0, 0)]
            for i, way in enumerate((-1, 1)):
                out.append((ys.at[i], yr.at[1 - i], 0, way, 0))
                out.append((zs.at[i, :, own, :], zr.at[1 - i, :, own, :], 0, 0, way))
            if ex["wide"]:
                yx, zx = R[f"yx_{name}"], R[f"zx_{name}"]
                pair = jnp.where(gx == 0, m - t, 0)
                group = jnp.where(gx == 0, ex["groups"] - 1, 0)
                for i, way in enumerate((-1, 1)):
                    out.append((ys.at[i, pl.ds(pair, t)], yx.at[1 - i], 1, way, 0))
                    out.append((zs.at[i, group, own, :], zx.at[1 - i, own, :], 1, 0, way))
                    for yway in (-1, 1):
                        here = pl.ds(lv.h if yway < 0 else lv.h + lv.n - t, t)
                        there = pl.ds(lv.h + lv.n if yway < 0 else lv.h - t, t)
                        out.append((zs.at[i, :, here, :], zr.at[1 - i, :, there, :], 0, yway, way))
                        out.append((zs.at[i, group, here, :], zx.at[1 - i, there, :], 1, yway, way))
            return out

        def each(name, f, getting):
            for i, (s, d, ox, oy, oz) in enumerate(messages(name)):
                copy = pltpu.make_async_remote_copy(
                    src_ref=s, dst_ref=d, send_sem=R[f"send_{name}"].at[i], recv_sem=R[f"recv_{name}"].at[i],
                    device_id={"gx": lax.rem(gx + ox, nx), "gy": gy + oy, "gz": gz + oz}, device_id_type=MESH)
                cond = None
                for at, n, way in ((gy, ny, oy), (gz, nz, oz)):
                    if way:
                        there = exists(at, n, -way if getting else way)
                        cond = there if cond is None else cond & there
                if cond is None:
                    f(copy)
                else:
                    pl.when(cond)(lambda copy=copy: f(copy))

        def send(name):
            each(name, lambda copy: copy.start(), False)

        def arrive(name):
            each(name, lambda copy: copy.wait_recv(), True)

        def sent(name):
            each(name, lambda copy: copy.wait_send(), False)

        def y_pack(name):
            ex = exchanges[name]
            lv, t, m = ex["lv"], ex["t"], ex["pairs"]
            f, a = R[ex["field"]], start_of(lv)
            lane = iota((t, 128), 1)
            for side, row in ((0, lv.first), (1, lv.first + lv.n - t)):
                for i in range(m):
                    v = f[a + i, row : row + t, :]
                    R[f"ys_{name}"][side, i] = jnp.where(lane < 64, v, roll(f[a + i + m, row : row + t, :], 64))

        def y_unpack(name):
            ex = exchanges[name]
            lv, t, m = ex["lv"], ex["t"], ex["pairs"]
            f, a = R[ex["field"]], start_of(lv)
            keep = iota((t, 128), 1) < B
            edge = jnp.where(gx == 0, 1 + lv.n, 1)
            for side, row in ((0, lv.first - t), (1, lv.first + lv.n)):
                for i in range(m):
                    v = R[f"yr_{name}"][side, i]
                    f[a + i, row : row + t, :] = jnp.where(keep, v, 0.0)
                    f[a + i + m, row : row + t, :] = jnp.where(keep, roll(v, 64), 0.0)
                if ex["wide"]:
                    for i in range(t):
                        v = pltpu.roll(R[f"yx_{name}"][side, i], gx * 64, 1)
                        f[edge + i, row : row + t, :] = jnp.where(keep, v, 0.0)

        def z_pack(name):
            ex = exchanges[name]
            lv, per = ex["lv"], ex["per"]
            wd = ex["t"] * lv.r
            f, a = R[ex["field"]], start_of(lv)
            lane = iota((lv.rows, 128), 1)
            for g in range(ex["groups"]):
                low = high = None
                count = min(per, lv.n - g * per)
                for j in reversed(range(count)):
                    v = f[a + g * per + j, 8 : 8 + lv.rows, :]
                    c = j * wd
                    one, two = roll(v, c), roll(v, c - (B - wd))
                    low = one if low is None else jnp.where(lane < c + wd, one, low)
                    high = two if high is None else jnp.where(lane < c + wd, two, high)
                R[f"zs_{name}"][0, g] = low
                R[f"zs_{name}"][1, g] = high

        def pack_send(name):
            y_pack(name)
            z_pack(name)
            send(name)

        def z_unpacked(name, use):
            ex = exchanges[name]
            lv, per, t = ex["lv"], ex["per"], ex["t"]
            wd = t * lv.r
            f, a = R[ex["field"]], start_of(lv)
            lane = iota((lv.rows, 128), 1)

            def put(i, below, above):
                v = jnp.where(lane < B + wd, above, jnp.where(lane >= 128 - wd, below, 0.0))
                use(i, jnp.where(lane < B, f[i, 8 : 8 + lv.rows, :], v))

            for j in range(lv.n):
                g, c = j // per, j % per * wd
                put(a + j, roll(R[f"zr_{name}"][0, g], -wd - c), roll(R[f"zr_{name}"][1, g], B - c))
            if ex["wide"]:
                edge = jnp.where(gx == 0, 1 + lv.n, 1)
                for j in range(t):
                    c0, c1 = j * wd, (lv.n - t + j - (ex["groups"] - 1) * per) * wd
                    one = jnp.where(gx == 0, (-wd - c0) % 128, (-wd - c1) % 128)
                    two = jnp.where(gx == 0, (B - c0) % 128, (B - c1) % 128)
                    put(edge + j, pltpu.roll(R[f"zx_{name}"][0], one, 1), pltpu.roll(R[f"zx_{name}"][1], two, 1))

        def beside_of(lv, ref, a):
            rows = lv.rows
            c = ref[a, 8 : 8 + rows, :]
            v = ref[a + 1, 8 : 8 + rows, :] + ref[a - 1, 8 : 8 + rows, :]
            v = v + (ref[a, 9 : 9 + rows, :] + ref[a, 7 : 7 + rows, :])
            return c, v + (roll(c, lv.r) + roll(c, -lv.r))

        def span(lv, far):
            return lv.n + far, 1 + gx * (lv.h - far)

        def relax(lv, src, dst, far):
            k = lv.k
            count, a0 = span(lv, far)

            def one(i, carry):
                a = a0 + i
                c, v = beside_of(lv, R[f"{src}{k}"], a)
                w = R[f"w{k}"][a, 8 : 8 + lv.rows, :]
                e = R[f"e{k}"][a, 8 : 8 + lv.rows, :]
                R[f"{dst}{k}"][a, 8 : 8 + lv.rows, :] = c * KEEP + (e + w * v)
                return carry

            loop(count, one, 0, lv.unroll)

        def weigh(lv):
            k = lv.k
            vm = R[f"vm{k}"]

            def use(i, s):
                R[f"w{k}"][i, 8 : 8 + lv.rows, :] = vm[...] * ((DAMPING * lv.q) / (6.0 * lv.q + s))

            z_unpacked(f"s{k}", use)

        def begin(lv):
            k = lv.k
            scale = 1.0 / lv.q

            def use(i, f):
                w = R[f"w{k}"][i, 8 : 8 + lv.rows, :]
                R[f"e{k}"][i, 8 : 8 + lv.rows, :] = (w * scale) * f if k else w * f

            z_unpacked(f"f{k}", use)

        def restrict(lv, of, name):
            k = lv.k
            a0 = start_of(lv)
            half = lv.n // 2
            lane = iota((lv.rows, 128), 1)
            t = R[f"t{k}"]

            def one(j, c):
                v = of(a0 + 2 * j) + of(a0 + 2 * j + 1)
                v = v + jnp.where((lane & lv.r) == 0, roll(v, -lv.r), roll(v, lv.r))
                t[j] = v
                return c

            loop(half, one, 0, lv.unroll // 2)
            wide = iota((half, 128), 1) < B

            def two(j, c):
                v = t[j, pl.ds(lv.h, half, stride=2), :] + t[j, pl.ds(lv.h + 1, half, stride=2), :]
                v = jnp.where(wide, 0.125 * v, 0.0)
                if k + 1 < SPLIT:
                    nxt = levels[k + 1]
                    R[f"{name}{k + 1}"][start_of(nxt) + j, nxt.first : nxt.first + half, :] = v
                else:
                    R["l3"][j, 0:half, :] = v
                return c

            loop(half, two, 0, 12)

        def left_of(lv, src):
            k = lv.k

            def f(a):
                c, v = beside_of(lv, R[f"{src}{k}"], a)
                s = R[f"s{k}"][a, 8 : 8 + lv.rows, :]
                return R[f"f{k}"][a, 8 : 8 + lv.rows, :] - ((6.0 * lv.q + s) * c - lv.q * v)

            return f

        def coefficient(lv):
            return lambda a: R[f"s{lv.k}"][a, 8 : 8 + lv.rows, :]

        def prolong(lv, coarse_rows):
            k = lv.k
            nxt_far = 2
            half = lv.n // 2
            m = half + 2 * nxt_far
            shift = lv.h - 2 * nxt_far
            u = R[f"u{k}"]

            def put(j, c):
                v = coarse_rows(j, m)
                u[j, pl.ds(shift, m, stride=2), :] = v
                u[j, pl.ds(shift + 1, m, stride=2), :] = v
                return c

            loop(half + nxt_far, put, 0, 7)

        def add_up(lv):
            k = lv.k
            a0 = 1 + gx * (lv.h - 4)

            def one(j, c):
                p = R[f"u{k}"][j, 0 : lv.rows, :]
                if k:
                    row = iota((lv.rows, 128), 0)
                    p = jnp.where((row >= lv.h - 4) & (row < lv.h + lv.n + 4), p, 0.0)
                if k == SPLIT - 1:
                    p = jnp.where(R[f"vm{k}"][...] > 0.0, p, 0.0)
                for d in range(2):
                    a = a0 + 2 * j + d
                    R[f"b{k}"][a, 8 : 8 + lv.rows, :] = R[f"a{k}"][a, 8 : 8 + lv.rows, :] + p
                return c

            loop((lv.n + 4) // 2, one, 0, 7)

        def gather_copy(name, dx, dy, dz):
            g = R[name]
            here = g.at[:, gz, pl.ds(mine, 1), :]
            return pltpu.make_async_remote_copy(
                src_ref=here, dst_ref=here, send_sem=R[f"{name}_send"].at[dz], recv_sem=R[f"{name}_recv"].at[gz],
                device_id=device(dx, dy, dz), device_id_type=MESH)

        def gather_start(name, rows):
            for p, v in enumerate(rows):
                R[name][p, gz, pl.ds(mine, 1), :] = v
            for to in others:
                gather_copy(name, *to).start()

        def gather_line(name, dz):
            z = lax.rem(gz + dz, nz)
            g = R[name]
            part = g.at[:, z, pl.ds(0, plane - 1), :] if dz == 0 else g.at[:, z]
            return pltpu.make_async_remote_copy(
                src_ref=part, dst_ref=part, send_sem=R[f"{name}_send"].at[dz], recv_sem=R[f"{name}_recv"].at[z],
                device_id=device(1, 0, 0), device_id_type=MESH)

        def gather_end(name):
            for dz in range(nz):
                gather_line(name, dz).wait_recv()

        def gather_sent(name):
            for dz in range(nz):
                gather_line(name, dz).wait_send()

        def local_vector():
            wide = planes * 128
            v = R["l3"][...].reshape(n3 * 8, 128)
            l, c = iota((128, wide), 0), iota((128, wide), 1)
            table = jnp.where((l == (c & 7) * (1 << SPLIT)) & ((c & 7) < n3) & (c < groups * 8), 1.0, 0.0).astype(BF16)
            v = picked(v, table)
            row, c = iota((n3 * 8, wide), 0), iota((n3 * 8, wide), 1)
            keep = ((row & 7) < n3) & ((c >> 3) == (row >> 3) * n3 + (row & 7))
            v = jnp.sum(jnp.where(keep, v, 0.0), axis=0, keepdims=True)
            return [v[:, 128 * p : 128 * p + 128] for p in range(planes)]

        def by_device(name, dst):
            for p in range(planes):
                v = R[name][p].reshape(plane * line, 128)
                R[dst][128 * p : 128 * p + 128, :] = v.T

        lv0, lv1, lv2 = levels
        inside = jnp.zeros((B, 128 - B), F32)

        def take(raw, dst):
            def one(x, c):
                v = jnp.concatenate([R[raw][x], inside], axis=1)
                R[dst][start_of(lv0) + x, lv0.first : lv0.first + B, :] = v
                return c

            loop(B, one, 0, 4)

        R["l3"][...] = jnp.zeros((n3, 8, 128), F32)
        inputs[0].wait()
        take("sgr", "sg")
        y_pack("sg")
        z_pack("sg")
        inputs[1].wait()
        take("rer", "s0")
        y_pack("s0")
        z_pack("s0")
        restrict(lv0, coefficient(lv0), "s")
        y_pack("s1")
        z_pack("s1")
        restrict(lv1, coefficient(lv1), "s")
        y_pack("s2")
        z_pack("s2")
        restrict(lv2, coefficient(lv2), "s")
        vector3 = local_vector()
        inputs[2].wait()
        take("rsr", "f0")
        pl.semaphore_wait(barrier, len(others))
        send("sg")
        for k in range(SPLIT):
            send(f"s{k}")
        gather_start("gs", vector3)
        arrive("sg")
        sent("sg")
        y_unpack("sg")

        def keep_guess(i, v):
            R["sg"][i, 8 : 8 + lv0.rows, :] = v

        z_unpacked("sg", keep_guess)

        def first_residual(x, carry):
            a = start_of(lv0) + x
            c, v = beside_of(lv0, R["sg"], a)
            s = R["s0"][a, 8 : 8 + lv0.rows, :]
            f = R["f0"][a, 8 : 8 + lv0.rows, :] - ((6.0 + s) * c - v)
            R["f0"][a, 8 : 8 + lv0.rows, :] = jnp.where(R["own"][...] > 0.0, f, 0.0)
            return carry

        loop(B, first_residual, 0, lv0.unroll)
        pack_send("f0")
        for lv in levels:
            arrive(f"s{lv.k}")
            y_unpack(f"s{lv.k}")
            weigh(lv)
        arrive("f0")
        y_unpack("f0")
        begin(lv0)

        def first_relax(lv):
            k = lv.k
            count, a0 = span(lv, 4)

            def one(i, carry):
                a = a0 + i
                c, v = beside_of(lv, R[f"e{k}"], a)
                w = R[f"w{k}"][a, 8 : 8 + lv.rows, :]
                R[f"a{k}"][a, 8 : 8 + lv.rows, :] = c * (1.0 + KEEP) + w * v
                return carry

            loop(count, one, 0, lv.unroll)

        first_relax(lv0)
        restrict(lv0, left_of(lv0, "a"), "f")

        def deeper(lv):
            name = f"f{lv.k}"
            pack_send(name)
            arrive(name)
            y_unpack(name)
            begin(lv)
            first_relax(lv)
            restrict(lv, left_of(lv, "a"), "f")

        deeper(lv1)
        deeper(lv2)
        gather_start("gf", local_vector())

        gather_end("gs")
        by_device("gs", "s3")
        lane8, row8 = iota((8, 128), 1), iota((8, 128), 0)
        dev_y, dev_x, dev_z = lane8 & (ny - 1), (lane8 >> 2) & 1, lane8 >> 3
        step_x, step_z = ny, plane
        has = {
            ("y", 1): dev_y < ny - 1, ("y", -1): dev_y > 0, ("x", 1): dev_x < nx - 1, ("x", -1): dev_x > 0,
            ("z", 1): dev_z < nz - 1, ("z", -1): dev_z > 0,
        }
        strides = {"y": 1, "x": step_x, "z": step_z}

        def across(v, axis, way):
            return jnp.where(has[axis, way], roll(v, -way * strides[axis]), 0.0)

        def around(get, m):
            def one(x, y):
                c = get(x, y)
                r = n3 // m
                up = jnp.where(row8 >= n3 - r, roll(across(c, "z", 1), n3 - r, 0), roll(c, -r, 0))
                dn = jnp.where(row8 < r, roll(across(c, "z", -1), r - n3, 0), roll(c, r, 0))
                v = up + dn
                v = v + (get(x + 1, y) if x + 1 < m else across(get(0, y), "x", 1))
                v = v + (get(x - 1, y) if x else across(get(m - 1, y), "x", -1))
                v = v + (get(x, y + 1) if y + 1 < m else across(get(x, 0), "y", 1))
                v = v + (get(x, y - 1) if y else across(get(x, m - 1), "y", -1))
                return c, v

            return one

        cells = [(x, y) for x in range(n3) for y in range(n3)]
        m4 = n3 // 2
        cells4 = [(x, y) for x in range(m4) for y in range(m4)]
        live = row8 < n3

        def tile(name, x, y):
            g = x * n3 + y
            return R[name][8 * g : 8 * g + 8, :]

        for x, y in cells:
            R["w3"][8 * (x * n3 + y) : 8 * (x * n3 + y) + 8, :] = jnp.where(
                live, (DAMPING * q3) / (6.0 * q3 + tile("s3", x, y)), 0.0)

        def coarser(get):
            out = {}
            for x, y in cells4:
                v = (get(2 * x, 2 * y) + get(2 * x, 2 * y + 1)) + (get(2 * x + 1, 2 * y) + get(2 * x + 1, 2 * y + 1))
                v = v + jnp.where((row8 & 1) == 0, roll(v, -1, 0), roll(v, 1, 0))
                out[x, y] = jnp.where(live, 0.125 * v, 0.0)
            return out

        s4 = coarser(lambda x, y: tile("s3", x, y))
        gather_end("gf")
        by_device("gf", "f3")
        e = {}
        e0 = {}
        for c in cells:
            e0[c] = (tile("w3", *c) * (1.0 / q3)) * tile("f3", *c)
        op = around(lambda x, y: e0[x, y], n3)
        for c in cells:
            u, v = op(*c)
            e[c] = u * (1.0 + KEEP) + tile("w3", *c) * v
        op = around(lambda x, y: e[x, y], n3)
        rest = {}
        for c in cells:
            u, v = op(*c)
            rest[c] = jnp.where(live, tile("f3", *c) - ((6.0 * q3 + tile("s3", *c)) * u - q3 * v), 0.0)
        f4 = coarser(lambda x, y: rest[x, y])

        def inner(u, v):
            s = None
            for c in cells4:
                s = u[c] * v[c] if s is None else s + u[c] * v[c]
            return total(s)

        r4 = dict(f4)
        p4 = dict(f4)
        e4 = {c: jnp.zeros((8, 128), F32) for c in cells4}
        rr = inner(r4, r4)
        for _ in range(BOTTOM_ITERS):
            op = around(lambda x, y: p4[x, y], m4)
            q = {}
            for c in cells4:
                u, v = op(*c)
                q[c] = jnp.where(live, (6.0 * q4 + s4[c]) * u - q4 * v, 0.0)
            a = rr / inner(p4, q)
            e4 = {c: e4[c] + a * p4[c] for c in cells4}
            r4 = {c: r4[c] - a * q[c] for c in cells4}
            new = inner(r4, r4)
            ratio = new / rr
            p4 = {c: r4[c] + ratio * p4[c] for c in cells4}
            rr = new
        e = {(x, y): e[x, y] + e4[x // 2, y // 2] for x, y in cells}
        for _ in range(2):
            op = around(lambda x, y: e[x, y], n3)
            nxt = {}
            for c in cells:
                u, v = op(*c)
                nxt[c] = u * KEEP + (e0[c] + tile("w3", *c) * v)
            e = nxt
        for x, y in cells:
            g = x * n3 + y
            R["e3"][8 * g : 8 * g + 8, :] = e[x, y]
        R["e3"][groups * 8 :, :] = jnp.zeros((planes * 128 - groups * 8, 128), F32)
        for p in range(planes):
            R["x3"][p] = R["e3"][128 * p : 128 * p + 128, :].T

        wide = planes * 128
        slabs3 = n3 + 2
        lane_w = iota((8, wide), 1) >> 3
        row_w = iota((8, wide), 0)
        lo_rows = jnp.where(row_w < 2, n3 - 2 + row_w, -1000)
        mid_rows = jnp.where(row_w < 2, -1000, row_w - 2)
        hi_rows = jnp.where(row_w < 2, row_w, -1000)
        y_below, y_above = jnp.maximum(gy - 1, 0), jnp.minimum(gy + 1, ny - 1)
        z_at = [jnp.maximum(gz - 1, 0), gz, jnp.minimum(gz + 1, nz - 1)]

        def vector(dev):
            return jnp.concatenate([R["x3"][p, pl.ds(dev, 1), :] for p in range(planes)], axis=1)

        for i in range(slabs3):
            partner = jnp.where(gx == 0, i >= n3, i < 2)
            px = jnp.where(partner, 1 - gx, gx)
            xx = jnp.where(gx == 0, i - jnp.where(i >= n3, n3, 0), i - 2 + jnp.where(i < 2, n3, 0))
            lo, mid, hi = (lane_w == xx * n3 + rows for rows in (lo_rows, mid_rows, hi_rows))
            for d in range(3):
                at_y = lambda g: vector(z_at[d] * plane + px * ny + g)
                first = jnp.where(mid, at_y(gy), jnp.where(lo, at_y(y_below), 0.0))
                second = jnp.where(hi, at_y(y_above), 0.0)
                R["lhs"][d, 16 * i : 16 * i + 8, :] = first
                R["lhs"][d, 16 * i + 8 : 16 * i + 16, :] = second
        l, c = iota((wide, 128), 1), iota((wide, 128), 0)
        table = jnp.where((l < B) & ((c & 7) == (l >> SPLIT)) & (c < groups * 8), 1.0, 0.0).astype(BF16)
        v = picked(R["lhs"][...].reshape(3 * slabs3 * 16, wide), table).reshape(3, slabs3, 16, 128)
        v = v[1] + roll(v[2].reshape(slabs3 * 16, 128), B).reshape(slabs3, 16, 128) + roll(
            v[0].reshape(slabs3 * 16, 128), -B).reshape(slabs3, 16, 128)
        u = R["u2"]
        shift = lv2.h - 4
        for i in range(slabs3):
            m = n3 + 4
            u[i, pl.ds(shift, m, stride=2), :] = v[i, 0:m]
            u[i, pl.ds(shift + 1, m, stride=2), :] = v[i, 0:m]

        add_up(lv2)
        relax(lv2, "b", "a", 4)
        relax(lv2, "a", "b", 2)

        def coarse_of(nxt, ref):
            a0 = 1 + gx * (nxt.h - 2)
            return lambda j, m: R[ref][a0 + j, nxt.first - 2 : nxt.first - 2 + m, :]

        prolong(lv1, coarse_of(lv2, "b2"))
        add_up(lv1)
        relax(lv1, "b", "a", 4)
        relax(lv1, "a", "b", 2)
        prolong(lv0, coarse_of(lv1, "b1"))
        add_up(lv0)
        relax(lv0, "b", "a", 4)
        relax(lv0, "a", "b", 2)

        def image(x, sums):
            upper, lower = sums
            a = start_of(lv0) + x
            c, v = beside_of(lv0, R["b0"], a)
            s = R["s0"][a, 8 : 8 + lv0.rows, :]
            ap = (6.0 + s) * c - v
            R["ap"][x] = ap
            c = jnp.where(R["own"][...] > 0.0, c, 0.0)
            return upper + R["f0"][a, 8 : 8 + lv0.rows, :] * c, lower + ap * c

        zero = jnp.zeros((lv0.rows, 128), F32)
        upper, lower = loop(B, image, (zero, zero), lv0.unroll)
        gather_start("gr", [jnp.sum(v, axis=0, keepdims=True) for v in (upper, lower)])
        gather_end("gr")
        sums = [total(jnp.sum(R["gr"][p], axis=0)) for p in range(2)]
        step_length = sums[0] / sums[1]

        def finish(x, c):
            a = start_of(lv0) + x
            p = R["b0"][a, lv0.first : lv0.first + B, :]
            f = R["f0"][a, lv0.first : lv0.first + B, :]
            q = R["ap"][x, lv0.h : lv0.h + B, :]
            sol_ref[x] = R["sgr"][x] + (step_length * p)[:, 0:B]
            res_ref[x] = (f - step_length * q)[:, 0:B]
            return c

        loop(B, finish, 0, 4)
        for name in exchanges:
            if name != "sg":
                sent(name)
        for name in ("gs", "gf", "gr"):
            gather_sent(name)

    return kernel, list(scratch.values())


def solution(mesh):
    sizes = tuple(mesh.shape[a] for a in AXES)

    def body(right_side, start_guess, reaction):
        kernel, scratch = make_kernel(sizes, right_side.shape)
        out = jax.ShapeDtypeStruct(right_side.shape, F32)
        return tuple(
            pl.pallas_call(
                kernel,
                out_shape=(out, out),
                in_specs=[pl.BlockSpec(memory_space=pl.ANY)] * 3,
                out_specs=(pl.BlockSpec(memory_space=pltpu.VMEM),) * 2,
                scratch_shapes=scratch,
                compiler_params=pltpu.CompilerParams(
                    collective_id=0, has_side_effects=True, vmem_limit_bytes=60 * 2**20
                ),
                name="cg_step",
            )(right_side, start_guess, reaction)
        )

    placed = P(*AXES)
    return jax.shard_map(
        body, mesh=mesh, in_specs=(placed,) * 3, out_specs=(placed,) * 2, check_vma=False
    )
```

```python
import jax
import jax.numpy as jnp
from jax import lax
from jax.experimental import pallas as pl
from jax.experimental.pallas import tpu as pltpu
from jax.sharding import PartitionSpec as P

BOTTOM_ITERS = 6
AXES = ("gx", "gy", "gz")
MESH = pl.DeviceIdType.MESH
F32 = jnp.float32
BF16 = jnp.bfloat16
DAMPING = 6.0 / 7.0
KEEP = 1.0 / 7.0
SPLIT = 3
HALO = (4, 5, 5)


def loop(n, f, carry=0, unroll=4):
    unroll = min(unroll, n)
    while n % unroll:
        unroll -= 1

    def step(i, c):
        for k in range(unroll):
            c = f(i * unroll + k, c)
        return c

    return lax.fori_loop(0, n // unroll, step, carry)


def iota(shape, axis):
    return lax.broadcasted_iota(jnp.int32, shape, axis)


def roll(v, shift, axis=1):
    shift = shift % v.shape[axis] if isinstance(shift, int) else shift
    return v if isinstance(shift, int) and shift == 0 else pltpu.roll(v, shift, axis)


def halves(v):
    high = v.astype(BF16)
    low = (v - high.astype(F32)).astype(BF16)
    return high, low


def picked(v, table):
    high, low = halves(v)
    return jnp.dot(high, table, preferred_element_type=F32) + jnp.dot(low, table, preferred_element_type=F32)


def total(v):
    v = jnp.sum(v, axis=0, keepdims=True)
    return jnp.sum(v, axis=1, keepdims=True)


class Level:
    def __init__(self, k, block):
        self.k = k
        self.n = block >> k
        self.h = HALO[k]
        self.r = 1 << k
        self.q = 0.25**k
        self.tiles = -(-(self.n + 2 * self.h) // 8)
        self.rows = 8 * self.tiles
        self.slabs = self.n + self.h
        self.first = 8 + self.h
        self.unroll = 14 if k == 0 else 28
        self.shape = (self.slabs + 2, self.rows + 16, 128)


def make_kernel(sizes, block):
    nx, ny, nz = sizes
    B = block[0]
    levels = [Level(k, B) for k in range(SPLIT)]
    n3 = B >> SPLIT
    groups = n3 * n3
    planes = -(-groups * 8 // 128)
    packed = -(-groups * n3 // 128)
    q3, q4 = 0.25**3, 0.25**4
    line = nz
    plane = nx * ny

    scratch = {}
    for name in ("rsr", "sgr", "rer"):
        scratch[name] = pltpu.VMEM((B, B, B), F32)
    scratch["insem"] = pltpu.SemaphoreType.DMA((3,))
    exchanges = {}

    def add_exchange(name, k, field, t, wide):
        lv = levels[k]
        per = 128 // (t * lv.r)
        ex = dict(lv=lv, field=field, t=t, wide=wide, per=per, pairs=lv.n // 2, groups=-(-lv.n // per))
        for d in ("s", "r"):
            scratch[f"y{d}_{name}"] = pltpu.VMEM((2, ex["pairs"], t, 128), F32)
            scratch[f"z{d}_{name}"] = pltpu.VMEM((2, ex["groups"], lv.rows, 128), F32)
        if wide:
            scratch[f"yx_{name}"] = pltpu.VMEM((2, t, t, 128), F32)
            scratch[f"zx_{name}"] = pltpu.VMEM((2, lv.rows, 128), F32)
        scratch[f"send_{name}"] = pltpu.SemaphoreType.DMA
        scratch[f"recv_{name}"] = pltpu.SemaphoreType.DMA
        exchanges[name] = ex

    for lv in levels:
        k = lv.k
        for name in ("f", "s", "w", "e", "a", "b"):
            scratch[f"{name}{k}"] = pltpu.VMEM(lv.shape, F32)
        scratch[f"vm{k}"] = pltpu.VMEM((lv.rows, 128), F32)
        scratch[f"t{k}"] = pltpu.VMEM((lv.n // 2, lv.rows, 128), F32)
        scratch[f"u{k}"] = pltpu.VMEM((lv.slabs // 2 + 1, lv.rows + 16, 128), F32)
        add_exchange(f"f{k}", k, f"f{k}", lv.h, True)
        add_exchange(f"s{k}", k, f"s{k}", lv.h, True)
    scratch["sg"] = pltpu.VMEM(levels[0].shape, F32)
    add_exchange("sg", 0, "sg", 1, False)
    scratch["ap"] = pltpu.VMEM((B, levels[0].rows, 128), F32)
    scratch["own"] = pltpu.VMEM((levels[0].rows, 128), F32)
    for name, count in (("gs", packed), ("gf", packed), ("gr", 1)):
        scratch[name] = pltpu.VMEM((count, line, plane, 128), F32)
        scratch[f"{name}_send"] = pltpu.SemaphoreType.DMA
        scratch[f"{name}_recv"] = pltpu.SemaphoreType.DMA
    scratch["count"] = pltpu.VMEM((1024, 128), F32)
    scratch["l3"] = pltpu.VMEM((n3, 8, 128), F32)
    for name in ("s3", "f3", "w3", "e3"):
        scratch[name] = pltpu.VMEM((planes * 128, 128), F32)
    scratch["x3"] = pltpu.VMEM((planes, plane * line, 128), F32)
    scratch["lhs"] = pltpu.VMEM((3, (n3 + 2) * 16, planes * 128), F32)

    names = list(scratch)

    def kernel(rs_ref, sg_ref, re_ref, sol_ref, res_ref, *refs):
        R = dict(zip(names, refs))
        gx, gy, gz = (lax.axis_index(a) for a in AXES)
        mine = gx * ny + gy

        inputs = [
            pltpu.make_async_copy(src, R[dst], R["insem"].at[i])
            for i, (src, dst) in enumerate(((sg_ref, "sgr"), (re_ref, "rer"), (rs_ref, "rsr")))
        ]
        for copy in inputs:
            copy.start()

        def start_of(lv):
            return 1 + gx * lv.h

        for lv in levels:
            k = lv.k
            z8 = jnp.zeros((8, 128), F32)
            zs = jnp.zeros((lv.rows, 128), F32)
            fields = ["e", "a", "b"] + (["sg"] if k == 0 else [])
            fields = [R[f if f == "sg" else f"{f}{k}"] for f in fields]

            def guard(a, c, fields=fields, lv=lv, z8=z8):
                for ref in fields:
                    ref[a, 0:8, :] = z8
                    ref[a, 8 + lv.rows : 16 + lv.rows, :] = z8
                return c

            loop(lv.shape[0], guard, 0, 2)
            for ref in fields:
                ref[0, 8 : 8 + lv.rows, :] = zs
                ref[lv.slabs + 1, 8 : 8 + lv.rows, :] = zs

            def blank(a, c, k=k, lv=lv):
                for name in ("f", "s"):
                    ref = R[f"{name}{k}"]
                    ref[a, 8:16, :] = jnp.zeros((8, 128), F32)
                    low = (lv.first + lv.n) // 8 * 8
                    ref[a, low : 8 + lv.rows, :] = jnp.zeros((8 + lv.rows - low, 128), F32)
                if k == 0:
                    ref = R["sg"]
                    ref[a, 8:16, :] = jnp.zeros((8, 128), F32)
                    ref[a, low : 8 + lv.rows, :] = jnp.zeros((8 + lv.rows - low, 128), F32)
                return c

            loop(lv.shape[0], blank, 0, 2)
            lane, row = iota((lv.rows, 128), 1), iota((lv.rows, 128), 0)
            wd = lv.h * lv.r
            ok = (lane < B) | ((lane < B + wd) & (gz < nz - 1)) | ((lane >= 128 - wd) & (gz > 0))
            ok = ok & (row >= jnp.where(gy > 0, 0, lv.h))
            ok = ok & (row < lv.n + lv.h + jnp.where(gy < ny - 1, lv.h, 0))
            R[f"vm{k}"][...] = jnp.where(ok, 1.0, 0.0)
            if k == 0:
                own = (lane < B) & (row >= lv.h) & (row < lv.h + lv.n)
                R["own"][...] = jnp.where(own, 1.0, 0.0)
        for name, ex in exchanges.items():
            for m in ("yr", "yx", "zr", "zx") if ex["wide"] else ("yr", "zr"):
                ref = R[f"{m}_{name}"]
                ref[...] = jnp.zeros(ref.shape, F32)

        barrier = pltpu.get_barrier_semaphore()
        others = []
        for dz in range(nz):
            for dx in range(nx):
                for dy in range(ny):
                    if dx or dy or dz:
                        others.append((dx, dy, dz))

        def hops(to):
            dx, dy, dz = to
            return dx + min(dy, ny - dy) + min(dz % 4, 4 - dz % 4) + min(dz // 4, nz // 4 - dz // 4)

        others.sort(key=lambda to: (-hops(to), to))

        def device(dx, dy, dz):
            return {"gx": lax.rem(gx + dx, nx), "gy": lax.rem(gy + dy, ny), "gz": lax.rem(gz + dz, nz)}

        for to in others:
            pl.semaphore_signal(barrier, inc=1, device_id=device(*to), device_id_type=MESH)

        def messages(name):
            ex = exchanges[name]
            lv, t, m = ex["lv"], ex["t"], ex["pairs"]
            f = R[ex["field"]]
            src = jnp.where(gx == 0, 1 + lv.n - t, 1 + lv.h)
            dst = jnp.where(gx == 0, 1 + lv.h - t, 1 + lv.n)
            rows = pl.ds(lv.first, lv.n)
            own = pl.ds(lv.h, lv.n)
            ys, yr, zs, zr = (R[f"{c}_{name}"] for c in ("ys", "yr", "zs", "zr"))
            out = [(f.at[pl.ds(src, t), rows, :], f.at[pl.ds(dst, t), rows, :], 1, 0, 0)]
            for i, way in enumerate((-1, 1)):
                out.append((ys.at[i], yr.at[1 - i], 0, way, 0))
                out.append((zs.at[i, :, own, :], zr.at[1 - i, :, own, :], 0, 0, way))
            if ex["wide"]:
                yx, zx = R[f"yx_{name}"], R[f"zx_{name}"]
                pair = jnp.where(gx == 0, m - t, 0)
                group = jnp.where(gx == 0, ex["groups"] - 1, 0)
                for i, way in enumerate((-1, 1)):
                    out.append((ys.at[i, pl.ds(pair, t)], yx.at[1 - i], 1, way, 0))
                    out.append((zs.at[i, group, own, :], zx.at[1 - i, own, :], 1, 0, way))
                    for yway in (-1, 1):
                        here = pl.ds(lv.h if yway < 0 else lv.h + lv.n - t, t)
                        there = pl.ds(lv.h + lv.n if yway < 0 else lv.h - t, t)
                        out.append((zs.at[i, :, here, :], zr.at[1 - i, :, there, :], 0, yway, way))
                        out.append((zs.at[i, group, here, :], zx.at[1 - i, there, :], 1, yway, way))
            return out

        def guarded(cond, f):
            if cond is None:
                f()
            else:
                pl.when(cond)(f)

        def send(name):
            for src, dst, ox, oy, oz in messages(name):
                copy = pltpu.make_async_remote_copy(
                    src_ref=src, dst_ref=dst, send_sem=R[f"send_{name}"], recv_sem=R[f"recv_{name}"],
                    device_id=device(ox, oy % ny, oz % nz), device_id_type=MESH)
                cond = None
                for at, n, way in ((gy, ny, oy), (gz, nz, oz)):
                    if way:
                        there = at > 0 if way < 0 else at < n - 1
                        cond = there if cond is None else cond & there
                guarded(cond, copy.start)

        def counted(size, send_sem, recv_sem):
            rows = R["count"].at[pl.ds(0, size), :]
            return pltpu.make_async_remote_copy(
                src_ref=rows, dst_ref=rows, send_sem=send_sem, recv_sem=recv_sem,
                device_id=device(1, 0, 0), device_id_type=MESH)

        def in_all(name, getting):
            sizes = [(src.shape, oy, oz) for src, _, _, oy, oz in messages(name)]
            for y, at_y in ((0, gy == 0), (1, (gy > 0) & (gy < ny - 1)), (2, gy == ny - 1)):
                for z, at_z in ((0, gz == 0), (1, (gz > 0) & (gz < nz - 1)), (2, gz == nz - 1)):
                    rows = 0
                    for shape, oy, oz in sizes:
                        oy, oz = (-oy, -oz) if getting else (oy, oz)
                        if y + oy in (0, 1, 2) and z + oz in (0, 1, 2):
                            count = 1
                            for d in shape[:-1]:
                                count *= d
                            rows += count
                    copy = counted(rows, R[f"send_{name}"], R[f"recv_{name}"])
                    pl.when(at_y & at_z)(copy.wait_recv if getting else copy.wait_send)

        def arrive(name):
            in_all(name, True)

        def sent(name):
            in_all(name, False)

        def y_pack(name):
            ex = exchanges[name]
            lv, t, m = ex["lv"], ex["t"], ex["pairs"]
            f, a = R[ex["field"]], start_of(lv)
            lane = iota((t, 128), 1)
            for side, row in ((0, lv.first), (1, lv.first + lv.n - t)):
                for i in range(m):
                    v = f[a + i, row : row + t, :]
                    R[f"ys_{name}"][side, i] = jnp.where(lane < 64, v, roll(f[a + i + m, row : row + t, :], 64))

        def y_unpack(name):
            ex = exchanges[name]
            lv, t, m = ex["lv"], ex["t"], ex["pairs"]
            f, a = R[ex["field"]], start_of(lv)
            keep = iota((t, 128), 1) < B
            edge = jnp.where(gx == 0, 1 + lv.n, 1)
            for side, row, ok in ((0, lv.first - t, gy > 0), (1, lv.first + lv.n, gy < ny - 1)):
                for i in range(m):
                    v = R[f"yr_{name}"][side, i]
                    v = v if ex["wide"] else jnp.where(ok, v, 0.0)
                    f[a + i, row : row + t, :] = jnp.where(keep, v, 0.0)
                    f[a + i + m, row : row + t, :] = jnp.where(keep, roll(v, 64), 0.0)
                if ex["wide"]:
                    for i in range(t):
                        v = pltpu.roll(R[f"yx_{name}"][side, i], gx * 64, 1)
                        f[edge + i, row : row + t, :] = jnp.where(keep, v, 0.0)

        def z_pack(name):
            ex = exchanges[name]
            lv, per = ex["lv"], ex["per"]
            wd = ex["t"] * lv.r
            f, a = R[ex["field"]], start_of(lv)
            lane = iota((lv.rows, 128), 1)
            for g in range(ex["groups"]):
                low = high = None
                count = min(per, lv.n - g * per)
                for j in reversed(range(count)):
                    v = f[a + g * per + j, 8 : 8 + lv.rows, :]
                    c = j * wd
                    one, two = roll(v, c), roll(v, c - (B - wd))
                    low = one if low is None else jnp.where(lane < c + wd, one, low)
                    high = two if high is None else jnp.where(lane < c + wd, two, high)
                R[f"zs_{name}"][0, g] = low
                R[f"zs_{name}"][1, g] = high

        def pack_send(name):
            y_pack(name)
            z_pack(name)
            send(name)

        def z_unpacked(name, use):
            ex = exchanges[name]
            lv, per, t = ex["lv"], ex["per"], ex["t"]
            wd = t * lv.r
            f, a = R[ex["field"]], start_of(lv)
            lane = iota((lv.rows, 128), 1)

            def put(i, below, above):
                if not ex["wide"]:
                    below, above = jnp.where(gz > 0, below, 0.0), jnp.where(gz < nz - 1, above, 0.0)
                v = jnp.where(lane < B + wd, above, jnp.where(lane >= 128 - wd, below, 0.0))
                use(i, jnp.where(lane < B, f[i, 8 : 8 + lv.rows, :], v))

            for j in range(lv.n):
                g, c = j // per, j % per * wd
                put(a + j, roll(R[f"zr_{name}"][0, g], -wd - c), roll(R[f"zr_{name}"][1, g], B - c))
            if ex["wide"]:
                edge = jnp.where(gx == 0, 1 + lv.n, 1)
                for j in range(t):
                    c0, c1 = j * wd, (lv.n - t + j - (ex["groups"] - 1) * per) * wd
                    one = jnp.where(gx == 0, (-wd - c0) % 128, (-wd - c1) % 128)
                    two = jnp.where(gx == 0, (B - c0) % 128, (B - c1) % 128)
                    put(edge + j, pltpu.roll(R[f"zx_{name}"][0], one, 1), pltpu.roll(R[f"zx_{name}"][1], two, 1))

        def beside_of(lv, ref, a):
            rows = lv.rows
            c = ref[a, 8 : 8 + rows, :]
            v = ref[a + 1, 8 : 8 + rows, :] + ref[a - 1, 8 : 8 + rows, :]
            v = v + (ref[a, 9 : 9 + rows, :] + ref[a, 7 : 7 + rows, :])
            return c, v + (roll(c, lv.r) + roll(c, -lv.r))

        def span(lv, far):
            return lv.n + far, 1 + gx * (lv.h - far)

        def relax(lv, src, dst, far):
            k = lv.k
            count, a0 = span(lv, far)

            def one(i, carry):
                a = a0 + i
                c, v = beside_of(lv, R[f"{src}{k}"], a)
                w = R[f"w{k}"][a, 8 : 8 + lv.rows, :]
                e = R[f"e{k}"][a, 8 : 8 + lv.rows, :]
                R[f"{dst}{k}"][a, 8 : 8 + lv.rows, :] = c * KEEP + (e + w * v)
                return carry

            loop(count, one, 0, lv.unroll)

        def weigh(lv):
            k = lv.k
            vm = R[f"vm{k}"]

            def use(i, s):
                R[f"w{k}"][i, 8 : 8 + lv.rows, :] = vm[...] * ((DAMPING * lv.q) / (6.0 * lv.q + s))

            z_unpacked(f"s{k}", use)

        def begin(lv):
            k = lv.k
            scale = 1.0 / lv.q

            def use(i, f):
                w = R[f"w{k}"][i, 8 : 8 + lv.rows, :]
                R[f"e{k}"][i, 8 : 8 + lv.rows, :] = (w * scale) * f if k else w * f

            z_unpacked(f"f{k}", use)

        def restrict(lv, of, name):
            k = lv.k
            a0 = start_of(lv)
            half = lv.n // 2
            lane = iota((lv.rows, 128), 1)
            t = R[f"t{k}"]

            def one(j, c):
                v = of(a0 + 2 * j) + of(a0 + 2 * j + 1)
                v = v + jnp.where((lane & lv.r) == 0, roll(v, -lv.r), roll(v, lv.r))
                t[j] = v
                return c

            loop(half, one, 0, lv.unroll // 2)
            wide = iota((half, 128), 1) < B

            def two(j, c):
                v = t[j, pl.ds(lv.h, half, stride=2), :] + t[j, pl.ds(lv.h + 1, half, stride=2), :]
                v = jnp.where(wide, 0.125 * v, 0.0)
                if k + 1 < SPLIT:
                    nxt = levels[k + 1]
                    R[f"{name}{k + 1}"][start_of(nxt) + j, nxt.first : nxt.first + half, :] = v
                else:
                    R["l3"][j, 0:half, :] = v
                return c

            loop(half, two, 0, 12)

        def left_of(lv, src):
            k = lv.k

            def f(a):
                c, v = beside_of(lv, R[f"{src}{k}"], a)
                s = R[f"s{k}"][a, 8 : 8 + lv.rows, :]
                return R[f"f{k}"][a, 8 : 8 + lv.rows, :] - ((6.0 * lv.q + s) * c - lv.q * v)

            return f

        def coefficient(lv):
            return lambda a: R[f"s{lv.k}"][a, 8 : 8 + lv.rows, :]

        def prolong(lv, coarse_rows):
            k = lv.k
            nxt_far = 2
            half = lv.n // 2
            m = half + 2 * nxt_far
            shift = lv.h - 2 * nxt_far
            u = R[f"u{k}"]

            def put(j, c):
                v = coarse_rows(j, m)
                u[j, pl.ds(shift, m, stride=2), :] = v
                u[j, pl.ds(shift + 1, m, stride=2), :] = v
                return c

            loop(half + nxt_far, put, 0, 7)

        def add_up(lv):
            k = lv.k
            a0 = 1 + gx * (lv.h - 4)

            def one(j, c):
                p = R[f"u{k}"][j, 0 : lv.rows, :]
                if k:
                    row = iota((lv.rows, 128), 0)
                    p = jnp.where((row >= lv.h - 4) & (row < lv.h + lv.n + 4), p, 0.0)
                if k == SPLIT - 1:
                    p = jnp.where(R[f"vm{k}"][...] > 0.0, p, 0.0)
                for d in range(2):
                    a = a0 + 2 * j + d
                    R[f"b{k}"][a, 8 : 8 + lv.rows, :] = R[f"a{k}"][a, 8 : 8 + lv.rows, :] + p
                return c

            loop((lv.n + 4) // 2, one, 0, 7)

        def gather_copy(name, dx, dy, dz):
            g = R[name]
            here = g.at[:, gz, pl.ds(mine, 1), :]
            return pltpu.make_async_remote_copy(
                src_ref=here, dst_ref=here, send_sem=R[f"{name}_send"], recv_sem=R[f"{name}_recv"],
                device_id=device(dx, dy, dz), device_id_type=MESH)

        def gather_start(name, rows):
            for p, v in enumerate(rows):
                R[name][p, gz, pl.ds(mine, 1), :] = v
            for to in others:
                gather_copy(name, *to).start()

        def gathered(name):
            size = len(others) * R[name].shape[0]
            return counted(size, R[f"{name}_send"], R[f"{name}_recv"])

        def gather_end(name):
            gathered(name).wait_recv()

        def gather_sent(name):
            gathered(name).wait_send()

        def local_vector():
            wide = packed * 128
            v = R["l3"][...].reshape(n3 * 8, 128)
            l, c = iota((128, wide), 0), iota((128, wide), 1)
            table = jnp.where((l == c % n3 * (1 << SPLIT)) & (c < groups * n3), 1.0, 0.0).astype(BF16)
            v = picked(v, table)
            row, c = iota((n3 * 8, wide), 0), iota((n3 * 8, wide), 1)
            keep = ((row & 7) < n3) & (c // n3 == (row >> 3) * n3 + (row & 7))
            v = jnp.sum(jnp.where(keep, v, 0.0), axis=0, keepdims=True)
            return [v[:, 128 * p : 128 * p + 128] for p in range(packed)]

        def by_device(name, dst):
            for p in range(packed):
                v = R[name][p].reshape(plane * line, 128)
                R[dst][128 * p : 128 * p + 128, :] = v.T

        lv0, lv1, lv2 = levels
        inside = jnp.zeros((B, 128 - B), F32)

        def take(raw, dst):
            def one(x, c):
                v = jnp.concatenate([R[raw][x], inside], axis=1)
                R[dst][start_of(lv0) + x, lv0.first : lv0.first + B, :] = v
                return c

            loop(B, one, 0, 4)

        R["l3"][...] = jnp.zeros((n3, 8, 128), F32)
        inputs[0].wait()
        take("sgr", "sg")
        y_pack("sg")
        z_pack("sg")
        inputs[1].wait()
        take("rer", "s0")
        y_pack("s0")
        z_pack("s0")
        restrict(lv0, coefficient(lv0), "s")
        y_pack("s1")
        z_pack("s1")
        restrict(lv1, coefficient(lv1), "s")
        y_pack("s2")
        z_pack("s2")
        restrict(lv2, coefficient(lv2), "s")
        vector3 = local_vector()
        inputs[2].wait()
        take("rsr", "f0")
        pl.semaphore_wait(barrier, len(others))
        send("sg")
        for k in range(SPLIT):
            send(f"s{k}")
        gather_start("gs", vector3)
        arrive("sg")
        sent("sg")
        y_unpack("sg")

        def keep_guess(i, v):
            R["sg"][i, 8 : 8 + lv0.rows, :] = v

        z_unpacked("sg", keep_guess)

        def first_residual(x, carry):
            a = start_of(lv0) + x
            c, v = beside_of(lv0, R["sg"], a)
            s = R["s0"][a, 8 : 8 + lv0.rows, :]
            f = R["f0"][a, 8 : 8 + lv0.rows, :] - ((6.0 + s) * c - v)
            R["f0"][a, 8 : 8 + lv0.rows, :] = jnp.where(R["own"][...] > 0.0, f, 0.0)
            return carry

        loop(B, first_residual, 0, lv0.unroll)
        pack_send("f0")
        for lv in levels:
            arrive(f"s{lv.k}")
            y_unpack(f"s{lv.k}")
            weigh(lv)
        arrive("f0")
        y_unpack("f0")
        begin(lv0)

        def first_relax(lv):
            k = lv.k
            count, a0 = span(lv, 4)

            def one(i, carry):
                a = a0 + i
                c, v = beside_of(lv, R[f"e{k}"], a)
                w = R[f"w{k}"][a, 8 : 8 + lv.rows, :]
                R[f"a{k}"][a, 8 : 8 + lv.rows, :] = c * (1.0 + KEEP) + w * v
                return carry

            loop(count, one, 0, lv.unroll)

        first_relax(lv0)
        restrict(lv0, left_of(lv0, "a"), "f")

        def deeper(lv):
            name = f"f{lv.k}"
            pack_send(name)
            arrive(name)
            y_unpack(name)
            begin(lv)
            first_relax(lv)
            restrict(lv, left_of(lv, "a"), "f")

        deeper(lv1)
        deeper(lv2)
        gather_start("gf", local_vector())

        gather_end("gs")
        by_device("gs", "s3")
        lane8, row8 = iota((8, 128), 1), iota((8, 128), 0)
        dev_y, dev_x, dev_z = lane8 & (ny - 1), (lane8 >> 2) & 1, lane8 >> 3
        step_x, step_z = ny, plane
        has = {
            ("y", 1): dev_y < ny - 1, ("y", -1): dev_y > 0, ("x", 1): dev_x < nx - 1, ("x", -1): dev_x > 0,
            ("z", 1): dev_z < nz - 1, ("z", -1): dev_z > 0,
        }
        strides = {"y": 1, "x": step_x, "z": step_z}

        def across(v, axis, way):
            return jnp.where(has[axis, way], roll(v, -way * strides[axis]), 0.0)

        def around(get, m):
            def one(x, y):
                c = get(x, y)
                r = n3 // m
                up = jnp.where(row8 >= n3 - r, roll(across(c, "z", 1), n3 - r, 0), roll(c, -r, 0))
                dn = jnp.where(row8 < r, roll(across(c, "z", -1), r - n3, 0), roll(c, r, 0))
                v = up + dn
                v = v + (get(x + 1, y) if x + 1 < m else across(get(0, y), "x", 1))
                v = v + (get(x - 1, y) if x else across(get(m - 1, y), "x", -1))
                v = v + (get(x, y + 1) if y + 1 < m else across(get(x, 0), "y", 1))
                v = v + (get(x, y - 1) if y else across(get(x, m - 1), "y", -1))
                return c, v

            return one

        cells = [(x, y) for x in range(n3) for y in range(n3)]
        m4 = n3 // 2
        cells4 = [(x, y) for x in range(m4) for y in range(m4)]
        live = row8 < n3

        def tile(name, x, y):
            g = (x * n3 + y) * (n3 if name in ("s3", "f3") else 8)
            return R[name][g : g + 8, :]

        for x, y in cells:
            R["w3"][8 * (x * n3 + y) : 8 * (x * n3 + y) + 8, :] = jnp.where(
                live, (DAMPING * q3) / (6.0 * q3 + tile("s3", x, y)), 0.0)

        def coarser(get):
            out = {}
            for x, y in cells4:
                v = (get(2 * x, 2 * y) + get(2 * x, 2 * y + 1)) + (get(2 * x + 1, 2 * y) + get(2 * x + 1, 2 * y + 1))
                v = v + jnp.where((row8 & 1) == 0, roll(v, -1, 0), roll(v, 1, 0))
                out[x, y] = jnp.where(live, 0.125 * v, 0.0)
            return out

        s4 = coarser(lambda x, y: tile("s3", x, y))
        gather_end("gf")
        by_device("gf", "f3")
        e = {}
        e0 = {}
        for c in cells:
            e0[c] = (tile("w3", *c) * (1.0 / q3)) * tile("f3", *c)
        op = around(lambda x, y: e0[x, y], n3)
        for c in cells:
            u, v = op(*c)
            e[c] = u * (1.0 + KEEP) + tile("w3", *c) * v
        op = around(lambda x, y: e[x, y], n3)
        rest = {}
        for c in cells:
            u, v = op(*c)
            rest[c] = jnp.where(live, tile("f3", *c) - ((6.0 * q3 + tile("s3", *c)) * u - q3 * v), 0.0)
        f4 = coarser(lambda x, y: rest[x, y])

        def inner(u, v):
            s = None
            for c in cells4:
                s = u[c] * v[c] if s is None else s + u[c] * v[c]
            return total(s)

        r4 = dict(f4)
        p4 = dict(f4)
        e4 = {c: jnp.zeros((8, 128), F32) for c in cells4}
        rr = inner(r4, r4)
        for _ in range(BOTTOM_ITERS):
            op = around(lambda x, y: p4[x, y], m4)
            q = {}
            for c in cells4:
                u, v = op(*c)
                q[c] = jnp.where(live, (6.0 * q4 + s4[c]) * u - q4 * v, 0.0)
            a = rr / inner(p4, q)
            e4 = {c: e4[c] + a * p4[c] for c in cells4}
            r4 = {c: r4[c] - a * q[c] for c in cells4}
            new = inner(r4, r4)
            ratio = new / rr
            p4 = {c: r4[c] + ratio * p4[c] for c in cells4}
            rr = new
        e = {(x, y): e[x, y] + e4[x // 2, y // 2] for x, y in cells}
        for _ in range(2):
            op = around(lambda x, y: e[x, y], n3)
            nxt = {}
            for c in cells:
                u, v = op(*c)
                nxt[c] = u * KEEP + (e0[c] + tile("w3", *c) * v)
            e = nxt
        for x, y in cells:
            g = x * n3 + y
            R["e3"][8 * g : 8 * g + 8, :] = e[x, y]
        R["e3"][groups * 8 :, :] = jnp.zeros((planes * 128 - groups * 8, 128), F32)
        for p in range(planes):
            R["x3"][p] = R["e3"][128 * p : 128 * p + 128, :].T

        wide = planes * 128
        slabs3 = n3 + 2
        lane_w = iota((8, wide), 1) >> 3
        row_w = iota((8, wide), 0)
        lo_rows = jnp.where(row_w < 2, n3 - 2 + row_w, -1000)
        mid_rows = jnp.where(row_w < 2, -1000, row_w - 2)
        hi_rows = jnp.where(row_w < 2, row_w, -1000)
        y_below, y_above = jnp.maximum(gy - 1, 0), jnp.minimum(gy + 1, ny - 1)
        z_at = [jnp.maximum(gz - 1, 0), gz, jnp.minimum(gz + 1, nz - 1)]

        def vector(dev):
            return jnp.concatenate([R["x3"][p, pl.ds(dev, 1), :] for p in range(planes)], axis=1)

        for i in range(slabs3):
            partner = jnp.where(gx == 0, i >= n3, i < 2)
            px = jnp.where(partner, 1 - gx, gx)
            xx = jnp.where(gx == 0, i - jnp.where(i >= n3, n3, 0), i - 2 + jnp.where(i < 2, n3, 0))
            lo, mid, hi = (lane_w == xx * n3 + rows for rows in (lo_rows, mid_rows, hi_rows))
            for d in range(3):
                at_y = lambda g: vector(z_at[d] * plane + px * ny + g)
                first = jnp.where(mid, at_y(gy), jnp.where(lo, at_y(y_below), 0.0))
                second = jnp.where(hi, at_y(y_above), 0.0)
                R["lhs"][d, 16 * i : 16 * i + 8, :] = first
                R["lhs"][d, 16 * i + 8 : 16 * i + 16, :] = second
        l, c = iota((wide, 128), 1), iota((wide, 128), 0)
        table = jnp.where((l < B) & ((c & 7) == (l >> SPLIT)) & (c < groups * 8), 1.0, 0.0).astype(BF16)
        v = picked(R["lhs"][...].reshape(3 * slabs3 * 16, wide), table).reshape(3, slabs3, 16, 128)
        v = v[1] + roll(v[2].reshape(slabs3 * 16, 128), B).reshape(slabs3, 16, 128) + roll(
            v[0].reshape(slabs3 * 16, 128), -B).reshape(slabs3, 16, 128)
        u = R["u2"]
        shift = lv2.h - 4
        for i in range(slabs3):
            m = n3 + 4
            u[i, pl.ds(shift, m, stride=2), :] = v[i, 0:m]
            u[i, pl.ds(shift + 1, m, stride=2), :] = v[i, 0:m]

        add_up(lv2)
        relax(lv2, "b", "a", 4)
        relax(lv2, "a", "b", 2)

        def coarse_of(nxt, ref):
            a0 = 1 + gx * (nxt.h - 2)
            return lambda j, m: R[ref][a0 + j, nxt.first - 2 : nxt.first - 2 + m, :]

        prolong(lv1, coarse_of(lv2, "b2"))
        add_up(lv1)
        relax(lv1, "b", "a", 4)
        relax(lv1, "a", "b", 2)
        prolong(lv0, coarse_of(lv1, "b1"))
        add_up(lv0)
        relax(lv0, "b", "a", 4)
        relax(lv0, "a", "b", 2)

        def image(x, sums):
            upper, lower = sums
            a = start_of(lv0) + x
            c, v = beside_of(lv0, R["b0"], a)
            s = R["s0"][a, 8 : 8 + lv0.rows, :]
            ap = (6.0 + s) * c - v
            R["ap"][x] = ap
            c = jnp.where(R["own"][...] > 0.0, c, 0.0)
            return upper + R["f0"][a, 8 : 8 + lv0.rows, :] * c, lower + ap * c

        zero = jnp.zeros((lv0.rows, 128), F32)
        upper, lower = loop(B, image, (zero, zero), lv0.unroll)
        upper, lower = (jnp.sum(v, axis=0, keepdims=True) for v in (upper, lower))
        half = iota((1, 128), 1) < 64
        gather_start("gr", [jnp.where(half, upper, roll(lower, 64))])
        gather_end("gr")
        v = jnp.sum(R["gr"][0], axis=0)
        half = iota((8, 128), 1) < 64
        sums = [total(jnp.where(half, v, 0.0)), total(jnp.where(half, 0.0, v))]
        step_length = sums[0] / sums[1]

        def finish(x, c):
            a = start_of(lv0) + x
            p = R["b0"][a, lv0.first : lv0.first + B, :]
            f = R["f0"][a, lv0.first : lv0.first + B, :]
            q = R["ap"][x, lv0.h : lv0.h + B, :]
            sol_ref[x] = R["sgr"][x] + (step_length * p)[:, 0:B]
            res_ref[x] = (f - step_length * q)[:, 0:B]
            return c

        loop(B, finish, 0, 4)
        for name in exchanges:
            if name != "sg":
                sent(name)
        for name in ("gs", "gf", "gr"):
            gather_sent(name)

    return kernel, list(scratch.values())


def solution(mesh):
    sizes = tuple(mesh.shape[a] for a in AXES)

    def body(right_side, start_guess, reaction):
        kernel, scratch = make_kernel(sizes, right_side.shape)
        out = jax.ShapeDtypeStruct(right_side.shape, F32)
        return tuple(
            pl.pallas_call(
                kernel,
                out_shape=(out, out),
                in_specs=[pl.BlockSpec(memory_space=pl.ANY)] * 3,
                out_specs=(pl.BlockSpec(memory_space=pltpu.VMEM),) * 2,
                scratch_shapes=scratch,
                compiler_params=pltpu.CompilerParams(
                    collective_id=0, has_side_effects=True, vmem_limit_bytes=60 * 2**20
                ),
                name="cg_step",
            )(right_side, start_guess, reaction)
        )

    placed = P(*AXES)
    return jax.shard_map(
        body, mesh=mesh, in_specs=(placed,) * 3, out_specs=(placed,) * 2, check_vma=False
    )
```

```python
import jax
import jax.numpy as jnp
from jax import lax
from jax.experimental import pallas as pl
from jax.experimental.pallas import tpu as pltpu
from jax.sharding import PartitionSpec as P

BOTTOM_ITERS = 6
AXES = ("gx", "gy", "gz")
MESH = pl.DeviceIdType.MESH
F32 = jnp.float32
BF16 = jnp.bfloat16
DAMPING = 6.0 / 7.0
KEEP = 1.0 / 7.0
SPLIT = 3
HALO = (4, 5, 5)


def loop(n, f, carry=0, unroll=4):
    unroll = min(unroll, n)
    while n % unroll:
        unroll -= 1

    def step(i, c):
        for k in range(unroll):
            c = f(i * unroll + k, c)
        return c

    return lax.fori_loop(0, n // unroll, step, carry)


def iota(shape, axis):
    return lax.broadcasted_iota(jnp.int32, shape, axis)


def roll(v, shift, axis=1):
    shift = shift % v.shape[axis] if isinstance(shift, int) else shift
    return v if isinstance(shift, int) and shift == 0 else pltpu.roll(v, shift, axis)


def halves(v):
    high = v.astype(BF16)
    low = (v - high.astype(F32)).astype(BF16)
    return high, low


def picked(v, table):
    high, low = halves(v)
    return jnp.dot(high, table, preferred_element_type=F32) + jnp.dot(low, table, preferred_element_type=F32)


def total(v):
    v = jnp.sum(v, axis=0, keepdims=True)
    return jnp.sum(v, axis=1, keepdims=True)


class Level:
    def __init__(self, k, block):
        self.k = k
        self.n = block >> k
        self.h = HALO[k]
        self.r = 1 << k
        self.q = 0.25**k
        self.tiles = -(-(self.n + 2 * self.h) // 8)
        self.rows = 8 * self.tiles
        self.slabs = self.n + self.h
        self.first = 8 + self.h
        self.unroll = 14 if k == 0 else 28
        self.shape = (self.slabs + 2, self.rows + 16, 128)


def make_kernel(sizes, block):
    nx, ny, nz = sizes
    B = block[0]
    levels = [Level(k, B) for k in range(SPLIT)]
    n3 = B >> SPLIT
    groups = n3 * n3
    planes = -(-groups * 8 // 128)
    packed = -(-groups * n3 // 128)
    q3, q4 = 0.25**3, 0.25**4
    line = nz
    plane = nx * ny

    scratch = {}
    for name in ("rsr", "sgr", "rer"):
        scratch[name] = pltpu.VMEM((B, B, B), F32)
    scratch["insem"] = pltpu.SemaphoreType.DMA((3,))
    exchanges = {}

    def add_exchange(name, k, field, t, wide):
        lv = levels[k]
        per = 128 // (t * lv.r)
        ex = dict(lv=lv, field=field, t=t, wide=wide, per=per, pairs=lv.n // 2, groups=-(-lv.n // per))
        for d in ("s", "r"):
            scratch[f"y{d}_{name}"] = pltpu.VMEM((2, ex["pairs"], t, 128), F32)
            scratch[f"z{d}_{name}"] = pltpu.VMEM((2, ex["groups"], lv.rows, 128), F32)
        if wide:
            scratch[f"yx_{name}"] = pltpu.VMEM((2, t, t, 128), F32)
            scratch[f"zx_{name}"] = pltpu.VMEM((2, lv.rows, 128), F32)
        scratch[f"send_{name}"] = pltpu.SemaphoreType.DMA
        scratch[f"recv_{name}"] = pltpu.SemaphoreType.DMA
        exchanges[name] = ex

    for lv in levels:
        k = lv.k
        for name in ("f", "s", "w", "e", "a", "b"):
            scratch[f"{name}{k}"] = pltpu.VMEM(lv.shape, F32)
        scratch[f"vm{k}"] = pltpu.VMEM((lv.rows, 128), F32)
        scratch[f"t{k}"] = pltpu.VMEM((lv.n // 2, lv.rows, 128), F32)
        scratch[f"u{k}"] = pltpu.VMEM((lv.slabs // 2 + 1, lv.rows + 16, 128), F32)
        add_exchange(f"f{k}", k, f"f{k}", lv.h, True)
        add_exchange(f"s{k}", k, f"s{k}", lv.h, True)
    scratch["sg"] = pltpu.VMEM(levels[0].shape, F32)
    add_exchange("sg", 0, "sg", 1, False)
    scratch["ap"] = pltpu.VMEM((B, levels[0].rows, 128), F32)
    scratch["own"] = pltpu.VMEM((levels[0].rows, 128), F32)
    for name, count in (("gs", packed), ("gf", packed), ("gr", 1)):
        scratch[name] = pltpu.VMEM((count, line, plane, 128), F32)
        scratch[f"{name}_send"] = pltpu.SemaphoreType.DMA
        scratch[f"{name}_recv"] = pltpu.SemaphoreType.DMA
    scratch["count"] = pltpu.VMEM((1024, 128), F32)
    for name in ("k2", "k3", "k4", "k5"):
        scratch[name] = pltpu.SemaphoreType.REGULAR
    scratch["l3"] = pltpu.VMEM((n3, 8, 128), F32)
    for name in ("s3", "f3", "w3", "e3"):
        scratch[name] = pltpu.VMEM((planes * 128, 128), F32)
    scratch["x3"] = pltpu.VMEM((planes, plane * line, 128), F32)
    scratch["lhs"] = pltpu.VMEM((3, (n3 + 2) * 16, planes * 128), F32)

    names = list(scratch)

    def kernel(rs_ref, sg_ref, re_ref, sol_ref, res_ref, *refs):
        R = dict(zip(names, refs))
        gx, gy, gz = (lax.axis_index(a) for a in AXES)
        mine = gx * ny + gy

        inputs = [
            pltpu.make_async_copy(src, R[dst], R["insem"].at[i])
            for i, (src, dst) in enumerate(((sg_ref, "sgr"), (re_ref, "rer"), (rs_ref, "rsr")))
        ]
        for copy in inputs:
            copy.start()

        def start_of(lv):
            return 1 + gx * lv.h

        for lv in levels:
            k = lv.k

            def blank(a, c, k=k, lv=lv):
                for name in ("f", "s"):
                    ref = R[f"{name}{k}"]
                    ref[a, 8:16, :] = jnp.zeros((8, 128), F32)
                    low = (lv.first + lv.n) // 8 * 8
                    ref[a, low : 8 + lv.rows, :] = jnp.zeros((8 + lv.rows - low, 128), F32)
                if k == 0:
                    ref = R["sg"]
                    ref[a, 8:16, :] = jnp.zeros((8, 128), F32)
                    ref[a, low : 8 + lv.rows, :] = jnp.zeros((8 + lv.rows - low, 128), F32)
                return c

            loop(lv.shape[0], blank, 0, 2)

        for name, ex in exchanges.items():
            for m in ("yr", "yx", "zr", "zx") if ex["wide"] else ("yr", "zr"):
                ref = R[f"{m}_{name}"]
                ref[...] = jnp.zeros(ref.shape, F32)

        barrier = pltpu.get_barrier_semaphore()
        others = []
        for dz in range(nz):
            for dx in range(nx):
                for dy in range(ny):
                    if dx or dy or dz:
                        others.append((dx, dy, dz))

        def hops(to):
            dx, dy, dz = to
            return dx + min(dy, ny - dy) + min(dz % 4, 4 - dz % 4) + min(dz // 4, nz // 4 - dz // 4)

        others.sort(key=lambda to: (-hops(to), to))

        def device(dx, dy, dz):
            return {"gx": lax.rem(gx + dx, nx), "gy": lax.rem(gy + dy, ny), "gz": lax.rem(gz + dz, nz)}

        faces = [(1, 0, 0), (0, 1, 0), (0, ny - 1, 0), (0, 0, 1), (0, 0, nz - 1)]
        two = nz // 8
        waves = {
            "k2": faces,
            "k3": faces[:3] + [(0, 0, two), (0, 0, nz - two)],
            "k4": [(0, 0, 2 * two), (0, 0, nz - 2 * two)],
            "k5": [to for to in others if to[2] == 0],
        }

        def greet(name):
            for to in waves[name]:
                pl.semaphore_signal(R[name], inc=1, device_id=device(*to), device_id_type=MESH)

        def greeted(name):
            pl.semaphore_wait(R[name], len(waves[name]))

        for to in faces:
            pl.semaphore_signal(barrier, inc=1, device_id=device(*to), device_id_type=MESH)

        for lv in levels:
            k = lv.k
            z8 = jnp.zeros((8, 128), F32)
            zs = jnp.zeros((lv.rows, 128), F32)
            fields = ["e", "a", "b"] + (["sg"] if k == 0 else [])
            fields = [R[f if f == "sg" else f"{f}{k}"] for f in fields]

            def guard(a, c, fields=fields, lv=lv, z8=z8):
                for ref in fields:
                    ref[a, 0:8, :] = z8
                    ref[a, 8 + lv.rows : 16 + lv.rows, :] = z8
                return c

            loop(lv.shape[0], guard, 0, 2)
            for ref in fields:
                ref[0, 8 : 8 + lv.rows, :] = zs
                ref[lv.slabs + 1, 8 : 8 + lv.rows, :] = zs

            lane, row = iota((lv.rows, 128), 1), iota((lv.rows, 128), 0)
            wd = lv.h * lv.r
            ok = (lane < B) | ((lane < B + wd) & (gz < nz - 1)) | ((lane >= 128 - wd) & (gz > 0))
            ok = ok & (row >= jnp.where(gy > 0, 0, lv.h))
            ok = ok & (row < lv.n + lv.h + jnp.where(gy < ny - 1, lv.h, 0))
            R[f"vm{k}"][...] = jnp.where(ok, 1.0, 0.0)
            if k == 0:
                own = (lane < B) & (row >= lv.h) & (row < lv.h + lv.n)
                R["own"][...] = jnp.where(own, 1.0, 0.0)

        def messages(name):
            ex = exchanges[name]
            lv, t, m = ex["lv"], ex["t"], ex["pairs"]
            f = R[ex["field"]]
            src = jnp.where(gx == 0, 1 + lv.n - t, 1 + lv.h)
            dst = jnp.where(gx == 0, 1 + lv.h - t, 1 + lv.n)
            rows = pl.ds(lv.first, lv.n)
            own = pl.ds(lv.h, lv.n)
            ys, yr, zs, zr = (R[f"{c}_{name}"] for c in ("ys", "yr", "zs", "zr"))
            out = [(f.at[pl.ds(src, t), rows, :], f.at[pl.ds(dst, t), rows, :], 1, 0, 0)]
            for i, way in enumerate((-1, 1)):
                out.append((ys.at[i], yr.at[1 - i], 0, way, 0))
                out.append((zs.at[i, :, own, :], zr.at[1 - i, :, own, :], 0, 0, way))
            if ex["wide"]:
                yx, zx = R[f"yx_{name}"], R[f"zx_{name}"]
                pair = jnp.where(gx == 0, m - t, 0)
                group = jnp.where(gx == 0, ex["groups"] - 1, 0)
                for i, way in enumerate((-1, 1)):
                    out.append((ys.at[i, pl.ds(pair, t)], yx.at[1 - i], 1, way, 0))
                    out.append((zs.at[i, group, own, :], zx.at[1 - i, own, :], 1, 0, way))
                    for yway in (-1, 1):
                        here = pl.ds(lv.h if yway < 0 else lv.h + lv.n - t, t)
                        there = pl.ds(lv.h + lv.n if yway < 0 else lv.h - t, t)
                        out.append((zs.at[i, :, here, :], zr.at[1 - i, :, there, :], 0, yway, way))
                        out.append((zs.at[i, group, here, :], zx.at[1 - i, there, :], 1, yway, way))
            return out

        def guarded(cond, f):
            if cond is None:
                f()
            else:
                pl.when(cond)(f)

        def send(name):
            for src, dst, ox, oy, oz in messages(name):
                copy = pltpu.make_async_remote_copy(
                    src_ref=src, dst_ref=dst, send_sem=R[f"send_{name}"], recv_sem=R[f"recv_{name}"],
                    device_id=device(ox, oy % ny, oz % nz), device_id_type=MESH)
                cond = None
                for at, n, way in ((gy, ny, oy), (gz, nz, oz)):
                    if way:
                        there = at > 0 if way < 0 else at < n - 1
                        cond = there if cond is None else cond & there
                guarded(cond, copy.start)

        def counted(size, send_sem, recv_sem):
            rows = R["count"].at[pl.ds(0, size), :]
            return pltpu.make_async_remote_copy(
                src_ref=rows, dst_ref=rows, send_sem=send_sem, recv_sem=recv_sem,
                device_id=device(1, 0, 0), device_id_type=MESH)

        def in_all(name, getting):
            sizes = [(src.shape, oy, oz) for src, _, _, oy, oz in messages(name)]
            for y, at_y in ((0, gy == 0), (1, (gy > 0) & (gy < ny - 1)), (2, gy == ny - 1)):
                for z, at_z in ((0, gz == 0), (1, (gz > 0) & (gz < nz - 1)), (2, gz == nz - 1)):
                    rows = 0
                    for shape, oy, oz in sizes:
                        oy, oz = (-oy, -oz) if getting else (oy, oz)
                        if y + oy in (0, 1, 2) and z + oz in (0, 1, 2):
                            count = 1
                            for d in shape[:-1]:
                                count *= d
                            rows += count
                    copy = counted(rows, R[f"send_{name}"], R[f"recv_{name}"])
                    pl.when(at_y & at_z)(copy.wait_recv if getting else copy.wait_send)

        def arrive(name):
            in_all(name, True)

        def sent(name):
            in_all(name, False)

        def y_pack(name):
            ex = exchanges[name]
            lv, t, m = ex["lv"], ex["t"], ex["pairs"]
            f, a = R[ex["field"]], start_of(lv)
            lane = iota((t, 128), 1)
            for side, row in ((0, lv.first), (1, lv.first + lv.n - t)):
                for i in range(m):
                    v = f[a + i, row : row + t, :]
                    R[f"ys_{name}"][side, i] = jnp.where(lane < 64, v, roll(f[a + i + m, row : row + t, :], 64))

        def y_unpack(name):
            ex = exchanges[name]
            lv, t, m = ex["lv"], ex["t"], ex["pairs"]
            f, a = R[ex["field"]], start_of(lv)
            keep = iota((t, 128), 1) < B
            edge = jnp.where(gx == 0, 1 + lv.n, 1)
            for side, row, ok in ((0, lv.first - t, gy > 0), (1, lv.first + lv.n, gy < ny - 1)):
                for i in range(m):
                    v = R[f"yr_{name}"][side, i]
                    v = v if ex["wide"] else jnp.where(ok, v, 0.0)
                    f[a + i, row : row + t, :] = jnp.where(keep, v, 0.0)
                    f[a + i + m, row : row + t, :] = jnp.where(keep, roll(v, 64), 0.0)
                if ex["wide"]:
                    for i in range(t):
                        v = pltpu.roll(R[f"yx_{name}"][side, i], gx * 64, 1)
                        f[edge + i, row : row + t, :] = jnp.where(keep, v, 0.0)

        def z_pack(name):
            ex = exchanges[name]
            lv, per = ex["lv"], ex["per"]
            wd = ex["t"] * lv.r
            f, a = R[ex["field"]], start_of(lv)
            lane = iota((lv.rows, 128), 1)
            for g in range(ex["groups"]):
                low = high = None
                count = min(per, lv.n - g * per)
                for j in reversed(range(count)):
                    v = f[a + g * per + j, 8 : 8 + lv.rows, :]
                    c = j * wd
                    one, two = roll(v, c), roll(v, c - (B - wd))
                    low = one if low is None else jnp.where(lane < c + wd, one, low)
                    high = two if high is None else jnp.where(lane < c + wd, two, high)
                R[f"zs_{name}"][0, g] = low
                R[f"zs_{name}"][1, g] = high

        def pack_send(name):
            y_pack(name)
            z_pack(name)
            send(name)

        def z_unpacked(name, use):
            ex = exchanges[name]
            lv, per, t = ex["lv"], ex["per"], ex["t"]
            wd = t * lv.r
            f, a = R[ex["field"]], start_of(lv)
            lane = iota((lv.rows, 128), 1)

            def put(i, below, above):
                if not ex["wide"]:
                    below, above = jnp.where(gz > 0, below, 0.0), jnp.where(gz < nz - 1, above, 0.0)
                v = jnp.where(lane < B + wd, above, jnp.where(lane >= 128 - wd, below, 0.0))
                use(i, jnp.where(lane < B, f[i, 8 : 8 + lv.rows, :], v))

            for j in range(lv.n):
                g, c = j // per, j % per * wd
                put(a + j, roll(R[f"zr_{name}"][0, g], -wd - c), roll(R[f"zr_{name}"][1, g], B - c))
            if ex["wide"]:
                edge = jnp.where(gx == 0, 1 + lv.n, 1)
                for j in range(t):
                    c0, c1 = j * wd, (lv.n - t + j - (ex["groups"] - 1) * per) * wd
                    one = jnp.where(gx == 0, (-wd - c0) % 128, (-wd - c1) % 128)
                    two = jnp.where(gx == 0, (B - c0) % 128, (B - c1) % 128)
                    put(edge + j, pltpu.roll(R[f"zx_{name}"][0], one, 1), pltpu.roll(R[f"zx_{name}"][1], two, 1))

        def beside_of(lv, ref, a):
            rows = lv.rows
            c = ref[a, 8 : 8 + rows, :]
            v = ref[a + 1, 8 : 8 + rows, :] + ref[a - 1, 8 : 8 + rows, :]
            v = v + (ref[a, 9 : 9 + rows, :] + ref[a, 7 : 7 + rows, :])
            return c, v + (roll(c, lv.r) + roll(c, -lv.r))

        def span(lv, far):
            return lv.n + far, 1 + gx * (lv.h - far)

        def relax(lv, src, dst, far):
            k = lv.k
            count, a0 = span(lv, far)

            def one(i, carry):
                a = a0 + i
                c, v = beside_of(lv, R[f"{src}{k}"], a)
                w = R[f"w{k}"][a, 8 : 8 + lv.rows, :]
                e = R[f"e{k}"][a, 8 : 8 + lv.rows, :]
                R[f"{dst}{k}"][a, 8 : 8 + lv.rows, :] = c * KEEP + (e + w * v)
                return carry

            loop(count, one, 0, lv.unroll)

        def weigh(lv):
            k = lv.k
            vm = R[f"vm{k}"]

            def use(i, s):
                R[f"w{k}"][i, 8 : 8 + lv.rows, :] = vm[...] * ((DAMPING * lv.q) / (6.0 * lv.q + s))

            z_unpacked(f"s{k}", use)

        def begin(lv):
            k = lv.k
            scale = 1.0 / lv.q

            def use(i, f):
                w = R[f"w{k}"][i, 8 : 8 + lv.rows, :]
                R[f"e{k}"][i, 8 : 8 + lv.rows, :] = (w * scale) * f if k else w * f

            z_unpacked(f"f{k}", use)

        def restrict(lv, of, name):
            k = lv.k
            a0 = start_of(lv)
            half = lv.n // 2
            lane = iota((lv.rows, 128), 1)
            t = R[f"t{k}"]

            def one(j, c):
                v = of(a0 + 2 * j) + of(a0 + 2 * j + 1)
                v = v + jnp.where((lane & lv.r) == 0, roll(v, -lv.r), roll(v, lv.r))
                t[j] = v
                return c

            loop(half, one, 0, lv.unroll // 2)
            wide = iota((half, 128), 1) < B

            def two(j, c):
                v = t[j, pl.ds(lv.h, half, stride=2), :] + t[j, pl.ds(lv.h + 1, half, stride=2), :]
                v = jnp.where(wide, 0.125 * v, 0.0)
                if k + 1 < SPLIT:
                    nxt = levels[k + 1]
                    R[f"{name}{k + 1}"][start_of(nxt) + j, nxt.first : nxt.first + half, :] = v
                else:
                    R["l3"][j, 0:half, :] = v
                return c

            loop(half, two, 0, 12)

        def left_of(lv, src):
            k = lv.k

            def f(a):
                c, v = beside_of(lv, R[f"{src}{k}"], a)
                s = R[f"s{k}"][a, 8 : 8 + lv.rows, :]
                return R[f"f{k}"][a, 8 : 8 + lv.rows, :] - ((6.0 * lv.q + s) * c - lv.q * v)

            return f

        def coefficient(lv):
            return lambda a: R[f"s{lv.k}"][a, 8 : 8 + lv.rows, :]

        def prolong(lv, coarse_rows):
            k = lv.k
            nxt_far = 2
            half = lv.n // 2
            m = half + 2 * nxt_far
            shift = lv.h - 2 * nxt_far
            u = R[f"u{k}"]

            def put(j, c):
                v = coarse_rows(j, m)
                u[j, pl.ds(shift, m, stride=2), :] = v
                u[j, pl.ds(shift + 1, m, stride=2), :] = v
                return c

            loop(half + nxt_far, put, 0, 7)

        def add_up(lv):
            k = lv.k
            a0 = 1 + gx * (lv.h - 4)

            def one(j, c):
                p = R[f"u{k}"][j, 0 : lv.rows, :]
                if k:
                    row = iota((lv.rows, 128), 0)
                    p = jnp.where((row >= lv.h - 4) & (row < lv.h + lv.n + 4), p, 0.0)
                if k == SPLIT - 1:
                    p = jnp.where(R[f"vm{k}"][...] > 0.0, p, 0.0)
                for d in range(2):
                    a = a0 + 2 * j + d
                    R[f"b{k}"][a, 8 : 8 + lv.rows, :] = R[f"a{k}"][a, 8 : 8 + lv.rows, :] + p
                return c

            loop((lv.n + 4) // 2, one, 0, 7)

        def gather_copy(name, dx, dy, dz):
            g = R[name]
            here = g.at[:, gz, pl.ds(mine, 1), :]
            return pltpu.make_async_remote_copy(
                src_ref=here, dst_ref=here, send_sem=R[f"{name}_send"], recv_sem=R[f"{name}_recv"],
                device_id=device(dx, dy, dz), device_id_type=MESH)

        def gather_start(name, rows):
            for p, v in enumerate(rows):
                R[name][p, gz, pl.ds(mine, 1), :] = v
            for to in others:
                gather_copy(name, *to).start()

        def gathered(name):
            size = len(others) * R[name].shape[0]
            return counted(size, R[f"{name}_send"], R[f"{name}_recv"])

        def gather_end(name):
            gathered(name).wait_recv()

        def gather_sent(name):
            gathered(name).wait_send()

        def local_vector():
            wide = packed * 128
            v = R["l3"][...].reshape(n3 * 8, 128)
            l, c = iota((128, wide), 0), iota((128, wide), 1)
            table = jnp.where((l == c % n3 * (1 << SPLIT)) & (c < groups * n3), 1.0, 0.0).astype(BF16)
            v = picked(v, table)
            row, c = iota((n3 * 8, wide), 0), iota((n3 * 8, wide), 1)
            keep = ((row & 7) < n3) & (c // n3 == (row >> 3) * n3 + (row & 7))
            v = jnp.sum(jnp.where(keep, v, 0.0), axis=0, keepdims=True)
            return [v[:, 128 * p : 128 * p + 128] for p in range(packed)]

        def by_device(name, dst):
            for p in range(packed):
                v = R[name][p].reshape(plane * line, 128)
                R[dst][128 * p : 128 * p + 128, :] = v.T

        lv0, lv1, lv2 = levels
        inside = jnp.zeros((B, 128 - B), F32)

        def take(raw, dst):
            def one(x, c):
                v = jnp.concatenate([R[raw][x], inside], axis=1)
                R[dst][start_of(lv0) + x, lv0.first : lv0.first + B, :] = v
                return c

            loop(B, one, 0, 4)

        R["l3"][...] = jnp.zeros((n3, 8, 128), F32)
        inputs[0].wait()
        take("sgr", "sg")
        y_pack("sg")
        z_pack("sg")
        inputs[1].wait()
        take("rer", "s0")
        y_pack("s0")
        z_pack("s0")
        pl.semaphore_wait(barrier, len(faces))
        send("sg")
        greet("k2")
        inputs[2].wait()
        take("rsr", "f0")
        restrict(lv0, coefficient(lv0), "s")
        greeted("k2")
        greet("k3")
        y_pack("s1")
        z_pack("s1")
        restrict(lv1, coefficient(lv1), "s")
        y_pack("s2")
        z_pack("s2")
        greeted("k3")
        greet("k4")
        for k in range(SPLIT):
            send(f"s{k}")
        restrict(lv2, coefficient(lv2), "s")
        vector3 = local_vector()
        arrive("sg")
        sent("sg")
        y_unpack("sg")

        def keep_guess(i, v):
            R["sg"][i, 8 : 8 + lv0.rows, :] = v

        z_unpacked("sg", keep_guess)

        def first_residual(x, carry):
            a = start_of(lv0) + x
            c, v = beside_of(lv0, R["sg"], a)
            s = R["s0"][a, 8 : 8 + lv0.rows, :]
            f = R["f0"][a, 8 : 8 + lv0.rows, :] - ((6.0 + s) * c - v)
            R["f0"][a, 8 : 8 + lv0.rows, :] = jnp.where(R["own"][...] > 0.0, f, 0.0)
            return carry

        loop(B, first_residual, 0, lv0.unroll)
        greeted("k4")
        greet("k5")
        pack_send("f0")
        greeted("k5")
        gather_start("gs", vector3)
        for lv in levels:
            arrive(f"s{lv.k}")
            y_unpack(f"s{lv.k}")
            weigh(lv)
        arrive("f0")
        y_unpack("f0")
        begin(lv0)

        def first_relax(lv):
            k = lv.k
            count, a0 = span(lv, 4)

            def one(i, carry):
                a = a0 + i
                c, v = beside_of(lv, R[f"e{k}"], a)
                w = R[f"w{k}"][a, 8 : 8 + lv.rows, :]
                R[f"a{k}"][a, 8 : 8 + lv.rows, :] = c * (1.0 + KEEP) + w * v
                return carry

            loop(count, one, 0, lv.unroll)

        first_relax(lv0)
        restrict(lv0, left_of(lv0, "a"), "f")

        def deeper(lv):
            name = f"f{lv.k}"
            pack_send(name)
            arrive(name)
            y_unpack(name)
            begin(lv)
            first_relax(lv)
            restrict(lv, left_of(lv, "a"), "f")

        deeper(lv1)
        deeper(lv2)
        gather_start("gf", local_vector())

        gather_end("gs")
        by_device("gs", "s3")
        lane8, row8 = iota((8, 128), 1), iota((8, 128), 0)
        dev_y, dev_x, dev_z = lane8 & (ny - 1), (lane8 >> 2) & 1, lane8 >> 3
        step_x, step_z = ny, plane
        has = {
            ("y", 1): dev_y < ny - 1, ("y", -1): dev_y > 0, ("x", 1): dev_x < nx - 1, ("x", -1): dev_x > 0,
            ("z", 1): dev_z < nz - 1, ("z", -1): dev_z > 0,
        }
        strides = {"y": 1, "x": step_x, "z": step_z}

        def across(v, axis, way):
            return jnp.where(has[axis, way], roll(v, -way * strides[axis]), 0.0)

        def around(get, m):
            def one(x, y):
                c = get(x, y)
                r = n3 // m
                up = jnp.where(row8 >= n3 - r, roll(across(c, "z", 1), n3 - r, 0), roll(c, -r, 0))
                dn = jnp.where(row8 < r, roll(across(c, "z", -1), r - n3, 0), roll(c, r, 0))
                v = up + dn
                v = v + (get(x + 1, y) if x + 1 < m else across(get(0, y), "x", 1))
                v = v + (get(x - 1, y) if x else across(get(m - 1, y), "x", -1))
                v = v + (get(x, y + 1) if y + 1 < m else across(get(x, 0), "y", 1))
                v = v + (get(x, y - 1) if y else across(get(x, m - 1), "y", -1))
                return c, v

            return one

        cells = [(x, y) for x in range(n3) for y in range(n3)]
        m4 = n3 // 2
        cells4 = [(x, y) for x in range(m4) for y in range(m4)]
        live = row8 < n3

        def tile(name, x, y):
            g = (x * n3 + y) * (n3 if name in ("s3", "f3") else 8)
            return R[name][g : g + 8, :]

        for x, y in cells:
            R["w3"][8 * (x * n3 + y) : 8 * (x * n3 + y) + 8, :] = jnp.where(
                live, (DAMPING * q3) / (6.0 * q3 + tile("s3", x, y)), 0.0)

        def coarser(get):
            out = {}
            for x, y in cells4:
                v = (get(2 * x, 2 * y) + get(2 * x, 2 * y + 1)) + (get(2 * x + 1, 2 * y) + get(2 * x + 1, 2 * y + 1))
                v = v + jnp.where((row8 & 1) == 0, roll(v, -1, 0), roll(v, 1, 0))
                out[x, y] = jnp.where(live, 0.125 * v, 0.0)
            return out

        s4 = coarser(lambda x, y: tile("s3", x, y))
        gather_end("gf")
        by_device("gf", "f3")
        e = {}
        e0 = {}
        for c in cells:
            e0[c] = (tile("w3", *c) * (1.0 / q3)) * tile("f3", *c)
        op = around(lambda x, y: e0[x, y], n3)
        for c in cells:
            u, v = op(*c)
            e[c] = u * (1.0 + KEEP) + tile("w3", *c) * v
        op = around(lambda x, y: e[x, y], n3)
        rest = {}
        for c in cells:
            u, v = op(*c)
            rest[c] = jnp.where(live, tile("f3", *c) - ((6.0 * q3 + tile("s3", *c)) * u - q3 * v), 0.0)
        f4 = coarser(lambda x, y: rest[x, y])

        def inner(u, v):
            s = None
            for c in cells4:
                s = u[c] * v[c] if s is None else s + u[c] * v[c]
            return total(s)

        r4 = dict(f4)
        p4 = dict(f4)
        e4 = {c: jnp.zeros((8, 128), F32) for c in cells4}
        rr = inner(r4, r4)
        for _ in range(BOTTOM_ITERS):
            op = around(lambda x, y: p4[x, y], m4)
            q = {}
            for c in cells4:
                u, v = op(*c)
                q[c] = jnp.where(live, (6.0 * q4 + s4[c]) * u - q4 * v, 0.0)
            a = rr / inner(p4, q)
            e4 = {c: e4[c] + a * p4[c] for c in cells4}
            r4 = {c: r4[c] - a * q[c] for c in cells4}
            new = inner(r4, r4)
            ratio = new / rr
            p4 = {c: r4[c] + ratio * p4[c] for c in cells4}
            rr = new
        e = {(x, y): e[x, y] + e4[x // 2, y // 2] for x, y in cells}
        for _ in range(2):
            op = around(lambda x, y: e[x, y], n3)
            nxt = {}
            for c in cells:
                u, v = op(*c)
                nxt[c] = u * KEEP + (e0[c] + tile("w3", *c) * v)
            e = nxt
        for x, y in cells:
            g = x * n3 + y
            R["e3"][8 * g : 8 * g + 8, :] = e[x, y]
        R["e3"][groups * 8 :, :] = jnp.zeros((planes * 128 - groups * 8, 128), F32)
        for p in range(planes):
            R["x3"][p] = R["e3"][128 * p : 128 * p + 128, :].T

        wide = planes * 128
        slabs3 = n3 + 2
        lane_w = iota((8, wide), 1) >> 3
        row_w = iota((8, wide), 0)
        lo_rows = jnp.where(row_w < 2, n3 - 2 + row_w, -1000)
        mid_rows = jnp.where(row_w < 2, -1000, row_w - 2)
        hi_rows = jnp.where(row_w < 2, row_w, -1000)
        y_below, y_above = jnp.maximum(gy - 1, 0), jnp.minimum(gy + 1, ny - 1)
        z_at = [jnp.maximum(gz - 1, 0), gz, jnp.minimum(gz + 1, nz - 1)]

        def vector(dev):
            return jnp.concatenate([R["x3"][p, pl.ds(dev, 1), :] for p in range(planes)], axis=1)

        for i in range(slabs3):
            partner = jnp.where(gx == 0, i >= n3, i < 2)
            px = jnp.where(partner, 1 - gx, gx)
            xx = jnp.where(gx == 0, i - jnp.where(i >= n3, n3, 0), i - 2 + jnp.where(i < 2, n3, 0))
            lo, mid, hi = (lane_w == xx * n3 + rows for rows in (lo_rows, mid_rows, hi_rows))
            for d in range(3):
                at_y = lambda g: vector(z_at[d] * plane + px * ny + g)
                first = jnp.where(mid, at_y(gy), jnp.where(lo, at_y(y_below), 0.0))
                second = jnp.where(hi, at_y(y_above), 0.0)
                R["lhs"][d, 16 * i : 16 * i + 8, :] = first
                R["lhs"][d, 16 * i + 8 : 16 * i + 16, :] = second
        l, c = iota((wide, 128), 1), iota((wide, 128), 0)
        table = jnp.where((l < B) & ((c & 7) == (l >> SPLIT)) & (c < groups * 8), 1.0, 0.0).astype(BF16)
        v = picked(R["lhs"][...].reshape(3 * slabs3 * 16, wide), table).reshape(3, slabs3, 16, 128)
        v = v[1] + roll(v[2].reshape(slabs3 * 16, 128), B).reshape(slabs3, 16, 128) + roll(
            v[0].reshape(slabs3 * 16, 128), -B).reshape(slabs3, 16, 128)
        u = R["u2"]
        shift = lv2.h - 4
        for i in range(slabs3):
            m = n3 + 4
            u[i, pl.ds(shift, m, stride=2), :] = v[i, 0:m]
            u[i, pl.ds(shift + 1, m, stride=2), :] = v[i, 0:m]

        add_up(lv2)
        relax(lv2, "b", "a", 4)
        relax(lv2, "a", "b", 2)

        def coarse_of(nxt, ref):
            a0 = 1 + gx * (nxt.h - 2)
            return lambda j, m: R[ref][a0 + j, nxt.first - 2 : nxt.first - 2 + m, :]

        prolong(lv1, coarse_of(lv2, "b2"))
        add_up(lv1)
        relax(lv1, "b", "a", 4)
        relax(lv1, "a", "b", 2)
        prolong(lv0, coarse_of(lv1, "b1"))
        add_up(lv0)
        relax(lv0, "b", "a", 4)
        relax(lv0, "a", "b", 2)

        def image(x, sums):
            upper, lower = sums
            a = start_of(lv0) + x
            c, v = beside_of(lv0, R["b0"], a)
            s = R["s0"][a, 8 : 8 + lv0.rows, :]
            ap = (6.0 + s) * c - v
            R["ap"][x] = ap
            c = jnp.where(R["own"][...] > 0.0, c, 0.0)
            return upper + R["f0"][a, 8 : 8 + lv0.rows, :] * c, lower + ap * c

        zero = jnp.zeros((lv0.rows, 128), F32)
        upper, lower = loop(B, image, (zero, zero), lv0.unroll)
        upper, lower = (jnp.sum(v, axis=0, keepdims=True) for v in (upper, lower))
        half = iota((1, 128), 1) < 64
        gather_start("gr", [jnp.where(half, upper, roll(lower, 64))])
        gather_end("gr")
        v = jnp.sum(R["gr"][0], axis=0)
        half = iota((8, 128), 1) < 64
        sums = [total(jnp.where(half, v, 0.0)), total(jnp.where(half, 0.0, v))]
        step_length = sums[0] / sums[1]

        def finish(x, c):
            a = start_of(lv0) + x
            p = R["b0"][a, lv0.first : lv0.first + B, :]
            f = R["f0"][a, lv0.first : lv0.first + B, :]
            q = R["ap"][x, lv0.h : lv0.h + B, :]
            sol_ref[x] = R["sgr"][x] + (step_length * p)[:, 0:B]
            res_ref[x] = (f - step_length * q)[:, 0:B]
            return c

        loop(B, finish, 0, 4)
        for name in exchanges:
            if name != "sg":
                sent(name)
        for name in ("gs", "gf", "gr"):
            gather_sent(name)

    return kernel, list(scratch.values())


def solution(mesh):
    sizes = tuple(mesh.shape[a] for a in AXES)

    def body(right_side, start_guess, reaction):
        kernel, scratch = make_kernel(sizes, right_side.shape)
        out = jax.ShapeDtypeStruct(right_side.shape, F32)
        return tuple(
            pl.pallas_call(
                kernel,
                out_shape=(out, out),
                in_specs=[pl.BlockSpec(memory_space=pl.ANY)] * 3,
                out_specs=(pl.BlockSpec(memory_space=pltpu.VMEM),) * 2,
                scratch_shapes=scratch,
                compiler_params=pltpu.CompilerParams(
                    collective_id=0, has_side_effects=True, vmem_limit_bytes=51 * 2**20
                ),
                name="cg_step",
            )(right_side, start_guess, reaction)
        )

    placed = P(*AXES)
    return jax.shard_map(
        body, mesh=mesh, in_specs=(placed,) * 3, out_specs=(placed,) * 2, check_vma=False
    )
```

```python
import jax
import jax.numpy as jnp
from jax import lax
from jax.experimental import pallas as pl
from jax.experimental.pallas import tpu as pltpu
from jax.sharding import PartitionSpec as P

BOTTOM_ITERS = 6
AXES = ("gx", "gy", "gz")
MESH = pl.DeviceIdType.MESH
F32 = jnp.float32
BF16 = jnp.bfloat16
DAMPING = 6.0 / 7.0
KEEP = 1.0 / 7.0
SPLIT = 3
HALO = (4, 5, 5)


def loop(n, f, carry=0, unroll=4):
    unroll = min(unroll, n)
    while n % unroll:
        unroll -= 1

    def step(i, c):
        for k in range(unroll):
            c = f(i * unroll + k, c)
        return c

    return lax.fori_loop(0, n // unroll, step, carry)


def iota(shape, axis):
    return lax.broadcasted_iota(jnp.int32, shape, axis)


def roll(v, shift, axis=1):
    shift = shift % v.shape[axis] if isinstance(shift, int) else shift
    return v if isinstance(shift, int) and shift == 0 else pltpu.roll(v, shift, axis)


def halves(v):
    high = v.astype(BF16)
    low = (v - high.astype(F32)).astype(BF16)
    return high, low


def picked(v, table):
    high, low = halves(v)
    return jnp.dot(high, table, preferred_element_type=F32) + jnp.dot(low, table, preferred_element_type=F32)


def total(v):
    v = jnp.sum(v, axis=0, keepdims=True)
    return jnp.sum(v, axis=1, keepdims=True)


class Level:
    def __init__(self, k, block):
        self.k = k
        self.n = block >> k
        self.h = HALO[k]
        self.r = 1 << k
        self.q = 0.25**k
        self.tiles = -(-(self.n + 2 * self.h) // 8)
        self.rows = 8 * self.tiles
        self.slabs = self.n + self.h
        self.first = 8 + self.h
        self.unroll = 26 if k == 0 else 28
        self.shape = (self.slabs + 2, self.rows + 16, 128)


def make_kernel(sizes, block):
    nx, ny, nz = sizes
    B = block[0]
    levels = [Level(k, B) for k in range(SPLIT)]
    n3 = B >> SPLIT
    groups = n3 * n3
    planes = -(-groups * 8 // 128)
    packed = -(-groups * n3 // 128)
    q3, q4 = 0.25**3, 0.25**4
    line = nz
    plane = nx * ny

    scratch = {}
    for name in ("rsr", "sgr", "rer"):
        scratch[name] = pltpu.VMEM((B, B, B), F32)
    scratch["insem"] = pltpu.SemaphoreType.DMA((3,))
    exchanges = {}

    def add_exchange(name, k, field, t, wide):
        lv = levels[k]
        per = 128 // (t * lv.r)
        ex = dict(lv=lv, field=field, t=t, wide=wide, per=per, pairs=lv.n // 2, groups=-(-lv.n // per))
        for d in ("s", "r"):
            scratch[f"y{d}_{name}"] = pltpu.VMEM((2, ex["pairs"], t, 128), F32)
            scratch[f"z{d}_{name}"] = pltpu.VMEM((2, ex["groups"], lv.rows, 128), F32)
        if wide:
            scratch[f"yx_{name}"] = pltpu.VMEM((2, t, t, 128), F32)
            scratch[f"zx_{name}"] = pltpu.VMEM((2, lv.rows, 128), F32)
        scratch[f"send_{name}"] = pltpu.SemaphoreType.DMA
        scratch[f"recv_{name}"] = pltpu.SemaphoreType.DMA
        exchanges[name] = ex

    for lv in levels:
        k = lv.k
        for name in ("f", "s", "w", "e", "a", "b"):
            scratch[f"{name}{k}"] = pltpu.VMEM(lv.shape, F32)
        scratch[f"vm{k}"] = pltpu.VMEM((lv.rows, 128), F32)
        scratch[f"t{k}"] = pltpu.VMEM((lv.n // 2, lv.rows, 128), F32)
        scratch[f"u{k}"] = pltpu.VMEM((lv.slabs // 2 + 1, lv.rows + 16, 128), F32)
        add_exchange(f"f{k}", k, f"f{k}", lv.h, True)
        add_exchange(f"s{k}", k, f"s{k}", lv.h, True)
    scratch["sg"] = pltpu.VMEM(levels[0].shape, F32)
    add_exchange("sg", 0, "sg", 1, False)
    scratch["ap"] = pltpu.VMEM((B, levels[0].rows, 128), F32)
    scratch["own"] = pltpu.VMEM((levels[0].rows, 128), F32)
    for name, count in (("gs", packed), ("gf", packed), ("gr", 1)):
        scratch[name] = pltpu.VMEM((count, line, plane, 128), F32)
        scratch[f"{name}_send"] = pltpu.SemaphoreType.DMA
        scratch[f"{name}_recv"] = pltpu.SemaphoreType.DMA
    scratch["count"] = pltpu.VMEM((1024, 128), F32)
    for name in ("k2", "k3", "k4", "k5"):
        scratch[name] = pltpu.SemaphoreType.REGULAR
    scratch["l3"] = pltpu.VMEM((n3, 8, 128), F32)
    for name in ("s3", "f3", "w3", "e3"):
        scratch[name] = pltpu.VMEM((planes * 128, 128), F32)
    scratch["x3"] = pltpu.VMEM((planes, plane * line, 128), F32)
    scratch["lhs"] = pltpu.VMEM((3, (n3 + 2) * 16, planes * 128), F32)

    names = list(scratch)

    def kernel(rs_ref, sg_ref, re_ref, sol_ref, res_ref, *refs):
        R = dict(zip(names, refs))
        gx, gy, gz = (lax.axis_index(a) for a in AXES)
        mine = gx * ny + gy

        inputs = [
            pltpu.make_async_copy(src, R[dst], R["insem"].at[i])
            for i, (src, dst) in enumerate(((sg_ref, "sgr"), (re_ref, "rer"), (rs_ref, "rsr")))
        ]
        for copy in inputs:
            copy.start()

        def start_of(lv):
            return 1 + gx * lv.h

        for lv in levels:
            k = lv.k

            def blank(a, c, k=k, lv=lv):
                for name in ("f", "s"):
                    ref = R[f"{name}{k}"]
                    ref[a, 8:16, :] = jnp.zeros((8, 128), F32)
                    low = (lv.first + lv.n) // 8 * 8
                    ref[a, low : 8 + lv.rows, :] = jnp.zeros((8 + lv.rows - low, 128), F32)
                if k == 0:
                    ref = R["sg"]
                    ref[a, 8:16, :] = jnp.zeros((8, 128), F32)
                    ref[a, low : 8 + lv.rows, :] = jnp.zeros((8 + lv.rows - low, 128), F32)
                return c

            loop(lv.shape[0], blank, 0, 2)

        for name, ex in exchanges.items():
            for m in ("yr", "yx", "zr", "zx") if ex["wide"] else ("yr", "zr"):
                ref = R[f"{m}_{name}"]
                ref[...] = jnp.zeros(ref.shape, F32)

        barrier = pltpu.get_barrier_semaphore()
        others = []
        for dz in range(nz):
            for dx in range(nx):
                for dy in range(ny):
                    if dx or dy or dz:
                        others.append((dx, dy, dz))

        def hops(to):
            dx, dy, dz = to
            return dx + min(dy, ny - dy) + min(dz % 4, 4 - dz % 4) + min(dz // 4, nz // 4 - dz // 4)

        others.sort(key=lambda to: (-hops(to), to))

        def device(dx, dy, dz):
            return {"gx": lax.rem(gx + dx, nx), "gy": lax.rem(gy + dy, ny), "gz": lax.rem(gz + dz, nz)}

        faces = [(1, 0, 0), (0, 1, 0), (0, ny - 1, 0), (0, 0, 1), (0, 0, nz - 1)]
        two = nz // 8
        waves = {
            "k2": faces,
            "k3": faces[:3] + [(0, 0, two), (0, 0, nz - two)],
            "k4": [(0, 0, 2 * two), (0, 0, nz - 2 * two)],
            "k5": [to for to in others if to[2] == 0],
        }

        def greet(name):
            for to in waves[name]:
                pl.semaphore_signal(R[name], inc=1, device_id=device(*to), device_id_type=MESH)

        def greeted(name):
            pl.semaphore_wait(R[name], len(waves[name]))

        for to in faces:
            pl.semaphore_signal(barrier, inc=1, device_id=device(*to), device_id_type=MESH)

        for lv in levels:
            k = lv.k
            z8 = jnp.zeros((8, 128), F32)
            zs = jnp.zeros((lv.rows, 128), F32)
            fields = ["e", "a", "b"] + (["sg"] if k == 0 else [])
            fields = [R[f if f == "sg" else f"{f}{k}"] for f in fields]

            def guard(a, c, fields=fields, lv=lv, z8=z8):
                for ref in fields:
                    ref[a, 0:8, :] = z8
                    ref[a, 8 + lv.rows : 16 + lv.rows, :] = z8
                return c

            loop(lv.shape[0], guard, 0, 2)
            for ref in fields:
                ref[0, 8 : 8 + lv.rows, :] = zs
                ref[lv.slabs + 1, 8 : 8 + lv.rows, :] = zs

            lane, row = iota((lv.rows, 128), 1), iota((lv.rows, 128), 0)
            wd = lv.h * lv.r
            ok = (lane < B) | ((lane < B + wd) & (gz < nz - 1)) | ((lane >= 128 - wd) & (gz > 0))
            ok = ok & (row >= jnp.where(gy > 0, 0, lv.h))
            ok = ok & (row < lv.n + lv.h + jnp.where(gy < ny - 1, lv.h, 0))
            R[f"vm{k}"][...] = jnp.where(ok, 1.0, 0.0)
            if k == 0:
                own = (lane < B) & (row >= lv.h) & (row < lv.h + lv.n)
                R["own"][...] = jnp.where(own, 1.0, 0.0)

        def messages(name):
            ex = exchanges[name]
            lv, t, m = ex["lv"], ex["t"], ex["pairs"]
            f = R[ex["field"]]
            src = jnp.where(gx == 0, 1 + lv.n - t, 1 + lv.h)
            dst = jnp.where(gx == 0, 1 + lv.h - t, 1 + lv.n)
            rows = pl.ds(lv.first, lv.n)
            own = pl.ds(lv.h, lv.n)
            ys, yr, zs, zr = (R[f"{c}_{name}"] for c in ("ys", "yr", "zs", "zr"))
            out = [(f.at[pl.ds(src, t), rows, :], f.at[pl.ds(dst, t), rows, :], 1, 0, 0)]
            for i, way in enumerate((-1, 1)):
                out.append((ys.at[i], yr.at[1 - i], 0, way, 0))
                out.append((zs.at[i, :, own, :], zr.at[1 - i, :, own, :], 0, 0, way))
            if ex["wide"]:
                yx, zx = R[f"yx_{name}"], R[f"zx_{name}"]
                pair = jnp.where(gx == 0, m - t, 0)
                group = jnp.where(gx == 0, ex["groups"] - 1, 0)
                for i, way in enumerate((-1, 1)):
                    out.append((ys.at[i, pl.ds(pair, t)], yx.at[1 - i], 1, way, 0))
                    out.append((zs.at[i, group, own, :], zx.at[1 - i, own, :], 1, 0, way))
                    for yway in (-1, 1):
                        here = pl.ds(lv.h if yway < 0 else lv.h + lv.n - t, t)
                        there = pl.ds(lv.h + lv.n if yway < 0 else lv.h - t, t)
                        out.append((zs.at[i, :, here, :], zr.at[1 - i, :, there, :], 0, yway, way))
                        out.append((zs.at[i, group, here, :], zx.at[1 - i, there, :], 1, yway, way))
            return out

        def guarded(cond, f):
            if cond is None:
                f()
            else:
                pl.when(cond)(f)

        def send(name, only=None):
            batch = [m for m in messages(name) if only is None or only(*m[2:])]
            batch.sort(key=lambda m: -(m[2] + abs(m[3]) + 2 * abs(m[4])))
            for src, dst, ox, oy, oz in batch:
                copy = pltpu.make_async_remote_copy(
                    src_ref=src, dst_ref=dst, send_sem=R[f"send_{name}"], recv_sem=R[f"recv_{name}"],
                    device_id=device(ox, oy % ny, oz % nz), device_id_type=MESH)
                cond = None
                for at, n, way in ((gy, ny, oy), (gz, nz, oz)):
                    if way:
                        there = at > 0 if way < 0 else at < n - 1
                        cond = there if cond is None else cond & there
                guarded(cond, copy.start)

        def counted(size, send_sem, recv_sem):
            rows = R["count"].at[pl.ds(0, size), :]
            return pltpu.make_async_remote_copy(
                src_ref=rows, dst_ref=rows, send_sem=send_sem, recv_sem=recv_sem,
                device_id=device(1, 0, 0), device_id_type=MESH)

        def in_all(name, getting):
            sizes = [(src.shape, oy, oz) for src, _, _, oy, oz in messages(name)]
            for y, at_y in ((0, gy == 0), (1, (gy > 0) & (gy < ny - 1)), (2, gy == ny - 1)):
                for z, at_z in ((0, gz == 0), (1, (gz > 0) & (gz < nz - 1)), (2, gz == nz - 1)):
                    rows = 0
                    for shape, oy, oz in sizes:
                        oy, oz = (-oy, -oz) if getting else (oy, oz)
                        if y + oy in (0, 1, 2) and z + oz in (0, 1, 2):
                            count = 1
                            for d in shape[:-1]:
                                count *= d
                            rows += count
                    copy = counted(rows, R[f"send_{name}"], R[f"recv_{name}"])
                    pl.when(at_y & at_z)(copy.wait_recv if getting else copy.wait_send)

        def arrive(name):
            in_all(name, True)

        def sent(name):
            in_all(name, False)

        def y_pack(name):
            ex = exchanges[name]
            lv, t, m = ex["lv"], ex["t"], ex["pairs"]
            f, a = R[ex["field"]], start_of(lv)
            lane = iota((t, 128), 1)
            for side, row in ((0, lv.first), (1, lv.first + lv.n - t)):
                for i in range(m):
                    v = f[a + i, row : row + t, :]
                    R[f"ys_{name}"][side, i] = jnp.where(lane < 64, v, roll(f[a + i + m, row : row + t, :], 64))

        def y_unpack(name):
            ex = exchanges[name]
            lv, t, m = ex["lv"], ex["t"], ex["pairs"]
            f, a = R[ex["field"]], start_of(lv)
            keep = iota((t, 128), 1) < B
            edge = jnp.where(gx == 0, 1 + lv.n, 1)
            for side, row, ok in ((0, lv.first - t, gy > 0), (1, lv.first + lv.n, gy < ny - 1)):
                for i in range(m):
                    v = R[f"yr_{name}"][side, i]
                    v = v if ex["wide"] else jnp.where(ok, v, 0.0)
                    f[a + i, row : row + t, :] = jnp.where(keep, v, 0.0)
                    f[a + i + m, row : row + t, :] = jnp.where(keep, roll(v, 64), 0.0)
                if ex["wide"]:
                    for i in range(t):
                        v = pltpu.roll(R[f"yx_{name}"][side, i], gx * 64, 1)
                        f[edge + i, row : row + t, :] = jnp.where(keep, v, 0.0)

        def z_pack(name):
            ex = exchanges[name]
            lv, per = ex["lv"], ex["per"]
            wd = ex["t"] * lv.r
            f, a = R[ex["field"]], start_of(lv)
            lane = iota((lv.rows, 128), 1)
            for g in range(ex["groups"]):
                low = high = None
                count = min(per, lv.n - g * per)
                for j in reversed(range(count)):
                    v = f[a + g * per + j, 8 : 8 + lv.rows, :]
                    c = j * wd
                    one, two = roll(v, c), roll(v, c - (B - wd))
                    low = one if low is None else jnp.where(lane < c + wd, one, low)
                    high = two if high is None else jnp.where(lane < c + wd, two, high)
                R[f"zs_{name}"][0, g] = low
                R[f"zs_{name}"][1, g] = high

        def pack_send(name):
            send(name, lambda ox, oy, oz: not oy and not oz)
            z_pack(name)
            send(name, lambda ox, oy, oz: oz)
            y_pack(name)
            send(name, lambda ox, oy, oz: oy and not oz)

        def z_unpacked(name, use):
            ex = exchanges[name]
            lv, per, t = ex["lv"], ex["per"], ex["t"]
            wd = t * lv.r
            f, a = R[ex["field"]], start_of(lv)
            lane = iota((lv.rows, 128), 1)

            def put(i, below, above):
                if not ex["wide"]:
                    below, above = jnp.where(gz > 0, below, 0.0), jnp.where(gz < nz - 1, above, 0.0)
                v = jnp.where(lane < B + wd, above, jnp.where(lane >= 128 - wd, below, 0.0))
                use(i, jnp.where(lane < B, f[i, 8 : 8 + lv.rows, :], v))

            for j in range(lv.n):
                g, c = j // per, j % per * wd
                put(a + j, roll(R[f"zr_{name}"][0, g], -wd - c), roll(R[f"zr_{name}"][1, g], B - c))
            if ex["wide"]:
                edge = jnp.where(gx == 0, 1 + lv.n, 1)
                for j in range(t):
                    c0, c1 = j * wd, (lv.n - t + j - (ex["groups"] - 1) * per) * wd
                    one = jnp.where(gx == 0, (-wd - c0) % 128, (-wd - c1) % 128)
                    two = jnp.where(gx == 0, (B - c0) % 128, (B - c1) % 128)
                    put(edge + j, pltpu.roll(R[f"zx_{name}"][0], one, 1), pltpu.roll(R[f"zx_{name}"][1], two, 1))

        def beside_of(lv, ref, a):
            rows = lv.rows
            c = ref[a, 8 : 8 + rows, :]
            v = ref[a + 1, 8 : 8 + rows, :] + ref[a - 1, 8 : 8 + rows, :]
            v = v + (ref[a, 9 : 9 + rows, :] + ref[a, 7 : 7 + rows, :])
            return c, v + (roll(c, lv.r) + roll(c, -lv.r))

        def span(lv, far):
            return lv.n + far, 1 + gx * (lv.h - far)

        def relax(lv, src, dst, far):
            k = lv.k
            count, a0 = span(lv, far)

            def one(i, carry):
                a = a0 + i
                c, v = beside_of(lv, R[f"{src}{k}"], a)
                w = R[f"w{k}"][a, 8 : 8 + lv.rows, :]
                e = R[f"e{k}"][a, 8 : 8 + lv.rows, :]
                R[f"{dst}{k}"][a, 8 : 8 + lv.rows, :] = c * KEEP + (e + w * v)
                return carry

            loop(count, one, 0, lv.unroll)

        def weigh(lv):
            k = lv.k
            vm = R[f"vm{k}"]

            def use(i, s):
                R[f"w{k}"][i, 8 : 8 + lv.rows, :] = vm[...] * ((DAMPING * lv.q) / (6.0 * lv.q + s))

            z_unpacked(f"s{k}", use)

        def begin(lv):
            k = lv.k
            scale = 1.0 / lv.q

            def use(i, f):
                w = R[f"w{k}"][i, 8 : 8 + lv.rows, :]
                R[f"e{k}"][i, 8 : 8 + lv.rows, :] = (w * scale) * f if k else w * f

            z_unpacked(f"f{k}", use)

        def restrict(lv, of, name):
            k = lv.k
            a0 = start_of(lv)
            half = lv.n // 2
            lane = iota((lv.rows, 128), 1)
            t = R[f"t{k}"]

            def one(j, c):
                v = of(a0 + 2 * j) + of(a0 + 2 * j + 1)
                v = v + jnp.where((lane & lv.r) == 0, roll(v, -lv.r), roll(v, lv.r))
                t[j] = v
                return c

            loop(half, one, 0, lv.unroll // 2)
            wide = iota((half, 128), 1) < B

            def two(j, c):
                v = t[j, pl.ds(lv.h, half, stride=2), :] + t[j, pl.ds(lv.h + 1, half, stride=2), :]
                v = jnp.where(wide, 0.125 * v, 0.0)
                if k + 1 < SPLIT:
                    nxt = levels[k + 1]
                    R[f"{name}{k + 1}"][start_of(nxt) + j, nxt.first : nxt.first + half, :] = v
                else:
                    R["l3"][j, 0:half, :] = v
                return c

            loop(half, two, 0, 12)

        def left_of(lv, src):
            k = lv.k

            def f(a):
                c, v = beside_of(lv, R[f"{src}{k}"], a)
                s = R[f"s{k}"][a, 8 : 8 + lv.rows, :]
                return R[f"f{k}"][a, 8 : 8 + lv.rows, :] - ((6.0 * lv.q + s) * c - lv.q * v)

            return f

        def coefficient(lv):
            return lambda a: R[f"s{lv.k}"][a, 8 : 8 + lv.rows, :]

        def prolong(lv, coarse_rows):
            k = lv.k
            nxt_far = 2
            half = lv.n // 2
            m = half + 2 * nxt_far
            shift = lv.h - 2 * nxt_far
            u = R[f"u{k}"]

            def put(j, c):
                v = coarse_rows(j, m)
                u[j, pl.ds(shift, m, stride=2), :] = v
                u[j, pl.ds(shift + 1, m, stride=2), :] = v
                return c

            loop(half + nxt_far, put, 0, 7)

        def add_up(lv):
            k = lv.k
            a0 = 1 + gx * (lv.h - 4)

            def one(j, c):
                p = R[f"u{k}"][j, 0 : lv.rows, :]
                if k:
                    row = iota((lv.rows, 128), 0)
                    p = jnp.where((row >= lv.h - 4) & (row < lv.h + lv.n + 4), p, 0.0)
                if k == SPLIT - 1:
                    p = jnp.where(R[f"vm{k}"][...] > 0.0, p, 0.0)
                for d in range(2):
                    a = a0 + 2 * j + d
                    R[f"b{k}"][a, 8 : 8 + lv.rows, :] = R[f"a{k}"][a, 8 : 8 + lv.rows, :] + p
                return c

            loop((lv.n + 4) // 2, one, 0, 7)

        def gather_copy(name, dx, dy, dz):
            g = R[name]
            here = g.at[:, gz, pl.ds(mine, 1), :]
            return pltpu.make_async_remote_copy(
                src_ref=here, dst_ref=here, send_sem=R[f"{name}_send"], recv_sem=R[f"{name}_recv"],
                device_id=device(dx, dy, dz), device_id_type=MESH)

        def gather_start(name, rows):
            for p, v in enumerate(rows):
                R[name][p, gz, pl.ds(mine, 1), :] = v
            for to in others:
                gather_copy(name, *to).start()

        def gathered(name):
            size = len(others) * R[name].shape[0]
            return counted(size, R[f"{name}_send"], R[f"{name}_recv"])

        def gather_end(name):
            gathered(name).wait_recv()

        def gather_sent(name):
            gathered(name).wait_send()

        def local_vector():
            wide = packed * 128
            v = R["l3"][...].reshape(n3 * 8, 128)
            l, c = iota((128, wide), 0), iota((128, wide), 1)
            table = jnp.where((l == c % n3 * (1 << SPLIT)) & (c < groups * n3), 1.0, 0.0).astype(BF16)
            v = picked(v, table)
            row, c = iota((n3 * 8, wide), 0), iota((n3 * 8, wide), 1)
            keep = ((row & 7) < n3) & (c // n3 == (row >> 3) * n3 + (row & 7))
            v = jnp.sum(jnp.where(keep, v, 0.0), axis=0, keepdims=True)
            return [v[:, 128 * p : 128 * p + 128] for p in range(packed)]

        def by_device(name, dst):
            for p in range(packed):
                v = R[name][p].reshape(plane * line, 128)
                R[dst][128 * p : 128 * p + 128, :] = v.T

        lv0, lv1, lv2 = levels
        inside = jnp.zeros((B, 128 - B), F32)

        def take(raw, dst):
            def one(x, c):
                v = jnp.concatenate([R[raw][x], inside], axis=1)
                R[dst][start_of(lv0) + x, lv0.first : lv0.first + B, :] = v
                return c

            loop(B, one, 0, 4)

        R["l3"][...] = jnp.zeros((n3, 8, 128), F32)
        inputs[0].wait()
        take("sgr", "sg")
        y_pack("sg")
        z_pack("sg")
        inputs[1].wait()
        take("rer", "s0")
        y_pack("s0")
        z_pack("s0")
        pl.semaphore_wait(barrier, len(faces))
        send("sg")
        greet("k2")
        inputs[2].wait()
        take("rsr", "f0")
        restrict(lv0, coefficient(lv0), "s")
        greeted("k2")
        greet("k3")
        y_pack("s1")
        z_pack("s1")
        restrict(lv1, coefficient(lv1), "s")
        y_pack("s2")
        z_pack("s2")
        greeted("k3")
        greet("k4")
        send("s0")
        restrict(lv2, coefficient(lv2), "s")
        vector3 = local_vector()
        arrive("sg")
        sent("sg")
        y_unpack("sg")

        def keep_guess(i, v):
            R["sg"][i, 8 : 8 + lv0.rows, :] = v

        z_unpacked("sg", keep_guess)

        def first_residual(x, carry):
            a = start_of(lv0) + x
            c, v = beside_of(lv0, R["sg"], a)
            s = R["s0"][a, 8 : 8 + lv0.rows, :]
            f = R["f0"][a, 8 : 8 + lv0.rows, :] - ((6.0 + s) * c - v)
            R["f0"][a, 8 : 8 + lv0.rows, :] = jnp.where(R["own"][...] > 0.0, f, 0.0)
            return carry

        loop(B, first_residual, 0, lv0.unroll)
        greeted("k4")
        greet("k5")
        pack_send("f0")
        send("s1")
        send("s2")

        def weigh_at(lv):
            arrive(f"s{lv.k}")
            y_unpack(f"s{lv.k}")
            weigh(lv)

        weigh_at(lv0)
        arrive("f0")
        y_unpack("f0")
        begin(lv0)

        def first_relax(lv):
            k = lv.k
            count, a0 = span(lv, 4)

            def one(i, carry):
                a = a0 + i
                c, v = beside_of(lv, R[f"e{k}"], a)
                w = R[f"w{k}"][a, 8 : 8 + lv.rows, :]
                R[f"a{k}"][a, 8 : 8 + lv.rows, :] = c * (1.0 + KEEP) + w * v
                return carry

            loop(count, one, 0, lv.unroll)

        first_relax(lv0)
        restrict(lv0, left_of(lv0, "a"), "f")

        def deeper(lv, fill):
            name = f"f{lv.k}"
            pack_send(name)
            fill()
            weigh_at(lv)
            arrive(name)
            y_unpack(name)
            begin(lv)
            first_relax(lv)
            restrict(lv, left_of(lv, "a"), "f")

        greeted("k5")
        deeper(lv1, lambda: None)
        deeper(lv2, lambda: gather_start("gs", vector3))
        gather_start("gf", local_vector())

        gather_end("gs")
        by_device("gs", "s3")
        lane8, row8 = iota((8, 128), 1), iota((8, 128), 0)
        dev_y, dev_x, dev_z = lane8 & (ny - 1), (lane8 >> 2) & 1, lane8 >> 3
        step_x, step_z = ny, plane
        has = {
            ("y", 1): dev_y < ny - 1, ("y", -1): dev_y > 0, ("x", 1): dev_x < nx - 1, ("x", -1): dev_x > 0,
            ("z", 1): dev_z < nz - 1, ("z", -1): dev_z > 0,
        }
        strides = {"y": 1, "x": step_x, "z": step_z}

        def across(v, axis, way):
            return jnp.where(has[axis, way], roll(v, -way * strides[axis]), 0.0)

        def around(get, m):
            def one(x, y):
                c = get(x, y)
                r = n3 // m
                up = jnp.where(row8 >= n3 - r, roll(across(c, "z", 1), n3 - r, 0), roll(c, -r, 0))
                dn = jnp.where(row8 < r, roll(across(c, "z", -1), r - n3, 0), roll(c, r, 0))
                v = up + dn
                v = v + (get(x + 1, y) if x + 1 < m else across(get(0, y), "x", 1))
                v = v + (get(x - 1, y) if x else across(get(m - 1, y), "x", -1))
                v = v + (get(x, y + 1) if y + 1 < m else across(get(x, 0), "y", 1))
                v = v + (get(x, y - 1) if y else across(get(x, m - 1), "y", -1))
                return c, v

            return one

        cells = [(x, y) for x in range(n3) for y in range(n3)]
        m4 = n3 // 2
        cells4 = [(x, y) for x in range(m4) for y in range(m4)]
        live = row8 < n3

        def tile(name, x, y):
            g = (x * n3 + y) * (n3 if name in ("s3", "f3") else 8)
            return R[name][g : g + 8, :]

        for x, y in cells:
            R["w3"][8 * (x * n3 + y) : 8 * (x * n3 + y) + 8, :] = jnp.where(
                live, (DAMPING * q3) / (6.0 * q3 + tile("s3", x, y)), 0.0)

        def coarser(get):
            out = {}
            for x, y in cells4:
                v = (get(2 * x, 2 * y) + get(2 * x, 2 * y + 1)) + (get(2 * x + 1, 2 * y) + get(2 * x + 1, 2 * y + 1))
                v = v + jnp.where((row8 & 1) == 0, roll(v, -1, 0), roll(v, 1, 0))
                out[x, y] = jnp.where(live, 0.125 * v, 0.0)
            return out

        s4 = coarser(lambda x, y: tile("s3", x, y))
        gather_end("gf")
        by_device("gf", "f3")
        e = {}
        e0 = {}
        for c in cells:
            e0[c] = (tile("w3", *c) * (1.0 / q3)) * tile("f3", *c)
        op = around(lambda x, y: e0[x, y], n3)
        for c in cells:
            u, v = op(*c)
            e[c] = u * (1.0 + KEEP) + tile("w3", *c) * v
        op = around(lambda x, y: e[x, y], n3)
        rest = {}
        for c in cells:
            u, v = op(*c)
            rest[c] = jnp.where(live, tile("f3", *c) - ((6.0 * q3 + tile("s3", *c)) * u - q3 * v), 0.0)
        f4 = coarser(lambda x, y: rest[x, y])

        def inner(u, v):
            s = None
            for c in cells4:
                s = u[c] * v[c] if s is None else s + u[c] * v[c]
            return total(s)

        r4 = dict(f4)
        p4 = dict(f4)
        e4 = {c: jnp.zeros((8, 128), F32) for c in cells4}
        rr = inner(r4, r4)
        for _ in range(BOTTOM_ITERS):
            op = around(lambda x, y: p4[x, y], m4)
            q = {}
            for c in cells4:
                u, v = op(*c)
                q[c] = jnp.where(live, (6.0 * q4 + s4[c]) * u - q4 * v, 0.0)
            a = rr / inner(p4, q)
            e4 = {c: e4[c] + a * p4[c] for c in cells4}
            r4 = {c: r4[c] - a * q[c] for c in cells4}
            new = inner(r4, r4)
            ratio = new / rr
            p4 = {c: r4[c] + ratio * p4[c] for c in cells4}
            rr = new
        e = {(x, y): e[x, y] + e4[x // 2, y // 2] for x, y in cells}
        for _ in range(2):
            op = around(lambda x, y: e[x, y], n3)
            nxt = {}
            for c in cells:
                u, v = op(*c)
                nxt[c] = u * KEEP + (e0[c] + tile("w3", *c) * v)
            e = nxt
        for x, y in cells:
            g = x * n3 + y
            R["e3"][8 * g : 8 * g + 8, :] = e[x, y]
        R["e3"][groups * 8 :, :] = jnp.zeros((planes * 128 - groups * 8, 128), F32)
        for p in range(planes):
            R["x3"][p] = R["e3"][128 * p : 128 * p + 128, :].T

        wide = planes * 128
        slabs3 = n3 + 2
        lane_w = iota((8, wide), 1) >> 3
        row_w = iota((8, wide), 0)
        lo_rows = jnp.where(row_w < 2, n3 - 2 + row_w, -1000)
        mid_rows = jnp.where(row_w < 2, -1000, row_w - 2)
        hi_rows = jnp.where(row_w < 2, row_w, -1000)
        y_below, y_above = jnp.maximum(gy - 1, 0), jnp.minimum(gy + 1, ny - 1)
        z_at = [jnp.maximum(gz - 1, 0), gz, jnp.minimum(gz + 1, nz - 1)]

        def vector(dev):
            return jnp.concatenate([R["x3"][p, pl.ds(dev, 1), :] for p in range(planes)], axis=1)

        for i in range(slabs3):
            partner = jnp.where(gx == 0, i >= n3, i < 2)
            px = jnp.where(partner, 1 - gx, gx)
            xx = jnp.where(gx == 0, i - jnp.where(i >= n3, n3, 0), i - 2 + jnp.where(i < 2, n3, 0))
            lo, mid, hi = (lane_w == xx * n3 + rows for rows in (lo_rows, mid_rows, hi_rows))
            for d in range(3):
                at_y = lambda g: vector(z_at[d] * plane + px * ny + g)
                first = jnp.where(mid, at_y(gy), jnp.where(lo, at_y(y_below), 0.0))
                second = jnp.where(hi, at_y(y_above), 0.0)
                R["lhs"][d, 16 * i : 16 * i + 8, :] = first
                R["lhs"][d, 16 * i + 8 : 16 * i + 16, :] = second
        l, c = iota((wide, 128), 1), iota((wide, 128), 0)
        table = jnp.where((l < B) & ((c & 7) == (l >> SPLIT)) & (c < groups * 8), 1.0, 0.0).astype(BF16)
        v = picked(R["lhs"][...].reshape(3 * slabs3 * 16, wide), table).reshape(3, slabs3, 16, 128)
        v = v[1] + roll(v[2].reshape(slabs3 * 16, 128), B).reshape(slabs3, 16, 128) + roll(
            v[0].reshape(slabs3 * 16, 128), -B).reshape(slabs3, 16, 128)
        u = R["u2"]
        shift = lv2.h - 4
        for i in range(slabs3):
            m = n3 + 4
            u[i, pl.ds(shift, m, stride=2), :] = v[i, 0:m]
            u[i, pl.ds(shift + 1, m, stride=2), :] = v[i, 0:m]

        add_up(lv2)
        relax(lv2, "b", "a", 4)
        relax(lv2, "a", "b", 2)

        def coarse_of(nxt, ref):
            a0 = 1 + gx * (nxt.h - 2)
            return lambda j, m: R[ref][a0 + j, nxt.first - 2 : nxt.first - 2 + m, :]

        prolong(lv1, coarse_of(lv2, "b2"))
        add_up(lv1)
        relax(lv1, "b", "a", 4)
        relax(lv1, "a", "b", 2)
        prolong(lv0, coarse_of(lv1, "b1"))
        add_up(lv0)
        relax(lv0, "b", "a", 4)
        relax(lv0, "a", "b", 2)

        def image(x, sums):
            upper, lower = sums
            a = start_of(lv0) + x
            c, v = beside_of(lv0, R["b0"], a)
            s = R["s0"][a, 8 : 8 + lv0.rows, :]
            ap = (6.0 + s) * c - v
            R["ap"][x] = ap
            c = jnp.where(R["own"][...] > 0.0, c, 0.0)
            return upper + R["f0"][a, 8 : 8 + lv0.rows, :] * c, lower + ap * c

        zero = jnp.zeros((lv0.rows, 128), F32)
        upper, lower = loop(B, image, (zero, zero), lv0.unroll)
        upper, lower = (jnp.sum(v, axis=0, keepdims=True) for v in (upper, lower))
        half = iota((1, 128), 1) < 64
        gather_start("gr", [jnp.where(half, upper, roll(lower, 64))])
        gather_end("gr")
        v = jnp.sum(R["gr"][0], axis=0)
        half = iota((8, 128), 1) < 64
        sums = [total(jnp.where(half, v, 0.0)), total(jnp.where(half, 0.0, v))]
        step_length = sums[0] / sums[1]

        def finish(x, c):
            a = start_of(lv0) + x
            p = R["b0"][a, lv0.first : lv0.first + B, :]
            f = R["f0"][a, lv0.first : lv0.first + B, :]
            q = R["ap"][x, lv0.h : lv0.h + B, :]
            sol_ref[x] = R["sgr"][x] + (step_length * p)[:, 0:B]
            res_ref[x] = (f - step_length * q)[:, 0:B]
            return c

        loop(B, finish, 0, 4)
        for name in exchanges:
            if name != "sg":
                sent(name)
        for name in ("gs", "gf", "gr"):
            gather_sent(name)

    return kernel, list(scratch.values())


def solution(mesh):
    sizes = tuple(mesh.shape[a] for a in AXES)

    def body(right_side, start_guess, reaction):
        kernel, scratch = make_kernel(sizes, right_side.shape)
        out = jax.ShapeDtypeStruct(right_side.shape, F32)
        return tuple(
            pl.pallas_call(
                kernel,
                out_shape=(out, out),
                in_specs=[pl.BlockSpec(memory_space=pl.ANY)] * 3,
                out_specs=(pl.BlockSpec(memory_space=pltpu.VMEM),) * 2,
                scratch_shapes=scratch,
                compiler_params=pltpu.CompilerParams(
                    collective_id=0, has_side_effects=True, vmem_limit_bytes=51 * 2**20
                ),
                name="cg_step",
            )(right_side, start_guess, reaction)
        )

    placed = P(*AXES)
    return jax.shard_map(
        body, mesh=mesh, in_specs=(placed,) * 3, out_specs=(placed,) * 2, check_vma=False
    )
```

```python
import jax
import jax.numpy as jnp
from jax import lax
from jax.experimental import pallas as pl
from jax.experimental.pallas import tpu as pltpu
from jax.sharding import PartitionSpec as P

BOTTOM_ITERS = 6
AXES = ("gx", "gy", "gz")
MESH = pl.DeviceIdType.MESH
F32 = jnp.float32
BF16 = jnp.bfloat16
DAMPING = 6.0 / 7.0
KEEP = 1.0 / 7.0
SPLIT = 3
HALO = (4, 5, 5)


def loop(n, f, carry=0, unroll=4):
    unroll = min(unroll, n)
    while n % unroll:
        unroll -= 1

    def step(i, c):
        for k in range(unroll):
            c = f(i * unroll + k, c)
        return c

    return lax.fori_loop(0, n // unroll, step, carry)


def iota(shape, axis):
    return lax.broadcasted_iota(jnp.int32, shape, axis)


def roll(v, shift, axis=1):
    shift = shift % v.shape[axis] if isinstance(shift, int) else shift
    return v if isinstance(shift, int) and shift == 0 else pltpu.roll(v, shift, axis)


def halves(v):
    high = v.astype(BF16)
    low = (v - high.astype(F32)).astype(BF16)
    return high, low


def picked(v, table):
    high, low = halves(v)
    return jnp.dot(high, table, preferred_element_type=F32) + jnp.dot(low, table, preferred_element_type=F32)


def total(v):
    v = jnp.sum(v, axis=0, keepdims=True)
    return jnp.sum(v, axis=1, keepdims=True)


class Level:
    def __init__(self, k, block):
        self.k = k
        self.n = block >> k
        self.h = HALO[k]
        self.r = 1 << k
        self.q = 0.25**k
        self.tiles = -(-(self.n + 2 * self.h) // 8)
        self.rows = 8 * self.tiles
        self.slabs = self.n + self.h
        self.first = 8 + self.h
        self.unroll = 52 if k == 0 else 28
        self.shape = (self.slabs + 2, self.rows + 16, 128)


def make_kernel(sizes, block):
    nx, ny, nz = sizes
    B = block[0]
    levels = [Level(k, B) for k in range(SPLIT)]
    n3 = B >> SPLIT
    groups = n3 * n3
    planes = -(-groups * 8 // 128)
    packed = -(-groups * n3 // 128)
    q3, q4 = 0.25**3, 0.25**4
    line = nz
    plane = nx * ny

    scratch = {}
    for name in ("rsr", "sgr", "rer"):
        scratch[name] = pltpu.VMEM((B, B, B), F32)
    scratch["insem"] = pltpu.SemaphoreType.DMA((3,))
    exchanges = {}

    def add_exchange(name, k, field, t, wide):
        lv = levels[k]
        per = 128 // (t * lv.r)
        ex = dict(lv=lv, field=field, t=t, wide=wide, per=per, pairs=lv.n // 2, groups=-(-lv.n // per))
        for d in ("s", "r"):
            scratch[f"y{d}_{name}"] = pltpu.VMEM((2, ex["pairs"], t, 128), F32)
            scratch[f"z{d}_{name}"] = pltpu.VMEM((2, ex["groups"], lv.rows, 128), F32)
        if wide:
            scratch[f"yx_{name}"] = pltpu.VMEM((2, t, t, 128), F32)
            scratch[f"zx_{name}"] = pltpu.VMEM((2, lv.rows, 128), F32)
        scratch[f"send_{name}"] = pltpu.SemaphoreType.DMA
        scratch[f"recv_{name}"] = pltpu.SemaphoreType.DMA
        exchanges[name] = ex

    for lv in levels:
        k = lv.k
        for name in ("f", "s", "w", "e", "a", "b"):
            scratch[f"{name}{k}"] = pltpu.VMEM(lv.shape, F32)
        scratch[f"vm{k}"] = pltpu.VMEM((lv.rows, 128), F32)
        scratch[f"t{k}"] = pltpu.VMEM((lv.n // 2, lv.rows, 128), F32)
        scratch[f"u{k}"] = pltpu.VMEM((lv.slabs // 2 + 1, lv.rows + 16, 128), F32)
        add_exchange(f"f{k}", k, f"f{k}", lv.h, True)
        add_exchange(f"s{k}", k, f"s{k}", lv.h, True)
    scratch["sg"] = pltpu.VMEM(levels[0].shape, F32)
    add_exchange("sg", 0, "sg", 1, False)
    scratch["ap"] = pltpu.VMEM((B, levels[0].rows, 128), F32)
    scratch["own"] = pltpu.VMEM((levels[0].rows, 128), F32)
    for name, count in (("gs", packed), ("gf", packed), ("gr", 1)):
        scratch[name] = pltpu.VMEM((count, line, plane, 128), F32)
        scratch[f"{name}_send"] = pltpu.SemaphoreType.DMA
        scratch[f"{name}_recv"] = pltpu.SemaphoreType.DMA
    scratch["count"] = pltpu.VMEM((1024, 128), F32)
    for name in ("k2", "k3", "k4", "k5"):
        scratch[name] = pltpu.SemaphoreType.REGULAR
    scratch["l3"] = pltpu.VMEM((n3, 8, 128), F32)
    for name in ("s3", "f3", "w3", "e3"):
        scratch[name] = pltpu.VMEM((planes * 128, 128), F32)
    scratch["x3"] = pltpu.VMEM((planes, plane * line, 128), F32)
    scratch["lhs"] = pltpu.VMEM((3, (n3 + 2) * 16, planes * 128), F32)

    names = list(scratch)

    def kernel(rs_ref, sg_ref, re_ref, sol_ref, res_ref, *refs):
        R = dict(zip(names, refs))
        gx, gy, gz = (lax.axis_index(a) for a in AXES)
        mine = gx * ny + gy

        inputs = [
            pltpu.make_async_copy(src, R[dst], R["insem"].at[i])
            for i, (src, dst) in enumerate(((sg_ref, "sgr"), (re_ref, "rer"), (rs_ref, "rsr")))
        ]
        for copy in inputs:
            copy.start()

        def start_of(lv):
            return 1 + gx * lv.h

        for lv in levels:
            k = lv.k

            def blank(a, c, k=k, lv=lv):
                for name in ("f", "s"):
                    ref = R[f"{name}{k}"]
                    ref[a, 8:16, :] = jnp.zeros((8, 128), F32)
                    low = (lv.first + lv.n) // 8 * 8
                    ref[a, low : 8 + lv.rows, :] = jnp.zeros((8 + lv.rows - low, 128), F32)
                if k == 0:
                    ref = R["sg"]
                    ref[a, 8:16, :] = jnp.zeros((8, 128), F32)
                    ref[a, low : 8 + lv.rows, :] = jnp.zeros((8 + lv.rows - low, 128), F32)
                return c

            loop(lv.shape[0], blank, 0, 2)

        for name, ex in exchanges.items():
            for m in ("yr", "yx", "zr", "zx") if ex["wide"] else ("yr", "zr"):
                ref = R[f"{m}_{name}"]
                ref[...] = jnp.zeros(ref.shape, F32)

        barrier = pltpu.get_barrier_semaphore()
        others = []
        for dz in range(nz):
            for dx in range(nx):
                for dy in range(ny):
                    if dx or dy or dz:
                        others.append((dx, dy, dz))

        def hops(to):
            dx, dy, dz = to
            return dx + min(dy, ny - dy) + min(dz % 4, 4 - dz % 4) + min(dz // 4, nz // 4 - dz // 4)

        others.sort(key=lambda to: (-hops(to), to))

        def device(dx, dy, dz):
            return {"gx": lax.rem(gx + dx, nx), "gy": lax.rem(gy + dy, ny), "gz": lax.rem(gz + dz, nz)}

        faces = [(1, 0, 0), (0, 1, 0), (0, ny - 1, 0), (0, 0, 1), (0, 0, nz - 1)]
        two = nz // 8
        waves = {
            "k2": faces,
            "k3": faces[:3] + [(0, 0, two), (0, 0, nz - two)],
            "k4": [(0, 0, 2 * two), (0, 0, nz - 2 * two)],
            "k5": [to for to in others if to[2] == 0],
        }

        def greet(name):
            for to in waves[name]:
                pl.semaphore_signal(R[name], inc=1, device_id=device(*to), device_id_type=MESH)

        def greeted(name):
            pl.semaphore_wait(R[name], len(waves[name]))

        for to in faces:
            pl.semaphore_signal(barrier, inc=1, device_id=device(*to), device_id_type=MESH)

        for lv in levels:
            k = lv.k
            z8 = jnp.zeros((8, 128), F32)
            zs = jnp.zeros((lv.rows, 128), F32)
            fields = ["e", "a", "b"] + (["sg"] if k == 0 else [])
            fields = [R[f if f == "sg" else f"{f}{k}"] for f in fields]

            def guard(a, c, fields=fields, lv=lv, z8=z8):
                for ref in fields:
                    ref[a, 0:8, :] = z8
                    ref[a, 8 + lv.rows : 16 + lv.rows, :] = z8
                return c

            loop(lv.shape[0], guard, 0, 2)
            for ref in fields:
                ref[0, 8 : 8 + lv.rows, :] = zs
                ref[lv.slabs + 1, 8 : 8 + lv.rows, :] = zs

            lane, row = iota((lv.rows, 128), 1), iota((lv.rows, 128), 0)
            wd = lv.h * lv.r
            ok = (lane < B) | ((lane < B + wd) & (gz < nz - 1)) | ((lane >= 128 - wd) & (gz > 0))
            ok = ok & (row >= jnp.where(gy > 0, 0, lv.h))
            ok = ok & (row < lv.n + lv.h + jnp.where(gy < ny - 1, lv.h, 0))
            R[f"vm{k}"][...] = jnp.where(ok, 1.0, 0.0)
            if k == 0:
                own = (lane < B) & (row >= lv.h) & (row < lv.h + lv.n)
                R["own"][...] = jnp.where(own, 1.0, 0.0)

        def messages(name):
            ex = exchanges[name]
            lv, t, m = ex["lv"], ex["t"], ex["pairs"]
            f = R[ex["field"]]
            src = jnp.where(gx == 0, 1 + lv.n - t, 1 + lv.h)
            dst = jnp.where(gx == 0, 1 + lv.h - t, 1 + lv.n)
            rows = pl.ds(lv.first, lv.n)
            own = pl.ds(lv.h, lv.n)
            ys, yr, zs, zr = (R[f"{c}_{name}"] for c in ("ys", "yr", "zs", "zr"))
            out = [(f.at[pl.ds(src, t), rows, :], f.at[pl.ds(dst, t), rows, :], 1, 0, 0)]
            for i, way in enumerate((-1, 1)):
                out.append((ys.at[i], yr.at[1 - i], 0, way, 0))
                out.append((zs.at[i, :, own, :], zr.at[1 - i, :, own, :], 0, 0, way))
            if ex["wide"]:
                yx, zx = R[f"yx_{name}"], R[f"zx_{name}"]
                pair = jnp.where(gx == 0, m - t, 0)
                group = jnp.where(gx == 0, ex["groups"] - 1, 0)
                for i, way in enumerate((-1, 1)):
                    out.append((ys.at[i, pl.ds(pair, t)], yx.at[1 - i], 1, way, 0))
                    out.append((zs.at[i, group, own, :], zx.at[1 - i, own, :], 1, 0, way))
                    for yway in (-1, 1):
                        here = pl.ds(lv.h if yway < 0 else lv.h + lv.n - t, t)
                        there = pl.ds(lv.h + lv.n if yway < 0 else lv.h - t, t)
                        out.append((zs.at[i, :, here, :], zr.at[1 - i, :, there, :], 0, yway, way))
                        out.append((zs.at[i, group, here, :], zx.at[1 - i, there, :], 1, yway, way))
            return out

        def guarded(cond, f):
            if cond is None:
                f()
            else:
                pl.when(cond)(f)

        def send(name, only=None):
            batch = [m for m in messages(name) if only is None or only(*m[2:])]
            batch.sort(key=lambda m: -(m[2] + abs(m[3]) + 2 * abs(m[4])))
            for src, dst, ox, oy, oz in batch:
                copy = pltpu.make_async_remote_copy(
                    src_ref=src, dst_ref=dst, send_sem=R[f"send_{name}"], recv_sem=R[f"recv_{name}"],
                    device_id=device(ox, oy % ny, oz % nz), device_id_type=MESH)
                cond = None
                for at, n, way in ((gy, ny, oy), (gz, nz, oz)):
                    if way:
                        there = at > 0 if way < 0 else at < n - 1
                        cond = there if cond is None else cond & there
                guarded(cond, copy.start)

        def counted(size, send_sem, recv_sem):
            rows = R["count"].at[pl.ds(0, size), :]
            return pltpu.make_async_remote_copy(
                src_ref=rows, dst_ref=rows, send_sem=send_sem, recv_sem=recv_sem,
                device_id=device(1, 0, 0), device_id_type=MESH)

        def in_all(name, getting):
            sizes = [(src.shape, oy, oz) for src, _, _, oy, oz in messages(name)]
            for y, at_y in ((0, gy == 0), (1, (gy > 0) & (gy < ny - 1)), (2, gy == ny - 1)):
                for z, at_z in ((0, gz == 0), (1, (gz > 0) & (gz < nz - 1)), (2, gz == nz - 1)):
                    rows = 0
                    for shape, oy, oz in sizes:
                        oy, oz = (-oy, -oz) if getting else (oy, oz)
                        if y + oy in (0, 1, 2) and z + oz in (0, 1, 2):
                            count = 1
                            for d in shape[:-1]:
                                count *= d
                            rows += count
                    copy = counted(rows, R[f"send_{name}"], R[f"recv_{name}"])
                    pl.when(at_y & at_z)(copy.wait_recv if getting else copy.wait_send)

        def arrive(name):
            in_all(name, True)

        def sent(name):
            in_all(name, False)

        def y_pack(name):
            ex = exchanges[name]
            lv, t, m = ex["lv"], ex["t"], ex["pairs"]
            f, a = R[ex["field"]], start_of(lv)
            lane = iota((t, 128), 1)
            for side, row in ((0, lv.first), (1, lv.first + lv.n - t)):
                for i in range(m):
                    v = f[a + i, row : row + t, :]
                    R[f"ys_{name}"][side, i] = jnp.where(lane < 64, v, roll(f[a + i + m, row : row + t, :], 64))

        def y_unpack(name):
            ex = exchanges[name]
            lv, t, m = ex["lv"], ex["t"], ex["pairs"]
            f, a = R[ex["field"]], start_of(lv)
            keep = iota((t, 128), 1) < B
            edge = jnp.where(gx == 0, 1 + lv.n, 1)
            for side, row, ok in ((0, lv.first - t, gy > 0), (1, lv.first + lv.n, gy < ny - 1)):
                for i in range(m):
                    v = R[f"yr_{name}"][side, i]
                    v = v if ex["wide"] else jnp.where(ok, v, 0.0)
                    f[a + i, row : row + t, :] = jnp.where(keep, v, 0.0)
                    f[a + i + m, row : row + t, :] = jnp.where(keep, roll(v, 64), 0.0)
                if ex["wide"]:
                    for i in range(t):
                        v = pltpu.roll(R[f"yx_{name}"][side, i], gx * 64, 1)
                        f[edge + i, row : row + t, :] = jnp.where(keep, v, 0.0)

        def z_pack(name):
            ex = exchanges[name]
            lv, per = ex["lv"], ex["per"]
            wd = ex["t"] * lv.r
            f, a = R[ex["field"]], start_of(lv)
            lane = iota((lv.rows, 128), 1)
            for g in range(ex["groups"]):
                low = high = None
                count = min(per, lv.n - g * per)
                for j in reversed(range(count)):
                    v = f[a + g * per + j, 8 : 8 + lv.rows, :]
                    c = j * wd
                    one, two = roll(v, c), roll(v, c - (B - wd))
                    low = one if low is None else jnp.where(lane < c + wd, one, low)
                    high = two if high is None else jnp.where(lane < c + wd, two, high)
                R[f"zs_{name}"][0, g] = low
                R[f"zs_{name}"][1, g] = high

        def pack_send(name):
            send(name, lambda ox, oy, oz: not oy and not oz)
            z_pack(name)
            send(name, lambda ox, oy, oz: oz)
            y_pack(name)
            send(name, lambda ox, oy, oz: oy and not oz)

        def z_unpacked(name, use):
            ex = exchanges[name]
            lv, per, t = ex["lv"], ex["per"], ex["t"]
            wd = t * lv.r
            f, a = R[ex["field"]], start_of(lv)
            lane = iota((lv.rows, 128), 1)

            def put(i, below, above):
                if not ex["wide"]:
                    below, above = jnp.where(gz > 0, below, 0.0), jnp.where(gz < nz - 1, above, 0.0)
                v = jnp.where(lane < B + wd, above, jnp.where(lane >= 128 - wd, below, 0.0))
                use(i, jnp.where(lane < B, f[i, 8 : 8 + lv.rows, :], v))

            for j in range(lv.n):
                g, c = j // per, j % per * wd
                put(a + j, roll(R[f"zr_{name}"][0, g], -wd - c), roll(R[f"zr_{name}"][1, g], B - c))
            if ex["wide"]:
                edge = jnp.where(gx == 0, 1 + lv.n, 1)
                for j in range(t):
                    c0, c1 = j * wd, (lv.n - t + j - (ex["groups"] - 1) * per) * wd
                    one = jnp.where(gx == 0, (-wd - c0) % 128, (-wd - c1) % 128)
                    two = jnp.where(gx == 0, (B - c0) % 128, (B - c1) % 128)
                    put(edge + j, pltpu.roll(R[f"zx_{name}"][0], one, 1), pltpu.roll(R[f"zx_{name}"][1], two, 1))

        def beside_of(lv, ref, a):
            rows = lv.rows
            c = ref[a, 8 : 8 + rows, :]
            v = ref[a + 1, 8 : 8 + rows, :] + ref[a - 1, 8 : 8 + rows, :]
            v = v + (ref[a, 9 : 9 + rows, :] + ref[a, 7 : 7 + rows, :])
            return c, v + (roll(c, lv.r) + roll(c, -lv.r))

        def span(lv, far):
            return lv.n + far, 1 + gx * (lv.h - far)

        def relax(lv, src, dst, far):
            k = lv.k
            count, a0 = span(lv, far)

            def one(i, carry):
                a = a0 + i
                c, v = beside_of(lv, R[f"{src}{k}"], a)
                w = R[f"w{k}"][a, 8 : 8 + lv.rows, :]
                e = R[f"e{k}"][a, 8 : 8 + lv.rows, :]
                R[f"{dst}{k}"][a, 8 : 8 + lv.rows, :] = c * KEEP + (e + w * v)
                return carry

            loop(count, one, 0, lv.unroll)

        def weigh(lv):
            k = lv.k
            vm = R[f"vm{k}"]

            def use(i, s):
                R[f"w{k}"][i, 8 : 8 + lv.rows, :] = vm[...] * ((DAMPING * lv.q) / (6.0 * lv.q + s))

            z_unpacked(f"s{k}", use)

        def begin(lv):
            k = lv.k
            scale = 1.0 / lv.q

            def use(i, f):
                w = R[f"w{k}"][i, 8 : 8 + lv.rows, :]
                R[f"e{k}"][i, 8 : 8 + lv.rows, :] = (w * scale) * f if k else w * f

            z_unpacked(f"f{k}", use)

        def restrict(lv, of, name):
            k = lv.k
            a0 = start_of(lv)
            half = lv.n // 2
            lane = iota((lv.rows, 128), 1)
            t = R[f"t{k}"]

            def one(j, c):
                v = of(a0 + 2 * j) + of(a0 + 2 * j + 1)
                v = v + jnp.where((lane & lv.r) == 0, roll(v, -lv.r), roll(v, lv.r))
                t[j] = v
                return c

            loop(half, one, 0, lv.unroll // 2)
            wide = iota((half, 128), 1) < B

            def two(j, c):
                v = t[j, pl.ds(lv.h, half, stride=2), :] + t[j, pl.ds(lv.h + 1, half, stride=2), :]
                v = jnp.where(wide, 0.125 * v, 0.0)
                if k + 1 < SPLIT:
                    nxt = levels[k + 1]
                    R[f"{name}{k + 1}"][start_of(nxt) + j, nxt.first : nxt.first + half, :] = v
                else:
                    R["l3"][j, 0:half, :] = v
                return c

            loop(half, two, 0, 12)

        def left_of(lv, src):
            k = lv.k

            def f(a):
                c, v = beside_of(lv, R[f"{src}{k}"], a)
                s = R[f"s{k}"][a, 8 : 8 + lv.rows, :]
                return R[f"f{k}"][a, 8 : 8 + lv.rows, :] - ((6.0 * lv.q + s) * c - lv.q * v)

            return f

        def coefficient(lv):
            return lambda a: R[f"s{lv.k}"][a, 8 : 8 + lv.rows, :]

        def prolong(lv, coarse_rows):
            k = lv.k
            nxt_far = 2
            half = lv.n // 2
            m = half + 2 * nxt_far
            shift = lv.h - 2 * nxt_far
            u = R[f"u{k}"]

            def put(j, c):
                v = coarse_rows(j, m)
                u[j, pl.ds(shift, m, stride=2), :] = v
                u[j, pl.ds(shift + 1, m, stride=2), :] = v
                return c

            loop(half + nxt_far, put, 0, 7)

        def add_up(lv):
            k = lv.k
            a0 = 1 + gx * (lv.h - 4)

            def one(j, c):
                p = R[f"u{k}"][j, 0 : lv.rows, :]
                if k:
                    row = iota((lv.rows, 128), 0)
                    p = jnp.where((row >= lv.h - 4) & (row < lv.h + lv.n + 4), p, 0.0)
                if k == SPLIT - 1:
                    p = jnp.where(R[f"vm{k}"][...] > 0.0, p, 0.0)
                for d in range(2):
                    a = a0 + 2 * j + d
                    R[f"b{k}"][a, 8 : 8 + lv.rows, :] = R[f"a{k}"][a, 8 : 8 + lv.rows, :] + p
                return c

            loop((lv.n + 4) // 2, one, 0, 7)

        def gather_copy(name, dx, dy, dz):
            g = R[name]
            here = g.at[:, gz, pl.ds(mine, 1), :]
            return pltpu.make_async_remote_copy(
                src_ref=here, dst_ref=here, send_sem=R[f"{name}_send"], recv_sem=R[f"{name}_recv"],
                device_id=device(dx, dy, dz), device_id_type=MESH)

        def gather_start(name, rows):
            for p, v in enumerate(rows):
                R[name][p, gz, pl.ds(mine, 1), :] = v
            for to in others:
                gather_copy(name, *to).start()

        def gathered(name):
            size = len(others) * R[name].shape[0]
            return counted(size, R[f"{name}_send"], R[f"{name}_recv"])

        def gather_end(name):
            gathered(name).wait_recv()

        def gather_sent(name):
            gathered(name).wait_send()

        def local_vector():
            wide = packed * 128
            v = R["l3"][...].reshape(n3 * 8, 128)
            l, c = iota((128, wide), 0), iota((128, wide), 1)
            table = jnp.where((l == c % n3 * (1 << SPLIT)) & (c < groups * n3), 1.0, 0.0).astype(BF16)
            v = picked(v, table)
            row, c = iota((n3 * 8, wide), 0), iota((n3 * 8, wide), 1)
            keep = ((row & 7) < n3) & (c // n3 == (row >> 3) * n3 + (row & 7))
            v = jnp.sum(jnp.where(keep, v, 0.0), axis=0, keepdims=True)
            return [v[:, 128 * p : 128 * p + 128] for p in range(packed)]

        def by_device(name, dst):
            for p in range(packed):
                v = R[name][p].reshape(plane * line, 128)
                R[dst][128 * p : 128 * p + 128, :] = v.T

        lv0, lv1, lv2 = levels
        inside = jnp.zeros((B, 128 - B), F32)

        def take(raw, dst):
            def one(x, c):
                v = jnp.concatenate([R[raw][x], inside], axis=1)
                R[dst][start_of(lv0) + x, lv0.first : lv0.first + B, :] = v
                return c

            loop(B, one, 0, 4)

        R["l3"][...] = jnp.zeros((n3, 8, 128), F32)
        inputs[0].wait()
        take("sgr", "sg")
        y_pack("sg")
        z_pack("sg")
        inputs[1].wait()
        take("rer", "s0")
        y_pack("s0")
        z_pack("s0")
        pl.semaphore_wait(barrier, len(faces))
        send("sg")
        greet("k2")
        send("s0", lambda *to: sum(map(abs, to)) == 1)
        inputs[2].wait()
        take("rsr", "f0")
        restrict(lv0, coefficient(lv0), "s")
        greeted("k2")
        greet("k3")
        y_pack("s1")
        z_pack("s1")
        restrict(lv1, coefficient(lv1), "s")
        y_pack("s2")
        z_pack("s2")
        greeted("k3")
        greet("k4")
        send("s0", lambda *to: sum(map(abs, to)) > 1)
        restrict(lv2, coefficient(lv2), "s")
        vector3 = local_vector()
        arrive("sg")
        sent("sg")
        y_unpack("sg")

        def keep_guess(i, v):
            R["sg"][i, 8 : 8 + lv0.rows, :] = v

        z_unpacked("sg", keep_guess)

        def first_residual(x, carry):
            a = start_of(lv0) + x
            c, v = beside_of(lv0, R["sg"], a)
            s = R["s0"][a, 8 : 8 + lv0.rows, :]
            f = R["f0"][a, 8 : 8 + lv0.rows, :] - ((6.0 + s) * c - v)
            R["f0"][a, 8 : 8 + lv0.rows, :] = jnp.where(R["own"][...] > 0.0, f, 0.0)
            return carry

        loop(B, first_residual, 0, lv0.unroll)
        greeted("k4")
        greet("k5")
        pack_send("f0")
        send("s1")
        send("s2")

        def weigh_at(lv):
            arrive(f"s{lv.k}")
            y_unpack(f"s{lv.k}")
            weigh(lv)

        weigh_at(lv0)
        arrive("f0")
        y_unpack("f0")
        begin(lv0)

        def first_relax(lv):
            k = lv.k
            count, a0 = span(lv, 4)

            def one(i, carry):
                a = a0 + i
                c, v = beside_of(lv, R[f"e{k}"], a)
                w = R[f"w{k}"][a, 8 : 8 + lv.rows, :]
                R[f"a{k}"][a, 8 : 8 + lv.rows, :] = c * (1.0 + KEEP) + w * v
                return carry

            loop(count, one, 0, lv.unroll)

        first_relax(lv0)
        restrict(lv0, left_of(lv0, "a"), "f")

        def deeper(lv, fill):
            name = f"f{lv.k}"
            pack_send(name)
            fill()
            weigh_at(lv)
            arrive(name)
            y_unpack(name)
            begin(lv)
            first_relax(lv)
            restrict(lv, left_of(lv, "a"), "f")

        greeted("k5")
        deeper(lv1, lambda: None)
        deeper(lv2, lambda: gather_start("gs", vector3))
        gather_start("gf", local_vector())

        gather_end("gs")
        by_device("gs", "s3")
        lane8, row8 = iota((8, 128), 1), iota((8, 128), 0)
        dev_y, dev_x, dev_z = lane8 & (ny - 1), (lane8 >> 2) & 1, lane8 >> 3
        step_x, step_z = ny, plane
        has = {
            ("y", 1): dev_y < ny - 1, ("y", -1): dev_y > 0, ("x", 1): dev_x < nx - 1, ("x", -1): dev_x > 0,
            ("z", 1): dev_z < nz - 1, ("z", -1): dev_z > 0,
        }
        strides = {"y": 1, "x": step_x, "z": step_z}

        def across(v, axis, way):
            return jnp.where(has[axis, way], roll(v, -way * strides[axis]), 0.0)

        def around(get, m):
            def one(x, y):
                c = get(x, y)
                r = n3 // m
                up = jnp.where(row8 >= n3 - r, roll(across(c, "z", 1), n3 - r, 0), roll(c, -r, 0))
                dn = jnp.where(row8 < r, roll(across(c, "z", -1), r - n3, 0), roll(c, r, 0))
                v = up + dn
                v = v + (get(x + 1, y) if x + 1 < m else across(get(0, y), "x", 1))
                v = v + (get(x - 1, y) if x else across(get(m - 1, y), "x", -1))
                v = v + (get(x, y + 1) if y + 1 < m else across(get(x, 0), "y", 1))
                v = v + (get(x, y - 1) if y else across(get(x, m - 1), "y", -1))
                return c, v

            return one

        cells = [(x, y) for x in range(n3) for y in range(n3)]
        m4 = n3 // 2
        cells4 = [(x, y) for x in range(m4) for y in range(m4)]
        live = row8 < n3

        def tile(name, x, y):
            g = (x * n3 + y) * (n3 if name in ("s3", "f3") else 8)
            return R[name][g : g + 8, :]

        for x, y in cells:
            R["w3"][8 * (x * n3 + y) : 8 * (x * n3 + y) + 8, :] = jnp.where(
                live, (DAMPING * q3) / (6.0 * q3 + tile("s3", x, y)), 0.0)

        def coarser(get):
            out = {}
            for x, y in cells4:
                v = (get(2 * x, 2 * y) + get(2 * x, 2 * y + 1)) + (get(2 * x + 1, 2 * y) + get(2 * x + 1, 2 * y + 1))
                v = v + jnp.where((row8 & 1) == 0, roll(v, -1, 0), roll(v, 1, 0))
                out[x, y] = jnp.where(live, 0.125 * v, 0.0)
            return out

        s4 = coarser(lambda x, y: tile("s3", x, y))
        gather_end("gf")
        by_device("gf", "f3")
        e = {}
        e0 = {}
        for c in cells:
            e0[c] = (tile("w3", *c) * (1.0 / q3)) * tile("f3", *c)
        op = around(lambda x, y: e0[x, y], n3)
        for c in cells:
            u, v = op(*c)
            e[c] = u * (1.0 + KEEP) + tile("w3", *c) * v
        op = around(lambda x, y: e[x, y], n3)
        rest = {}
        for c in cells:
            u, v = op(*c)
            rest[c] = jnp.where(live, tile("f3", *c) - ((6.0 * q3 + tile("s3", *c)) * u - q3 * v), 0.0)
        f4 = coarser(lambda x, y: rest[x, y])

        def inner(u, v):
            s = None
            for c in cells4:
                s = u[c] * v[c] if s is None else s + u[c] * v[c]
            return total(s)

        r4 = dict(f4)
        p4 = dict(f4)
        e4 = {c: jnp.zeros((8, 128), F32) for c in cells4}
        rr = inner(r4, r4)
        for _ in range(BOTTOM_ITERS):
            op = around(lambda x, y: p4[x, y], m4)
            q = {}
            for c in cells4:
                u, v = op(*c)
                q[c] = jnp.where(live, (6.0 * q4 + s4[c]) * u - q4 * v, 0.0)
            a = rr / inner(p4, q)
            e4 = {c: e4[c] + a * p4[c] for c in cells4}
            r4 = {c: r4[c] - a * q[c] for c in cells4}
            new = inner(r4, r4)
            ratio = new / rr
            p4 = {c: r4[c] + ratio * p4[c] for c in cells4}
            rr = new
        e = {(x, y): e[x, y] + e4[x // 2, y // 2] for x, y in cells}
        for _ in range(2):
            op = around(lambda x, y: e[x, y], n3)
            nxt = {}
            for c in cells:
                u, v = op(*c)
                nxt[c] = u * KEEP + (e0[c] + tile("w3", *c) * v)
            e = nxt
        for x, y in cells:
            g = x * n3 + y
            R["e3"][8 * g : 8 * g + 8, :] = e[x, y]
        R["e3"][groups * 8 :, :] = jnp.zeros((planes * 128 - groups * 8, 128), F32)
        for p in range(planes):
            R["x3"][p] = R["e3"][128 * p : 128 * p + 128, :].T

        wide = planes * 128
        slabs3 = n3 + 2
        lane_w = iota((8, wide), 1) >> 3
        row_w = iota((8, wide), 0)
        lo_rows = jnp.where(row_w < 2, n3 - 2 + row_w, -1000)
        mid_rows = jnp.where(row_w < 2, -1000, row_w - 2)
        hi_rows = jnp.where(row_w < 2, row_w, -1000)
        y_below, y_above = jnp.maximum(gy - 1, 0), jnp.minimum(gy + 1, ny - 1)
        z_at = [jnp.maximum(gz - 1, 0), gz, jnp.minimum(gz + 1, nz - 1)]

        def vector(dev):
            return jnp.concatenate([R["x3"][p, pl.ds(dev, 1), :] for p in range(planes)], axis=1)

        for i in range(slabs3):
            partner = jnp.where(gx == 0, i >= n3, i < 2)
            px = jnp.where(partner, 1 - gx, gx)
            xx = jnp.where(gx == 0, i - jnp.where(i >= n3, n3, 0), i - 2 + jnp.where(i < 2, n3, 0))
            lo, mid, hi = (lane_w == xx * n3 + rows for rows in (lo_rows, mid_rows, hi_rows))
            for d in range(3):
                at_y = lambda g: vector(z_at[d] * plane + px * ny + g)
                first = jnp.where(mid, at_y(gy), jnp.where(lo, at_y(y_below), 0.0))
                second = jnp.where(hi, at_y(y_above), 0.0)
                R["lhs"][d, 16 * i : 16 * i + 8, :] = first
                R["lhs"][d, 16 * i + 8 : 16 * i + 16, :] = second
        l, c = iota((wide, 128), 1), iota((wide, 128), 0)
        table = jnp.where((l < B) & ((c & 7) == (l >> SPLIT)) & (c < groups * 8), 1.0, 0.0).astype(BF16)
        v = picked(R["lhs"][...].reshape(3 * slabs3 * 16, wide), table).reshape(3, slabs3, 16, 128)
        v = v[1] + roll(v[2].reshape(slabs3 * 16, 128), B).reshape(slabs3, 16, 128) + roll(
            v[0].reshape(slabs3 * 16, 128), -B).reshape(slabs3, 16, 128)
        u = R["u2"]
        shift = lv2.h - 4
        for i in range(slabs3):
            m = n3 + 4
            u[i, pl.ds(shift, m, stride=2), :] = v[i, 0:m]
            u[i, pl.ds(shift + 1, m, stride=2), :] = v[i, 0:m]

        add_up(lv2)
        relax(lv2, "b", "a", 4)
        relax(lv2, "a", "b", 2)

        def coarse_of(nxt, ref):
            a0 = 1 + gx * (nxt.h - 2)
            return lambda j, m: R[ref][a0 + j, nxt.first - 2 : nxt.first - 2 + m, :]

        prolong(lv1, coarse_of(lv2, "b2"))
        add_up(lv1)
        relax(lv1, "b", "a", 4)
        relax(lv1, "a", "b", 2)
        prolong(lv0, coarse_of(lv1, "b1"))
        add_up(lv0)
        relax(lv0, "b", "a", 4)
        relax(lv0, "a", "b", 2)

        def image(x, sums):
            upper, lower = sums
            a = start_of(lv0) + x
            c, v = beside_of(lv0, R["b0"], a)
            s = R["s0"][a, 8 : 8 + lv0.rows, :]
            ap = (6.0 + s) * c - v
            R["ap"][x] = ap
            c = jnp.where(R["own"][...] > 0.0, c, 0.0)
            return upper + R["f0"][a, 8 : 8 + lv0.rows, :] * c, lower + ap * c

        zero = jnp.zeros((lv0.rows, 128), F32)
        upper, lower = loop(B, image, (zero, zero), lv0.unroll)
        upper, lower = (jnp.sum(v, axis=0, keepdims=True) for v in (upper, lower))
        half = iota((1, 128), 1) < 64
        gather_start("gr", [jnp.where(half, upper, roll(lower, 64))])
        gather_end("gr")
        v = jnp.sum(R["gr"][0], axis=0)
        half = iota((8, 128), 1) < 64
        sums = [total(jnp.where(half, v, 0.0)), total(jnp.where(half, 0.0, v))]
        step_length = sums[0] / sums[1]

        def finish(x, c):
            a = start_of(lv0) + x
            p = R["b0"][a, lv0.first : lv0.first + B, :]
            f = R["f0"][a, lv0.first : lv0.first + B, :]
            q = R["ap"][x, lv0.h : lv0.h + B, :]
            sol_ref[x] = R["sgr"][x] + (step_length * p)[:, 0:B]
            res_ref[x] = (f - step_length * q)[:, 0:B]
            return c

        loop(B, finish, 0, 12)
        for name in exchanges:
            if name != "sg":
                sent(name)
        for name in ("gs", "gf", "gr"):
            gather_sent(name)

    return kernel, list(scratch.values())


def solution(mesh):
    sizes = tuple(mesh.shape[a] for a in AXES)

    def body(right_side, start_guess, reaction):
        kernel, scratch = make_kernel(sizes, right_side.shape)
        out = jax.ShapeDtypeStruct(right_side.shape, F32)
        return tuple(
            pl.pallas_call(
                kernel,
                out_shape=(out, out),
                in_specs=[pl.BlockSpec(memory_space=pl.ANY)] * 3,
                out_specs=(pl.BlockSpec(memory_space=pltpu.VMEM),) * 2,
                scratch_shapes=scratch,
                compiler_params=pltpu.CompilerParams(
                    collective_id=0, has_side_effects=True, vmem_limit_bytes=51 * 2**20
                ),
                name="cg_step",
            )(right_side, start_guess, reaction)
        )

    placed = P(*AXES)
    return jax.shard_map(
        body, mesh=mesh, in_specs=(placed,) * 3, out_specs=(placed,) * 2, check_vma=False
    )
```

```python
import jax
import jax.numpy as jnp
from jax import lax
from jax.experimental import pallas as pl
from jax.experimental.pallas import tpu as pltpu
from jax.sharding import PartitionSpec as P

BOTTOM_ITERS = 6
AXES = ("gx", "gy", "gz")
MESH = pl.DeviceIdType.MESH
F32 = jnp.float32
BF16 = jnp.bfloat16
DAMPING = 6.0 / 7.0
KEEP = 1.0 / 7.0
SPLIT = 3
HALO = (4, 5, 5)


def loop(n, f, carry=0, unroll=4):
    unroll = min(unroll, n)
    while n % unroll:
        unroll -= 1

    def step(i, c):
        for k in range(unroll):
            c = f(i * unroll + k, c)
        return c

    return lax.fori_loop(0, n // unroll, step, carry)


def iota(shape, axis):
    return lax.broadcasted_iota(jnp.int32, shape, axis)


def roll(v, shift, axis=1):
    shift = shift % v.shape[axis] if isinstance(shift, int) else shift
    return v if isinstance(shift, int) and shift == 0 else pltpu.roll(v, shift, axis)


def halves(v):
    high = v.astype(BF16)
    low = (v - high.astype(F32)).astype(BF16)
    return high, low


def picked(v, table):
    high, low = halves(v)
    return jnp.dot(high, table, preferred_element_type=F32) + jnp.dot(low, table, preferred_element_type=F32)


def total(v):
    v = jnp.sum(v, axis=0, keepdims=True)
    return jnp.sum(v, axis=1, keepdims=True)


class Level:
    def __init__(self, k, block):
        self.k = k
        self.n = block >> k
        self.h = HALO[k]
        self.r = 1 << k
        self.q = 0.25**k
        self.tiles = -(-(self.n + 2 * self.h) // 8)
        self.rows = 8 * self.tiles
        self.slabs = self.n + self.h
        self.first = 8 + self.h
        self.unroll = 52 if k == 0 else 28
        self.shape = (self.slabs + 2, self.rows + 16, 128)


def make_kernel(sizes, block):
    nx, ny, nz = sizes
    B = block[0]
    levels = [Level(k, B) for k in range(SPLIT)]
    n3 = B >> SPLIT
    groups = n3 * n3
    planes = -(-groups * 8 // 128)
    packed = -(-groups * n3 // 128)
    q3, q4 = 0.25**3, 0.25**4
    line = nz
    plane = nx * ny

    scratch = {}
    for name in ("rsr", "sgr", "rer"):
        scratch[name] = pltpu.VMEM((B, B, B), F32)
    scratch["insem"] = pltpu.SemaphoreType.DMA((3,))
    exchanges = {}

    def add_exchange(name, k, field, t, wide):
        lv = levels[k]
        per = 128 // (t * lv.r)
        ex = dict(lv=lv, field=field, t=t, wide=wide, per=per, pairs=lv.n // 2, groups=-(-lv.n // per))
        for d in ("s", "r"):
            scratch[f"y{d}_{name}"] = pltpu.VMEM((3, ex["pairs"], t, 128), F32)
            scratch[f"z{d}_{name}"] = pltpu.VMEM((2, ex["groups"], lv.rows, 128), F32)
        if wide:
            scratch[f"yx_{name}"] = pltpu.VMEM((3, t, t, 128), F32)
            scratch[f"zx_{name}"] = pltpu.VMEM((2, lv.rows, 128), F32)
        scratch[f"send_{name}"] = pltpu.SemaphoreType.DMA
        scratch[f"recv_{name}"] = pltpu.SemaphoreType.DMA
        exchanges[name] = ex

    for lv in levels:
        k = lv.k
        for name in ("f", "s", "w", "e", "a", "b"):
            scratch[f"{name}{k}"] = pltpu.VMEM(lv.shape, F32)
        scratch[f"vm{k}"] = pltpu.VMEM((lv.rows, 128), F32)
        scratch[f"t{k}"] = pltpu.VMEM((lv.n // 2, lv.rows, 128), F32)
        scratch[f"u{k}"] = pltpu.VMEM((lv.slabs // 2 + 1, lv.rows + 16, 128), F32)
        add_exchange(f"f{k}", k, f"f{k}", lv.h, True)
        add_exchange(f"s{k}", k, f"s{k}", lv.h, True)
    scratch["sg"] = pltpu.VMEM(levels[0].shape, F32)
    add_exchange("sg", 0, "sg", 1, False)
    scratch["ap"] = pltpu.VMEM((B, levels[0].rows, 128), F32)
    scratch["own"] = pltpu.VMEM((levels[0].rows, 128), F32)
    for name, count in (("gs", packed), ("gf", packed), ("gr", 1)):
        scratch[name] = pltpu.VMEM((count, line + 1, plane, 128), F32)
        scratch[f"{name}_send"] = pltpu.SemaphoreType.DMA
        scratch[f"{name}_recv"] = pltpu.SemaphoreType.DMA
    scratch["count"] = pltpu.VMEM((1024, 128), F32)
    for name in ("k2", "k3", "k4", "k5"):
        scratch[name] = pltpu.SemaphoreType.REGULAR
    scratch["l3"] = pltpu.VMEM((n3, 8, 128), F32)
    for name in ("s3", "f3", "w3", "e3"):
        scratch[name] = pltpu.VMEM((planes * 128, 128), F32)
    scratch["x3"] = pltpu.VMEM((planes, plane * line + 8, 128), F32)
    scratch["lhs"] = pltpu.VMEM((3, (n3 + 2) * 16, planes * 128), F32)

    names = list(scratch)

    def kernel(rs_ref, sg_ref, re_ref, sol_ref, res_ref, *refs):
        R = dict(zip(names, refs))
        gx, gy, gz = (lax.axis_index(a) for a in AXES)
        mine = gx * ny + gy

        inputs = [
            pltpu.make_async_copy(src, R[dst], R["insem"].at[i])
            for i, (src, dst) in enumerate(((sg_ref, "sgr"), (re_ref, "rer"), (rs_ref, "rsr")))
        ]
        for copy in inputs:
            copy.start()

        def start_of(lv):
            return 1 + gx * lv.h

        for lv in levels:
            k = lv.k

            def blank(a, c, k=k, lv=lv):
                for name in ("f", "s"):
                    ref = R[f"{name}{k}"]
                    ref[a, 8:16, :] = jnp.zeros((8, 128), F32)
                    low = (lv.first + lv.n) // 8 * 8
                    ref[a, low : 8 + lv.rows, :] = jnp.zeros((8 + lv.rows - low, 128), F32)
                if k == 0:
                    ref = R["sg"]
                    ref[a, 8:16, :] = jnp.zeros((8, 128), F32)
                    ref[a, low : 8 + lv.rows, :] = jnp.zeros((8 + lv.rows - low, 128), F32)
                return c

            loop(lv.shape[0], blank, 0, 2)

        for name, ex in exchanges.items():
            for m in ("yr", "yx", "zr", "zx") if ex["wide"] else ("yr", "zr"):
                ref = R[f"{m}_{name}"]
                ref[...] = jnp.zeros(ref.shape, F32)

        barrier = pltpu.get_barrier_semaphore()
        others = []
        for dz in range(nz):
            for dx in range(nx):
                for dy in range(ny):
                    if dx or dy or dz:
                        others.append((dx, dy, dz))

        def hops(to):
            dx, dy, dz = to
            return dx + min(dy, ny - dy) + min(dz % 4, 4 - dz % 4) + min(dz // 4, nz // 4 - dz // 4)

        others.sort(key=lambda to: (-hops(to), to))

        def device(dx, dy, dz):
            return {"gx": lax.rem(gx + dx, nx), "gy": lax.rem(gy + dy, ny), "gz": lax.rem(gz + dz, nz)}

        faces = [(1, 0, 0), (0, 1, 0), (0, ny - 1, 0), (0, 0, 1), (0, 0, nz - 1)]
        two = nz // 8
        waves = {
            "k2": faces,
            "k3": faces[:3] + [(0, 0, two), (0, 0, nz - two)],
            "k4": [(0, 0, 2 * two), (0, 0, nz - 2 * two)],
            "k5": [to for to in others if to[2] == 0],
        }

        def greet(name):
            for to in waves[name]:
                pl.semaphore_signal(R[name], inc=1, device_id=device(*to), device_id_type=MESH)

        def greeted(name):
            pl.semaphore_wait(R[name], len(waves[name]))

        for to in faces:
            pl.semaphore_signal(barrier, inc=1, device_id=device(*to), device_id_type=MESH)

        for lv in levels:
            k = lv.k
            z8 = jnp.zeros((8, 128), F32)
            zs = jnp.zeros((lv.rows, 128), F32)
            fields = ["e", "a", "b"] + (["sg"] if k == 0 else [])
            fields = [R[f if f == "sg" else f"{f}{k}"] for f in fields]

            def guard(a, c, fields=fields, lv=lv, z8=z8):
                for ref in fields:
                    ref[a, 0:8, :] = z8
                    ref[a, 8 + lv.rows : 16 + lv.rows, :] = z8
                return c

            loop(lv.shape[0], guard, 0, 2)
            for ref in fields:
                ref[0, 8 : 8 + lv.rows, :] = zs
                ref[lv.slabs + 1, 8 : 8 + lv.rows, :] = zs

            lane, row = iota((lv.rows, 128), 1), iota((lv.rows, 128), 0)
            wd = lv.h * lv.r
            ok = (lane < B) | ((lane < B + wd) & (gz < nz - 1)) | ((lane >= 128 - wd) & (gz > 0))
            ok = ok & (row >= jnp.where(gy > 0, 0, lv.h))
            ok = ok & (row < lv.n + lv.h + jnp.where(gy < ny - 1, lv.h, 0))
            R[f"vm{k}"][...] = jnp.where(ok, 1.0, 0.0)
            if k == 0:
                own = (lane < B) & (row >= lv.h) & (row < lv.h + lv.n)
                R["own"][...] = jnp.where(own, 1.0, 0.0)

        def messages(name):
            ex = exchanges[name]
            lv, t, m = ex["lv"], ex["t"], ex["pairs"]
            f = R[ex["field"]]
            src = jnp.where(gx == 0, 1 + lv.n - t, 1 + lv.h)
            dst = jnp.where(gx == 0, 1 + lv.h - t, 1 + lv.n)
            rows = pl.ds(lv.first, lv.n)
            own = pl.ds(lv.h, lv.n)
            ys, yr, zs, zr = (R[f"{c}_{name}"] for c in ("ys", "yr", "zs", "zr"))
            out = [(f.at[pl.ds(src, t), rows, :], f.at[pl.ds(dst, t), rows, :], 1, 0, 0)]
            for i, way in enumerate((-1, 1)):
                out.append((ys.at[i], yr.at[1 - i], 0, way, 0))
                out.append((zs.at[i, :, own, :], zr.at[1 - i, :, own, :], 0, 0, way))
            if ex["wide"]:
                yx, zx = R[f"yx_{name}"], R[f"zx_{name}"]
                pair = jnp.where(gx == 0, m - t, 0)
                group = jnp.where(gx == 0, ex["groups"] - 1, 0)
                for i, way in enumerate((-1, 1)):
                    out.append((ys.at[i, pl.ds(pair, t)], yx.at[1 - i], 1, way, 0))
                    out.append((zs.at[i, group, own, :], zx.at[1 - i, own, :], 1, 0, way))
                    for yway in (-1, 1):
                        here = pl.ds(lv.h if yway < 0 else lv.h + lv.n - t, t)
                        there = pl.ds(lv.h + lv.n if yway < 0 else lv.h - t, t)
                        out.append((zs.at[i, :, here, :], zr.at[1 - i, :, there, :], 0, yway, way))
                        out.append((zs.at[i, group, here, :], zx.at[1 - i, there, :], 1, yway, way))
            return out

        def guarded(cond, f):
            if cond is None:
                f()
            else:
                pl.when(cond)(f)

        def send(name, only=None):
            batch = [m for m in messages(name) if only is None or only(*m[2:])]
            batch.sort(key=lambda m: -(m[2] + abs(m[3]) + 2 * abs(m[4])))
            for src, dst, ox, oy, oz in batch:
                copy = pltpu.make_async_remote_copy(
                    src_ref=src, dst_ref=dst, send_sem=R[f"send_{name}"], recv_sem=R[f"recv_{name}"],
                    device_id=device(ox, oy % ny, oz % nz), device_id_type=MESH)
                cond = None
                for at, n, way in ((gy, ny, oy), (gz, nz, oz)):
                    if way:
                        there = at > 0 if way < 0 else at < n - 1
                        cond = there if cond is None else cond & there
                guarded(cond, copy.start)

        def counted(size, send_sem, recv_sem):
            rows = R["count"].at[pl.ds(0, size), :]
            return pltpu.make_async_remote_copy(
                src_ref=rows, dst_ref=rows, send_sem=send_sem, recv_sem=recv_sem,
                device_id=device(1, 0, 0), device_id_type=MESH)

        def in_all(name, getting):
            sizes = [(src.shape, oy, oz) for src, _, _, oy, oz in messages(name)]
            for y, at_y in ((0, gy == 0), (1, (gy > 0) & (gy < ny - 1)), (2, gy == ny - 1)):
                for z, at_z in ((0, gz == 0), (1, (gz > 0) & (gz < nz - 1)), (2, gz == nz - 1)):
                    rows = 0
                    for shape, oy, oz in sizes:
                        oy, oz = (-oy, -oz) if getting else (oy, oz)
                        if y + oy in (0, 1, 2) and z + oz in (0, 1, 2):
                            count = 1
                            for d in shape[:-1]:
                                count *= d
                            rows += count
                    copy = counted(rows, R[f"send_{name}"], R[f"recv_{name}"])
                    pl.when(at_y & at_z)(copy.wait_recv if getting else copy.wait_send)

        def arrive(name):
            in_all(name, True)

        def sent(name):
            in_all(name, False)

        def y_pack(name):
            ex = exchanges[name]
            lv, t, m = ex["lv"], ex["t"], ex["pairs"]
            f, a = R[ex["field"]], start_of(lv)
            lane = iota((t, 128), 1)
            for side, row in ((0, lv.first), (1, lv.first + lv.n - t)):
                for i in range(m):
                    v = f[a + i, row : row + t, :]
                    R[f"ys_{name}"][side, i] = jnp.where(lane < 64, v, roll(f[a + i + m, row : row + t, :], 64))

        def y_unpack(name):
            ex = exchanges[name]
            lv, t, m = ex["lv"], ex["t"], ex["pairs"]
            f, a = R[ex["field"]], start_of(lv)
            keep = iota((t, 128), 1) < B
            edge = jnp.where(gx == 0, 1 + lv.n, 1)
            for side, row, ok in ((0, lv.first - t, gy > 0), (1, lv.first + lv.n, gy < ny - 1)):
                for i in range(m):
                    v = R[f"yr_{name}"][side, i]
                    v = v if ex["wide"] else jnp.where(ok, v, 0.0)
                    f[a + i, row : row + t, :] = jnp.where(keep, v, 0.0)
                    f[a + i + m, row : row + t, :] = jnp.where(keep, roll(v, 64), 0.0)
                if ex["wide"]:
                    for i in range(t):
                        v = pltpu.roll(R[f"yx_{name}"][side, i], gx * 64, 1)
                        f[edge + i, row : row + t, :] = jnp.where(keep, v, 0.0)

        def z_pack(name):
            ex = exchanges[name]
            lv, per = ex["lv"], ex["per"]
            wd = ex["t"] * lv.r
            f, a = R[ex["field"]], start_of(lv)
            lane = iota((lv.rows, 128), 1)
            for g in range(ex["groups"]):
                low = high = None
                count = min(per, lv.n - g * per)
                for j in reversed(range(count)):
                    v = f[a + g * per + j, 8 : 8 + lv.rows, :]
                    c = j * wd
                    one, two = roll(v, c), roll(v, c - (B - wd))
                    low = one if low is None else jnp.where(lane < c + wd, one, low)
                    high = two if high is None else jnp.where(lane < c + wd, two, high)
                R[f"zs_{name}"][0, g] = low
                R[f"zs_{name}"][1, g] = high

        def pack_send(name):
            send(name, lambda ox, oy, oz: not oy and not oz)
            z_pack(name)
            send(name, lambda ox, oy, oz: oz)
            y_pack(name)
            send(name, lambda ox, oy, oz: oy and not oz)

        def z_unpacked(name, use):
            ex = exchanges[name]
            lv, per, t = ex["lv"], ex["per"], ex["t"]
            wd = t * lv.r
            f, a = R[ex["field"]], start_of(lv)
            lane = iota((lv.rows, 128), 1)

            def put(i, below, above):
                if not ex["wide"]:
                    below, above = jnp.where(gz > 0, below, 0.0), jnp.where(gz < nz - 1, above, 0.0)
                v = jnp.where(lane < B + wd, above, jnp.where(lane >= 128 - wd, below, 0.0))
                use(i, jnp.where(lane < B, f[i, 8 : 8 + lv.rows, :], v))

            for j in range(lv.n):
                g, c = j // per, j % per * wd
                put(a + j, roll(R[f"zr_{name}"][0, g], -wd - c), roll(R[f"zr_{name}"][1, g], B - c))
            if ex["wide"]:
                edge = jnp.where(gx == 0, 1 + lv.n, 1)
                for j in range(t):
                    c0, c1 = j * wd, (lv.n - t + j - (ex["groups"] - 1) * per) * wd
                    one = jnp.where(gx == 0, (-wd - c0) % 128, (-wd - c1) % 128)
                    two = jnp.where(gx == 0, (B - c0) % 128, (B - c1) % 128)
                    put(edge + j, pltpu.roll(R[f"zx_{name}"][0], one, 1), pltpu.roll(R[f"zx_{name}"][1], two, 1))

        def beside_of(lv, ref, a):
            rows = lv.rows
            c = ref[a, 8 : 8 + rows, :]
            v = ref[a + 1, 8 : 8 + rows, :] + ref[a - 1, 8 : 8 + rows, :]
            v = v + (ref[a, 9 : 9 + rows, :] + ref[a, 7 : 7 + rows, :])
            return c, v + (roll(c, lv.r) + roll(c, -lv.r))

        def span(lv, far):
            return lv.n + far, 1 + gx * (lv.h - far)

        def relax(lv, src, dst, far):
            k = lv.k
            count, a0 = span(lv, far)

            def one(i, carry):
                a = a0 + i
                c, v = beside_of(lv, R[f"{src}{k}"], a)
                w = R[f"w{k}"][a, 8 : 8 + lv.rows, :]
                e = R[f"e{k}"][a, 8 : 8 + lv.rows, :]
                R[f"{dst}{k}"][a, 8 : 8 + lv.rows, :] = c * KEEP + (e + w * v)
                return carry

            loop(count, one, 0, lv.unroll)

        def weigh(lv):
            k = lv.k
            vm = R[f"vm{k}"]

            def use(i, s):
                R[f"w{k}"][i, 8 : 8 + lv.rows, :] = vm[...] * ((DAMPING * lv.q) / (6.0 * lv.q + s))

            z_unpacked(f"s{k}", use)

        def begin(lv):
            k = lv.k
            scale = 1.0 / lv.q

            def use(i, f):
                w = R[f"w{k}"][i, 8 : 8 + lv.rows, :]
                R[f"e{k}"][i, 8 : 8 + lv.rows, :] = (w * scale) * f if k else w * f

            z_unpacked(f"f{k}", use)

        def restrict(lv, of, name):
            k = lv.k
            a0 = start_of(lv)
            half = lv.n // 2
            lane = iota((lv.rows, 128), 1)
            t = R[f"t{k}"]

            def one(j, c):
                v = of(a0 + 2 * j) + of(a0 + 2 * j + 1)
                v = v + jnp.where((lane & lv.r) == 0, roll(v, -lv.r), roll(v, lv.r))
                t[j] = v
                return c

            loop(half, one, 0, lv.unroll // 2)
            wide = iota((half, 128), 1) < B

            def two(j, c):
                v = t[j, pl.ds(lv.h, half, stride=2), :] + t[j, pl.ds(lv.h + 1, half, stride=2), :]
                v = jnp.where(wide, 0.125 * v, 0.0)
                if k + 1 < SPLIT:
                    nxt = levels[k + 1]
                    R[f"{name}{k + 1}"][start_of(nxt) + j, nxt.first : nxt.first + half, :] = v
                else:
                    R["l3"][j, 0:half, :] = v
                return c

            loop(half, two, 0, 12)

        def left_of(lv, src):
            k = lv.k

            def f(a):
                c, v = beside_of(lv, R[f"{src}{k}"], a)
                s = R[f"s{k}"][a, 8 : 8 + lv.rows, :]
                return R[f"f{k}"][a, 8 : 8 + lv.rows, :] - ((6.0 * lv.q + s) * c - lv.q * v)

            return f

        def coefficient(lv):
            return lambda a: R[f"s{lv.k}"][a, 8 : 8 + lv.rows, :]

        def prolong(lv, coarse_rows):
            k = lv.k
            nxt_far = 2
            half = lv.n // 2
            m = half + 2 * nxt_far
            shift = lv.h - 2 * nxt_far
            u = R[f"u{k}"]

            def put(j, c):
                v = coarse_rows(j, m)
                u[j, pl.ds(shift, m, stride=2), :] = v
                u[j, pl.ds(shift + 1, m, stride=2), :] = v
                return c

            loop(half + nxt_far, put, 0, 7)

        def add_up(lv):
            k = lv.k
            a0 = 1 + gx * (lv.h - 4)

            def one(j, c):
                p = R[f"u{k}"][j, 0 : lv.rows, :]
                if k:
                    row = iota((lv.rows, 128), 0)
                    p = jnp.where((row >= lv.h - 4) & (row < lv.h + lv.n + 4), p, 0.0)
                if k == SPLIT - 1:
                    p = jnp.where(R[f"vm{k}"][...] > 0.0, p, 0.0)
                for d in range(2):
                    a = a0 + 2 * j + d
                    R[f"b{k}"][a, 8 : 8 + lv.rows, :] = R[f"a{k}"][a, 8 : 8 + lv.rows, :] + p
                return c

            loop((lv.n + 4) // 2, one, 0, 7)

        def gather_copy(name, dx, dy, dz):
            g = R[name]
            here = g.at[:, gz, pl.ds(mine, 1), :]
            return pltpu.make_async_remote_copy(
                src_ref=here, dst_ref=here, send_sem=R[f"{name}_send"], recv_sem=R[f"{name}_recv"],
                device_id=device(dx, dy, dz), device_id_type=MESH)

        def gather_start(name, rows):
            for p, v in enumerate(rows):
                R[name][p, gz, pl.ds(mine, 1), :] = v
            for to in others:
                gather_copy(name, *to).start()

        def gathered(name):
            size = len(others) * R[name].shape[0]
            return counted(size, R[f"{name}_send"], R[f"{name}_recv"])

        def gather_end(name):
            gathered(name).wait_recv()

        def gather_sent(name):
            gathered(name).wait_send()

        def local_vector():
            wide = packed * 128
            v = R["l3"][...].reshape(n3 * 8, 128)
            l, c = iota((128, wide), 0), iota((128, wide), 1)
            table = jnp.where((l == c % n3 * (1 << SPLIT)) & (c < groups * n3), 1.0, 0.0).astype(BF16)
            v = picked(v, table)
            row, c = iota((n3 * 8, wide), 0), iota((n3 * 8, wide), 1)
            keep = ((row & 7) < n3) & (c // n3 == (row >> 3) * n3 + (row & 7))
            v = jnp.sum(jnp.where(keep, v, 0.0), axis=0, keepdims=True)
            return [v[:, 128 * p : 128 * p + 128] for p in range(packed)]

        def by_device(name, dst):
            for p in range(packed):
                v = R[name][p, 0:line].reshape(plane * line, 128)
                R[dst][128 * p : 128 * p + 128, :] = v.T

        lv0, lv1, lv2 = levels
        inside = jnp.zeros((B, 128 - B), F32)

        def take(raw, dst):
            def one(x, c):
                v = jnp.concatenate([R[raw][x], inside], axis=1)
                R[dst][start_of(lv0) + x, lv0.first : lv0.first + B, :] = v
                return c

            loop(B, one, 0, 4)

        R["l3"][...] = jnp.zeros((n3, 8, 128), F32)
        inputs[0].wait()
        take("sgr", "sg")
        y_pack("sg")
        z_pack("sg")
        inputs[1].wait()
        take("rer", "s0")
        y_pack("s0")
        z_pack("s0")
        pl.semaphore_wait(barrier, len(faces))
        send("sg")
        greet("k2")
        send("s0", lambda *to: sum(map(abs, to)) == 1)
        inputs[2].wait()
        take("rsr", "f0")
        restrict(lv0, coefficient(lv0), "s")
        greeted("k2")
        greet("k3")
        y_pack("s1")
        z_pack("s1")
        restrict(lv1, coefficient(lv1), "s")
        y_pack("s2")
        z_pack("s2")
        greeted("k3")
        greet("k4")
        send("s0", lambda *to: sum(map(abs, to)) > 1)
        restrict(lv2, coefficient(lv2), "s")
        vector3 = local_vector()
        arrive("sg")
        sent("sg")
        y_unpack("sg")

        def keep_guess(i, v):
            R["sg"][i, 8 : 8 + lv0.rows, :] = v

        z_unpacked("sg", keep_guess)

        def first_residual(x, carry):
            a = start_of(lv0) + x
            c, v = beside_of(lv0, R["sg"], a)
            s = R["s0"][a, 8 : 8 + lv0.rows, :]
            f = R["f0"][a, 8 : 8 + lv0.rows, :] - ((6.0 + s) * c - v)
            R["f0"][a, 8 : 8 + lv0.rows, :] = jnp.where(R["own"][...] > 0.0, f, 0.0)
            return carry

        loop(B, first_residual, 0, lv0.unroll)
        greeted("k4")
        greet("k5")
        pack_send("f0")
        send("s1")
        send("s2")

        def weigh_at(lv):
            arrive(f"s{lv.k}")
            y_unpack(f"s{lv.k}")
            weigh(lv)

        weigh_at(lv0)
        arrive("f0")
        y_unpack("f0")
        begin(lv0)

        def first_relax(lv):
            k = lv.k
            count, a0 = span(lv, 4)

            def one(i, carry):
                a = a0 + i
                c, v = beside_of(lv, R[f"e{k}"], a)
                w = R[f"w{k}"][a, 8 : 8 + lv.rows, :]
                R[f"a{k}"][a, 8 : 8 + lv.rows, :] = c * (1.0 + KEEP) + w * v
                return carry

            loop(count, one, 0, lv.unroll)

        first_relax(lv0)
        restrict(lv0, left_of(lv0, "a"), "f")

        def deeper(lv, fill):
            name = f"f{lv.k}"
            pack_send(name)
            fill()
            weigh_at(lv)
            arrive(name)
            y_unpack(name)
            begin(lv)
            first_relax(lv)
            restrict(lv, left_of(lv, "a"), "f")

        greeted("k5")
        deeper(lv1, lambda: None)
        deeper(lv2, lambda: gather_start("gs", vector3))
        gather_start("gf", local_vector())

        gather_end("gs")
        by_device("gs", "s3")
        lane8, row8 = iota((8, 128), 1), iota((8, 128), 0)
        dev_y, dev_x, dev_z = lane8 & (ny - 1), (lane8 >> 2) & 1, lane8 >> 3
        step_x, step_z = ny, plane
        has = {
            ("y", 1): dev_y < ny - 1, ("y", -1): dev_y > 0, ("x", 1): dev_x < nx - 1, ("x", -1): dev_x > 0,
            ("z", 1): dev_z < nz - 1, ("z", -1): dev_z > 0,
        }
        strides = {"y": 1, "x": step_x, "z": step_z}

        def across(v, axis, way):
            return jnp.where(has[axis, way], roll(v, -way * strides[axis]), 0.0)

        def around(get, m):
            def one(x, y):
                c = get(x, y)
                r = n3 // m
                up = jnp.where(row8 >= n3 - r, roll(across(c, "z", 1), n3 - r, 0), roll(c, -r, 0))
                dn = jnp.where(row8 < r, roll(across(c, "z", -1), r - n3, 0), roll(c, r, 0))
                v = up + dn
                v = v + (get(x + 1, y) if x + 1 < m else across(get(0, y), "x", 1))
                v = v + (get(x - 1, y) if x else across(get(m - 1, y), "x", -1))
                v = v + (get(x, y + 1) if y + 1 < m else across(get(x, 0), "y", 1))
                v = v + (get(x, y - 1) if y else across(get(x, m - 1), "y", -1))
                return c, v

            return one

        cells = [(x, y) for x in range(n3) for y in range(n3)]
        m4 = n3 // 2
        cells4 = [(x, y) for x in range(m4) for y in range(m4)]
        live = row8 < n3

        def tile(name, x, y):
            g = (x * n3 + y) * (n3 if name in ("s3", "f3") else 8)
            return R[name][g : g + 8, :]

        for x, y in cells:
            R["w3"][8 * (x * n3 + y) : 8 * (x * n3 + y) + 8, :] = jnp.where(
                live, (DAMPING * q3) / (6.0 * q3 + tile("s3", x, y)), 0.0)

        def coarser(get):
            out = {}
            for x, y in cells4:
                v = (get(2 * x, 2 * y) + get(2 * x, 2 * y + 1)) + (get(2 * x + 1, 2 * y) + get(2 * x + 1, 2 * y + 1))
                v = v + jnp.where((row8 & 1) == 0, roll(v, -1, 0), roll(v, 1, 0))
                out[x, y] = jnp.where(live, 0.125 * v, 0.0)
            return out

        s4 = coarser(lambda x, y: tile("s3", x, y))
        gather_end("gf")
        by_device("gf", "f3")
        e = {}
        e0 = {}
        for c in cells:
            e0[c] = (tile("w3", *c) * (1.0 / q3)) * tile("f3", *c)
        op = around(lambda x, y: e0[x, y], n3)
        for c in cells:
            u, v = op(*c)
            e[c] = u * (1.0 + KEEP) + tile("w3", *c) * v
        op = around(lambda x, y: e[x, y], n3)
        rest = {}
        for c in cells:
            u, v = op(*c)
            rest[c] = jnp.where(live, tile("f3", *c) - ((6.0 * q3 + tile("s3", *c)) * u - q3 * v), 0.0)
        f4 = coarser(lambda x, y: rest[x, y])

        def inner(u, v):
            s = None
            for c in cells4:
                s = u[c] * v[c] if s is None else s + u[c] * v[c]
            return total(s)

        r4 = dict(f4)
        p4 = dict(f4)
        e4 = {c: jnp.zeros((8, 128), F32) for c in cells4}
        rr = inner(r4, r4)
        for _ in range(BOTTOM_ITERS):
            op = around(lambda x, y: p4[x, y], m4)
            q = {}
            for c in cells4:
                u, v = op(*c)
                q[c] = jnp.where(live, (6.0 * q4 + s4[c]) * u - q4 * v, 0.0)
            a = rr / inner(p4, q)
            e4 = {c: e4[c] + a * p4[c] for c in cells4}
            r4 = {c: r4[c] - a * q[c] for c in cells4}
            new = inner(r4, r4)
            ratio = new / rr
            p4 = {c: r4[c] + ratio * p4[c] for c in cells4}
            rr = new
        e = {(x, y): e[x, y] + e4[x // 2, y // 2] for x, y in cells}
        for _ in range(2):
            op = around(lambda x, y: e[x, y], n3)
            nxt = {}
            for c in cells:
                u, v = op(*c)
                nxt[c] = u * KEEP + (e0[c] + tile("w3", *c) * v)
            e = nxt
        for x, y in cells:
            g = x * n3 + y
            R["e3"][8 * g : 8 * g + 8, :] = e[x, y]
        R["e3"][groups * 8 :, :] = jnp.zeros((planes * 128 - groups * 8, 128), F32)
        for p in range(planes):
            R["x3"][p, 0:128, :] = R["e3"][128 * p : 128 * p + 128, :].T

        wide = planes * 128
        slabs3 = n3 + 2
        lane_w = iota((8, wide), 1) >> 3
        row_w = iota((8, wide), 0)
        lo_rows = jnp.where(row_w < 2, n3 - 2 + row_w, -1000)
        mid_rows = jnp.where(row_w < 2, -1000, row_w - 2)
        hi_rows = jnp.where(row_w < 2, row_w, -1000)
        y_below, y_above = jnp.maximum(gy - 1, 0), jnp.minimum(gy + 1, ny - 1)
        z_at = [jnp.maximum(gz - 1, 0), gz, jnp.minimum(gz + 1, nz - 1)]

        def vector(dev):
            return jnp.concatenate([R["x3"][p, pl.ds(dev, 1), :] for p in range(planes)], axis=1)

        for i in range(slabs3):
            partner = jnp.where(gx == 0, i >= n3, i < 2)
            px = jnp.where(partner, 1 - gx, gx)
            xx = jnp.where(gx == 0, i - jnp.where(i >= n3, n3, 0), i - 2 + jnp.where(i < 2, n3, 0))
            lo, mid, hi = (lane_w == xx * n3 + rows for rows in (lo_rows, mid_rows, hi_rows))
            for d in range(3):
                at_y = lambda g: vector(z_at[d] * plane + px * ny + g)
                first = jnp.where(mid, at_y(gy), jnp.where(lo, at_y(y_below), 0.0))
                second = jnp.where(hi, at_y(y_above), 0.0)
                R["lhs"][d, 16 * i : 16 * i + 8, :] = first
                R["lhs"][d, 16 * i + 8 : 16 * i + 16, :] = second
        l, c = iota((wide, 128), 1), iota((wide, 128), 0)
        table = jnp.where((l < B) & ((c & 7) == (l >> SPLIT)) & (c < groups * 8), 1.0, 0.0).astype(BF16)
        v = picked(R["lhs"][...].reshape(3 * slabs3 * 16, wide), table).reshape(3, slabs3, 16, 128)
        v = v[1] + roll(v[2].reshape(slabs3 * 16, 128), B).reshape(slabs3, 16, 128) + roll(
            v[0].reshape(slabs3 * 16, 128), -B).reshape(slabs3, 16, 128)
        u = R["u2"]
        shift = lv2.h - 4
        for i in range(slabs3):
            m = n3 + 4
            u[i, pl.ds(shift, m, stride=2), :] = v[i, 0:m]
            u[i, pl.ds(shift + 1, m, stride=2), :] = v[i, 0:m]

        add_up(lv2)
        relax(lv2, "b", "a", 4)
        relax(lv2, "a", "b", 2)

        def coarse_of(nxt, ref):
            a0 = 1 + gx * (nxt.h - 2)
            return lambda j, m: R[ref][a0 + j, nxt.first - 2 : nxt.first - 2 + m, :]

        prolong(lv1, coarse_of(lv2, "b2"))
        add_up(lv1)
        relax(lv1, "b", "a", 4)
        relax(lv1, "a", "b", 2)
        prolong(lv0, coarse_of(lv1, "b1"))
        add_up(lv0)
        relax(lv0, "b", "a", 4)
        relax(lv0, "a", "b", 2)

        def image(x, sums):
            upper, lower = sums
            a = start_of(lv0) + x
            c, v = beside_of(lv0, R["b0"], a)
            s = R["s0"][a, 8 : 8 + lv0.rows, :]
            ap = (6.0 + s) * c - v
            R["ap"][x] = ap
            c = jnp.where(R["own"][...] > 0.0, c, 0.0)
            return upper + R["f0"][a, 8 : 8 + lv0.rows, :] * c, lower + ap * c

        zero = jnp.zeros((lv0.rows, 128), F32)
        upper, lower = loop(B, image, (zero, zero), lv0.unroll)
        upper, lower = (jnp.sum(v, axis=0, keepdims=True) for v in (upper, lower))
        half = iota((1, 128), 1) < 64
        gather_start("gr", [jnp.where(half, upper, roll(lower, 64))])
        gather_end("gr")
        v = jnp.sum(R["gr"][0, 0:line], axis=0)
        half = iota((8, 128), 1) < 64
        sums = [total(jnp.where(half, v, 0.0)), total(jnp.where(half, 0.0, v))]
        step_length = sums[0] / sums[1]

        def finish(x, c):
            a = start_of(lv0) + x
            p = R["b0"][a, lv0.first : lv0.first + B, :]
            f = R["f0"][a, lv0.first : lv0.first + B, :]
            q = R["ap"][x, lv0.h : lv0.h + B, :]
            sol_ref[x] = R["sgr"][x] + (step_length * p)[:, 0:B]
            res_ref[x] = (f - step_length * q)[:, 0:B]
            return c

        loop(B, finish, 0, 12)
        for name in exchanges:
            if name != "sg":
                sent(name)
        for name in ("gs", "gf", "gr"):
            gather_sent(name)

    return kernel, list(scratch.values())


def solution(mesh):
    sizes = tuple(mesh.shape[a] for a in AXES)

    def body(right_side, start_guess, reaction):
        kernel, scratch = make_kernel(sizes, right_side.shape)
        out = jax.ShapeDtypeStruct(right_side.shape, F32)
        return tuple(
            pl.pallas_call(
                kernel,
                out_shape=(out, out),
                in_specs=[pl.BlockSpec(memory_space=pl.ANY)] * 3,
                out_specs=(pl.BlockSpec(memory_space=pltpu.VMEM),) * 2,
                scratch_shapes=scratch,
                compiler_params=pltpu.CompilerParams(
                    collective_id=0, has_side_effects=True, vmem_limit_bytes=51 * 2**20
                ),
                name="cg_step",
            )(right_side, start_guess, reaction)
        )

    placed = P(*AXES)
    return jax.shard_map(
        body, mesh=mesh, in_specs=(placed,) * 3, out_specs=(placed,) * 2, check_vma=False
    )
```

```python
import jax
import jax.numpy as jnp
from jax import lax
from jax.experimental import pallas as pl
from jax.experimental.pallas import tpu as pltpu
from jax.sharding import PartitionSpec as P

BOTTOM_ITERS = 6
AXES = ("gx", "gy", "gz")
MESH = pl.DeviceIdType.MESH
F32 = jnp.float32
BF16 = jnp.bfloat16
DAMPING = 6.0 / 7.0
KEEP = 1.0 / 7.0
SPLIT = 3
HALO = (4, 5, 5)


def loop(n, f, carry=0, unroll=4):
    unroll = min(unroll, n)
    while n % unroll:
        unroll -= 1

    def step(i, c):
        for k in range(unroll):
            c = f(i * unroll + k, c)
        return c

    return lax.fori_loop(0, n // unroll, step, carry)


def iota(shape, axis):
    return lax.broadcasted_iota(jnp.int32, shape, axis)


def roll(v, shift, axis=1):
    shift = shift % v.shape[axis] if isinstance(shift, int) else shift
    return v if isinstance(shift, int) and shift == 0 else pltpu.roll(v, shift, axis)


def halves(v):
    high = v.astype(BF16)
    low = (v - high.astype(F32)).astype(BF16)
    return high, low


def picked(v, table):
    high, low = halves(v)
    return jnp.dot(high, table, preferred_element_type=F32) + jnp.dot(low, table, preferred_element_type=F32)


def total(v):
    v = jnp.sum(v, axis=0, keepdims=True)
    return jnp.sum(v, axis=1, keepdims=True)


class Level:
    def __init__(self, k, block):
        self.k = k
        self.n = block >> k
        self.h = HALO[k]
        self.r = 1 << k
        self.q = 0.25**k
        self.tiles = -(-(self.n + 2 * self.h) // 8)
        self.rows = 8 * self.tiles
        self.slabs = self.n + self.h
        self.first = 8 + self.h
        self.unroll = 52 if k == 0 else 28
        self.shape = (self.slabs + 2, self.rows + 16, 128)


def make_kernel(sizes, block):
    nx, ny, nz = sizes
    B = block[0]
    levels = [Level(k, B) for k in range(SPLIT)]
    n3 = B >> SPLIT
    groups = n3 * n3
    planes = -(-groups * 8 // 128)
    packed = -(-groups * n3 // 128)
    q3, q4 = 0.25**3, 0.25**4
    line = nz
    plane = nx * ny

    scratch = {}
    for name in ("rsr", "sgr", "rer"):
        scratch[name] = pltpu.VMEM((B, B, B), F32)
    scratch["insem"] = pltpu.SemaphoreType.DMA((3,))
    exchanges = {}

    def add_exchange(name, k, field, t, wide):
        lv = levels[k]
        per = 128 // (t * lv.r)
        ex = dict(lv=lv, field=field, t=t, wide=wide, per=per, pairs=lv.n // 2, groups=-(-lv.n // per))
        for d in ("s", "r"):
            scratch[f"y{d}_{name}"] = pltpu.VMEM((3, ex["pairs"], t, 128), F32)
            scratch[f"z{d}_{name}"] = pltpu.VMEM((2, ex["groups"], lv.rows, 128), F32)
        if wide:
            scratch[f"yx_{name}"] = pltpu.VMEM((3, t, t, 128), F32)
            scratch[f"zx_{name}"] = pltpu.VMEM((2, lv.rows, 128), F32)
        scratch[f"send_{name}"] = pltpu.SemaphoreType.DMA
        scratch[f"recv_{name}"] = pltpu.SemaphoreType.DMA
        exchanges[name] = ex

    for lv in levels:
        k = lv.k
        for name in ("f", "s", "w", "e", "a", "b"):
            scratch[f"{name}{k}"] = pltpu.VMEM(lv.shape, F32)
        scratch[f"vm{k}"] = pltpu.VMEM((lv.rows, 128), F32)
        scratch[f"t{k}"] = pltpu.VMEM((lv.n // 2, lv.rows, 128), F32)
        scratch[f"u{k}"] = pltpu.VMEM((lv.slabs // 2 + 1, lv.rows + 16, 128), F32)
        add_exchange(f"f{k}", k, f"f{k}", lv.h, True)
        add_exchange(f"s{k}", k, f"s{k}", lv.h, True)
    scratch["sg"] = pltpu.VMEM(levels[0].shape, F32)
    add_exchange("sg", 0, "sg", 1, False)
    scratch["ap"] = pltpu.VMEM((B, levels[0].rows, 128), F32)
    scratch["own"] = pltpu.VMEM((levels[0].rows, 128), F32)
    for name, count in (("gs", packed), ("gf", packed), ("gr", 1)):
        scratch[name] = pltpu.VMEM((count, line + 1, plane, 128), F32)
        scratch[f"{name}_send"] = pltpu.SemaphoreType.DMA
        scratch[f"{name}_recv"] = pltpu.SemaphoreType.DMA
    scratch["count"] = pltpu.VMEM((1024, 128), F32)
    for name in ("k2", "k3", "k4", "k5"):
        scratch[name] = pltpu.SemaphoreType.REGULAR
    scratch["l3"] = pltpu.VMEM((n3, 8, 128), F32)
    for name in ("s3", "f3", "w3", "e3"):
        scratch[name] = pltpu.VMEM((planes * 128, 128), F32)
    scratch["x3"] = pltpu.VMEM((planes, plane * line + 8, 128), F32)
    scratch["lhs"] = pltpu.VMEM((3, (n3 + 2) * 16, planes * 128), F32)

    names = list(scratch)

    def kernel(rs_ref, sg_ref, re_ref, sol_ref, res_ref, *refs):
        R = dict(zip(names, refs))
        gx, gy, gz = (lax.axis_index(a) for a in AXES)
        mine = gx * ny + gy

        inputs = [
            pltpu.make_async_copy(src, R[dst], R["insem"].at[i])
            for i, (src, dst) in enumerate(((sg_ref, "sgr"), (re_ref, "rer"), (rs_ref, "rsr")))
        ]
        for copy in inputs:
            copy.start()

        def start_of(lv):
            return 1 + gx * lv.h

        for lv in levels:
            k = lv.k

            def blank(a, c, k=k, lv=lv):
                for name in ("f", "s"):
                    ref = R[f"{name}{k}"]
                    ref[a, 8:16, :] = jnp.zeros((8, 128), F32)
                    low = (lv.first + lv.n) // 8 * 8
                    ref[a, low : 8 + lv.rows, :] = jnp.zeros((8 + lv.rows - low, 128), F32)
                if k == 0:
                    ref = R["sg"]
                    ref[a, 8:16, :] = jnp.zeros((8, 128), F32)
                    ref[a, low : 8 + lv.rows, :] = jnp.zeros((8 + lv.rows - low, 128), F32)
                return c

            loop(lv.shape[0], blank, 0, 2)

        for name, ex in exchanges.items():
            for m in ("yr", "yx", "zr", "zx") if ex["wide"] else ("yr", "zr"):
                ref = R[f"{m}_{name}"]
                ref[...] = jnp.zeros(ref.shape, F32)

        barrier = pltpu.get_barrier_semaphore()
        others = []
        for dz in range(nz):
            for dx in range(nx):
                for dy in range(ny):
                    if dx or dy or dz:
                        others.append((dx, dy, dz))

        def hops(to):
            dx, dy, dz = to
            return dx + min(dy, ny - dy) + min(dz % 4, 4 - dz % 4) + min(dz // 4, nz // 4 - dz // 4)

        others.sort(key=lambda to: (-hops(to), to))

        def device(dx, dy, dz):
            return {"gx": lax.rem(gx + dx, nx), "gy": lax.rem(gy + dy, ny), "gz": lax.rem(gz + dz, nz)}

        faces = [(1, 0, 0), (0, 1, 0), (0, ny - 1, 0), (0, 0, 1), (0, 0, nz - 1)]
        two = nz // 8
        waves = {
            "k2": faces,
            "k3": faces[:3] + [(0, 0, two), (0, 0, nz - two)],
            "k4": [(0, 0, 2 * two), (0, 0, nz - 2 * two)],
            "k5": [to for to in others if to[2] == 0],
        }

        def greet(name):
            for to in waves[name]:
                pl.semaphore_signal(R[name], inc=1, device_id=device(*to), device_id_type=MESH)

        def greeted(name):
            pl.semaphore_wait(R[name], len(waves[name]))

        for to in faces:
            pl.semaphore_signal(barrier, inc=1, device_id=device(*to), device_id_type=MESH)

        for lv in levels:
            k = lv.k
            z8 = jnp.zeros((8, 128), F32)
            zs = jnp.zeros((lv.rows, 128), F32)
            fields = ["e", "a", "b"] + (["sg"] if k == 0 else [])
            fields = [R[f if f == "sg" else f"{f}{k}"] for f in fields]

            def guard(a, c, fields=fields, lv=lv, z8=z8):
                for ref in fields:
                    ref[a, 0:8, :] = z8
                    ref[a, 8 + lv.rows : 16 + lv.rows, :] = z8
                return c

            loop(lv.shape[0], guard, 0, 2)
            for ref in fields:
                ref[0, 8 : 8 + lv.rows, :] = zs
                ref[lv.slabs + 1, 8 : 8 + lv.rows, :] = zs

            lane, row = iota((lv.rows, 128), 1), iota((lv.rows, 128), 0)
            wd = lv.h * lv.r
            ok = (lane < B) | ((lane < B + wd) & (gz < nz - 1)) | ((lane >= 128 - wd) & (gz > 0))
            ok = ok & (row >= jnp.where(gy > 0, 0, lv.h))
            ok = ok & (row < lv.n + lv.h + jnp.where(gy < ny - 1, lv.h, 0))
            R[f"vm{k}"][...] = jnp.where(ok, 1.0, 0.0)
            if k == 0:
                own = (lane < B) & (row >= lv.h) & (row < lv.h + lv.n)
                R["own"][...] = jnp.where(own, 1.0, 0.0)

        def messages(name):
            ex = exchanges[name]
            lv, t, m = ex["lv"], ex["t"], ex["pairs"]
            f = R[ex["field"]]
            src = jnp.where(gx == 0, 1 + lv.n - t, 1 + lv.h)
            dst = jnp.where(gx == 0, 1 + lv.h - t, 1 + lv.n)
            rows = pl.ds(lv.first, lv.n)
            own = pl.ds(lv.h, lv.n)
            ys, yr, zs, zr = (R[f"{c}_{name}"] for c in ("ys", "yr", "zs", "zr"))
            out = [(f.at[pl.ds(src, t), rows, :], f.at[pl.ds(dst, t), rows, :], 1, 0, 0)]
            for i, way in enumerate((-1, 1)):
                out.append((ys.at[i], yr.at[1 - i], 0, way, 0))
                out.append((zs.at[i, :, own, :], zr.at[1 - i, :, own, :], 0, 0, way))
            if ex["wide"]:
                yx, zx = R[f"yx_{name}"], R[f"zx_{name}"]
                pair = jnp.where(gx == 0, m - t, 0)
                group = jnp.where(gx == 0, ex["groups"] - 1, 0)
                for i, way in enumerate((-1, 1)):
                    out.append((ys.at[i, pl.ds(pair, t)], yx.at[1 - i], 1, way, 0))
                    out.append((zs.at[i, group, own, :], zx.at[1 - i, own, :], 1, 0, way))
                    for yway in (-1, 1):
                        here = pl.ds(lv.h if yway < 0 else lv.h + lv.n - t, t)
                        there = pl.ds(lv.h + lv.n if yway < 0 else lv.h - t, t)
                        out.append((zs.at[i, :, here, :], zr.at[1 - i, :, there, :], 0, yway, way))
                        out.append((zs.at[i, group, here, :], zx.at[1 - i, there, :], 1, yway, way))
            return out

        def guarded(cond, f):
            if cond is None:
                f()
            else:
                pl.when(cond)(f)

        def send(name, only=None):
            batch = [m for m in messages(name) if only is None or only(*m[2:])]
            batch.sort(key=lambda m: -(m[2] + abs(m[3]) + 2 * abs(m[4])))
            for src, dst, ox, oy, oz in batch:
                copy = pltpu.make_async_remote_copy(
                    src_ref=src, dst_ref=dst, send_sem=R[f"send_{name}"], recv_sem=R[f"recv_{name}"],
                    device_id=device(ox, oy % ny, oz % nz), device_id_type=MESH)
                cond = None
                for at, n, way in ((gy, ny, oy), (gz, nz, oz)):
                    if way:
                        there = at > 0 if way < 0 else at < n - 1
                        cond = there if cond is None else cond & there
                guarded(cond, copy.start)

        def counted(size, send_sem, recv_sem):
            rows = R["count"].at[pl.ds(0, size), :]
            return pltpu.make_async_remote_copy(
                src_ref=rows, dst_ref=rows, send_sem=send_sem, recv_sem=recv_sem,
                device_id=device(1, 0, 0), device_id_type=MESH)

        def in_all(name, getting):
            sizes = [(src.shape, oy, oz) for src, _, _, oy, oz in messages(name)]
            for y, at_y in ((0, gy == 0), (1, (gy > 0) & (gy < ny - 1)), (2, gy == ny - 1)):
                for z, at_z in ((0, gz == 0), (1, (gz > 0) & (gz < nz - 1)), (2, gz == nz - 1)):
                    rows = 0
                    for shape, oy, oz in sizes:
                        oy, oz = (-oy, -oz) if getting else (oy, oz)
                        if y + oy in (0, 1, 2) and z + oz in (0, 1, 2):
                            count = 1
                            for d in shape[:-1]:
                                count *= d
                            rows += count
                    copy = counted(rows, R[f"send_{name}"], R[f"recv_{name}"])
                    pl.when(at_y & at_z)(copy.wait_recv if getting else copy.wait_send)

        def arrive(name):
            in_all(name, True)

        def sent(name):
            in_all(name, False)

        def y_pack(name):
            ex = exchanges[name]
            lv, t, m = ex["lv"], ex["t"], ex["pairs"]
            f, a = R[ex["field"]], start_of(lv)
            lane = iota((t, 128), 1)
            for side, row in ((0, lv.first), (1, lv.first + lv.n - t)):
                for i in range(m):
                    v = f[a + i, row : row + t, :]
                    R[f"ys_{name}"][side, i] = jnp.where(lane < 64, v, roll(f[a + i + m, row : row + t, :], 64))

        def y_unpack(name):
            ex = exchanges[name]
            lv, t, m = ex["lv"], ex["t"], ex["pairs"]
            f, a = R[ex["field"]], start_of(lv)
            keep = iota((t, 128), 1) < B
            edge = jnp.where(gx == 0, 1 + lv.n, 1)
            for side, row, ok in ((0, lv.first - t, gy > 0), (1, lv.first + lv.n, gy < ny - 1)):
                for i in range(m):
                    v = R[f"yr_{name}"][side, i]
                    v = v if ex["wide"] else jnp.where(ok, v, 0.0)
                    f[a + i, row : row + t, :] = jnp.where(keep, v, 0.0)
                    f[a + i + m, row : row + t, :] = jnp.where(keep, roll(v, 64), 0.0)
                if ex["wide"]:
                    for i in range(t):
                        v = pltpu.roll(R[f"yx_{name}"][side, i], gx * 64, 1)
                        f[edge + i, row : row + t, :] = jnp.where(keep, v, 0.0)

        def z_pack(name):
            ex = exchanges[name]
            lv, per = ex["lv"], ex["per"]
            wd = ex["t"] * lv.r
            f, a = R[ex["field"]], start_of(lv)
            lane = iota((lv.rows, 128), 1)
            for g in range(ex["groups"]):
                low = high = None
                count = min(per, lv.n - g * per)
                for j in reversed(range(count)):
                    v = f[a + g * per + j, 8 : 8 + lv.rows, :]
                    c = j * wd
                    one, two = roll(v, c), roll(v, c - (B - wd))
                    low = one if low is None else jnp.where(lane < c + wd, one, low)
                    high = two if high is None else jnp.where(lane < c + wd, two, high)
                R[f"zs_{name}"][0, g] = low
                R[f"zs_{name}"][1, g] = high

        def pack_send(name):
            send(name, lambda ox, oy, oz: not oy and not oz)
            z_pack(name)
            send(name, lambda ox, oy, oz: oz)
            y_pack(name)
            send(name, lambda ox, oy, oz: oy and not oz)

        def z_unpacked(name, use):
            ex = exchanges[name]
            lv, per, t = ex["lv"], ex["per"], ex["t"]
            wd = t * lv.r
            f, a = R[ex["field"]], start_of(lv)
            lane = iota((lv.rows, 128), 1)

            def put(i, below, above):
                if not ex["wide"]:
                    below, above = jnp.where(gz > 0, below, 0.0), jnp.where(gz < nz - 1, above, 0.0)
                v = jnp.where(lane < B + wd, above, jnp.where(lane >= 128 - wd, below, 0.0))
                use(i, jnp.where(lane < B, f[i, 8 : 8 + lv.rows, :], v))

            for j in range(lv.n):
                g, c = j // per, j % per * wd
                put(a + j, roll(R[f"zr_{name}"][0, g], -wd - c), roll(R[f"zr_{name}"][1, g], B - c))
            if ex["wide"]:
                edge = jnp.where(gx == 0, 1 + lv.n, 1)
                for j in range(t):
                    c0, c1 = j * wd, (lv.n - t + j - (ex["groups"] - 1) * per) * wd
                    one = jnp.where(gx == 0, (-wd - c0) % 128, (-wd - c1) % 128)
                    two = jnp.where(gx == 0, (B - c0) % 128, (B - c1) % 128)
                    put(edge + j, pltpu.roll(R[f"zx_{name}"][0], one, 1), pltpu.roll(R[f"zx_{name}"][1], two, 1))

        def beside_of(lv, ref, a):
            rows = lv.rows
            c = ref[a, 8 : 8 + rows, :]
            v = ref[a + 1, 8 : 8 + rows, :] + ref[a - 1, 8 : 8 + rows, :]
            v = v + (ref[a, 9 : 9 + rows, :] + ref[a, 7 : 7 + rows, :])
            return c, v + (roll(c, lv.r) + roll(c, -lv.r))

        def span(lv, far):
            return lv.n + far, 1 + gx * (lv.h - far)

        def relax(lv, src, dst, far):
            k = lv.k
            count, a0 = span(lv, far)

            def one(i, carry):
                a = a0 + i
                c, v = beside_of(lv, R[f"{src}{k}"], a)
                w = R[f"w{k}"][a, 8 : 8 + lv.rows, :]
                e = R[f"e{k}"][a, 8 : 8 + lv.rows, :]
                R[f"{dst}{k}"][a, 8 : 8 + lv.rows, :] = c * KEEP + (e + w * v)
                return carry

            loop(count, one, 0, lv.unroll)

        def weigh(lv):
            k = lv.k
            vm = R[f"vm{k}"]

            def use(i, s):
                R[f"w{k}"][i, 8 : 8 + lv.rows, :] = vm[...] * ((DAMPING * lv.q) / (6.0 * lv.q + s))

            z_unpacked(f"s{k}", use)

        def begin(lv):
            k = lv.k
            scale = 1.0 / lv.q

            def use(i, f):
                w = R[f"w{k}"][i, 8 : 8 + lv.rows, :]
                R[f"e{k}"][i, 8 : 8 + lv.rows, :] = (w * scale) * f if k else w * f

            z_unpacked(f"f{k}", use)

        def restrict(lv, of, name):
            k = lv.k
            a0 = start_of(lv)
            half = lv.n // 2
            lane = iota((lv.rows, 128), 1)
            t = R[f"t{k}"]

            def one(j, c):
                v = of(a0 + 2 * j) + of(a0 + 2 * j + 1)
                v = v + jnp.where((lane & lv.r) == 0, roll(v, -lv.r), roll(v, lv.r))
                t[j] = v
                return c

            loop(half, one, 0, lv.unroll // 2)
            wide = iota((half, 128), 1) < B

            def two(j, c):
                v = t[j, pl.ds(lv.h, half, stride=2), :] + t[j, pl.ds(lv.h + 1, half, stride=2), :]
                v = jnp.where(wide, 0.125 * v, 0.0)
                if k + 1 < SPLIT:
                    nxt = levels[k + 1]
                    R[f"{name}{k + 1}"][start_of(nxt) + j, nxt.first : nxt.first + half, :] = v
                else:
                    R["l3"][j, 0:half, :] = v
                return c

            loop(half, two, 0, 24)

        def left_of(lv, src):
            k = lv.k

            def f(a):
                c, v = beside_of(lv, R[f"{src}{k}"], a)
                s = R[f"s{k}"][a, 8 : 8 + lv.rows, :]
                return R[f"f{k}"][a, 8 : 8 + lv.rows, :] - ((6.0 * lv.q + s) * c - lv.q * v)

            return f

        def coefficient(lv):
            return lambda a: R[f"s{lv.k}"][a, 8 : 8 + lv.rows, :]

        def prolong(lv, coarse_rows):
            k = lv.k
            nxt_far = 2
            half = lv.n // 2
            m = half + 2 * nxt_far
            shift = lv.h - 2 * nxt_far
            u = R[f"u{k}"]

            def put(j, c):
                v = coarse_rows(j, m)
                u[j, pl.ds(shift, m, stride=2), :] = v
                u[j, pl.ds(shift + 1, m, stride=2), :] = v
                return c

            loop(half + nxt_far, put, 0, 13)

        def add_up(lv):
            k = lv.k
            a0 = 1 + gx * (lv.h - 4)

            def one(j, c):
                p = R[f"u{k}"][j, 0 : lv.rows, :]
                if k:
                    row = iota((lv.rows, 128), 0)
                    p = jnp.where((row >= lv.h - 4) & (row < lv.h + lv.n + 4), p, 0.0)
                if k == SPLIT - 1:
                    p = jnp.where(R[f"vm{k}"][...] > 0.0, p, 0.0)
                for d in range(2):
                    a = a0 + 2 * j + d
                    R[f"b{k}"][a, 8 : 8 + lv.rows, :] = R[f"a{k}"][a, 8 : 8 + lv.rows, :] + p
                return c

            loop((lv.n + 4) // 2, one, 0, 14)

        def gather_copy(name, dx, dy, dz):
            g = R[name]
            here = g.at[:, gz, pl.ds(mine, 1), :]
            return pltpu.make_async_remote_copy(
                src_ref=here, dst_ref=here, send_sem=R[f"{name}_send"], recv_sem=R[f"{name}_recv"],
                device_id=device(dx, dy, dz), device_id_type=MESH)

        def gather_start(name, rows):
            for p, v in enumerate(rows):
                R[name][p, gz, pl.ds(mine, 1), :] = v
            for to in others:
                gather_copy(name, *to).start()

        def gathered(name):
            size = len(others) * R[name].shape[0]
            return counted(size, R[f"{name}_send"], R[f"{name}_recv"])

        def gather_end(name):
            gathered(name).wait_recv()

        def gather_sent(name):
            gathered(name).wait_send()

        def local_vector():
            wide = packed * 128
            v = R["l3"][...].reshape(n3 * 8, 128)
            l, c = iota((128, wide), 0), iota((128, wide), 1)
            table = jnp.where((l == c % n3 * (1 << SPLIT)) & (c < groups * n3), 1.0, 0.0).astype(BF16)
            v = picked(v, table)
            row, c = iota((n3 * 8, wide), 0), iota((n3 * 8, wide), 1)
            keep = ((row & 7) < n3) & (c // n3 == (row >> 3) * n3 + (row & 7))
            v = jnp.sum(jnp.where(keep, v, 0.0), axis=0, keepdims=True)
            return [v[:, 128 * p : 128 * p + 128] for p in range(packed)]

        def by_device(name, dst):
            for p in range(packed):
                v = R[name][p, 0:line].reshape(plane * line, 128)
                R[dst][128 * p : 128 * p + 128, :] = v.T

        lv0, lv1, lv2 = levels
        inside = jnp.zeros((B, 128 - B), F32)

        def take(raw, dst):
            def one(x, c):
                v = jnp.concatenate([R[raw][x], inside], axis=1)
                R[dst][start_of(lv0) + x, lv0.first : lv0.first + B, :] = v
                return c

            loop(B, one, 0, 4)

        R["l3"][...] = jnp.zeros((n3, 8, 128), F32)
        inputs[0].wait()
        take("sgr", "sg")
        y_pack("sg")
        z_pack("sg")
        inputs[1].wait()
        take("rer", "s0")
        y_pack("s0")
        z_pack("s0")
        pl.semaphore_wait(barrier, len(faces))
        send("sg")
        greet("k2")
        send("s0", lambda *to: sum(map(abs, to)) == 1)
        inputs[2].wait()
        take("rsr", "f0")
        restrict(lv0, coefficient(lv0), "s")
        greeted("k2")
        greet("k3")
        y_pack("s1")
        z_pack("s1")
        restrict(lv1, coefficient(lv1), "s")
        y_pack("s2")
        z_pack("s2")
        greeted("k3")
        greet("k4")
        send("s0", lambda *to: sum(map(abs, to)) > 1)
        restrict(lv2, coefficient(lv2), "s")
        vector3 = local_vector()
        arrive("sg")
        sent("sg")
        y_unpack("sg")

        def keep_guess(i, v):
            R["sg"][i, 8 : 8 + lv0.rows, :] = v

        z_unpacked("sg", keep_guess)

        def first_residual(x, carry):
            a = start_of(lv0) + x
            c, v = beside_of(lv0, R["sg"], a)
            s = R["s0"][a, 8 : 8 + lv0.rows, :]
            f = R["f0"][a, 8 : 8 + lv0.rows, :] - ((6.0 + s) * c - v)
            R["f0"][a, 8 : 8 + lv0.rows, :] = jnp.where(R["own"][...] > 0.0, f, 0.0)
            return carry

        loop(B, first_residual, 0, lv0.unroll)
        greeted("k4")
        greet("k5")
        pack_send("f0")
        send("s1")
        send("s2")

        def weigh_at(lv):
            arrive(f"s{lv.k}")
            y_unpack(f"s{lv.k}")
            weigh(lv)

        weigh_at(lv0)
        arrive("f0")
        y_unpack("f0")
        begin(lv0)

        def first_relax(lv):
            k = lv.k
            count, a0 = span(lv, 4)

            def one(i, carry):
                a = a0 + i
                c, v = beside_of(lv, R[f"e{k}"], a)
                w = R[f"w{k}"][a, 8 : 8 + lv.rows, :]
                R[f"a{k}"][a, 8 : 8 + lv.rows, :] = c * (1.0 + KEEP) + w * v
                return carry

            loop(count, one, 0, lv.unroll)

        first_relax(lv0)
        restrict(lv0, left_of(lv0, "a"), "f")

        def deeper(lv, fill):
            name = f"f{lv.k}"
            pack_send(name)
            fill()
            weigh_at(lv)
            arrive(name)
            y_unpack(name)
            begin(lv)
            first_relax(lv)
            restrict(lv, left_of(lv, "a"), "f")

        greeted("k5")
        deeper(lv1, lambda: None)
        deeper(lv2, lambda: gather_start("gs", vector3))
        gather_start("gf", local_vector())

        gather_end("gs")
        by_device("gs", "s3")
        lane8, row8 = iota((8, 128), 1), iota((8, 128), 0)
        dev_y, dev_x, dev_z = lane8 & (ny - 1), (lane8 >> 2) & 1, lane8 >> 3
        step_x, step_z = ny, plane
        has = {
            ("y", 1): dev_y < ny - 1, ("y", -1): dev_y > 0, ("x", 1): dev_x < nx - 1, ("x", -1): dev_x > 0,
            ("z", 1): dev_z < nz - 1, ("z", -1): dev_z > 0,
        }
        strides = {"y": 1, "x": step_x, "z": step_z}

        def across(v, axis, way):
            return jnp.where(has[axis, way], roll(v, -way * strides[axis]), 0.0)

        def around(get, m):
            def one(x, y):
                c = get(x, y)
                r = n3 // m
                up = jnp.where(row8 >= n3 - r, roll(across(c, "z", 1), n3 - r, 0), roll(c, -r, 0))
                dn = jnp.where(row8 < r, roll(across(c, "z", -1), r - n3, 0), roll(c, r, 0))
                v = up + dn
                v = v + (get(x + 1, y) if x + 1 < m else across(get(0, y), "x", 1))
                v = v + (get(x - 1, y) if x else across(get(m - 1, y), "x", -1))
                v = v + (get(x, y + 1) if y + 1 < m else across(get(x, 0), "y", 1))
                v = v + (get(x, y - 1) if y else across(get(x, m - 1), "y", -1))
                return c, v

            return one

        cells = [(x, y) for x in range(n3) for y in range(n3)]
        m4 = n3 // 2
        cells4 = [(x, y) for x in range(m4) for y in range(m4)]
        live = row8 < n3

        def tile(name, x, y):
            g = (x * n3 + y) * (n3 if name in ("s3", "f3") else 8)
            return R[name][g : g + 8, :]

        for x, y in cells:
            R["w3"][8 * (x * n3 + y) : 8 * (x * n3 + y) + 8, :] = jnp.where(
                live, (DAMPING * q3) / (6.0 * q3 + tile("s3", x, y)), 0.0)

        def coarser(get):
            out = {}
            for x, y in cells4:
                v = (get(2 * x, 2 * y) + get(2 * x, 2 * y + 1)) + (get(2 * x + 1, 2 * y) + get(2 * x + 1, 2 * y + 1))
                v = v + jnp.where((row8 & 1) == 0, roll(v, -1, 0), roll(v, 1, 0))
                out[x, y] = jnp.where(live, 0.125 * v, 0.0)
            return out

        s4 = coarser(lambda x, y: tile("s3", x, y))
        gather_end("gf")
        by_device("gf", "f3")
        e = {}
        e0 = {}
        for c in cells:
            e0[c] = (tile("w3", *c) * (1.0 / q3)) * tile("f3", *c)
        op = around(lambda x, y: e0[x, y], n3)
        for c in cells:
            u, v = op(*c)
            e[c] = u * (1.0 + KEEP) + tile("w3", *c) * v
        op = around(lambda x, y: e[x, y], n3)
        rest = {}
        for c in cells:
            u, v = op(*c)
            rest[c] = jnp.where(live, tile("f3", *c) - ((6.0 * q3 + tile("s3", *c)) * u - q3 * v), 0.0)
        f4 = coarser(lambda x, y: rest[x, y])

        def inner(u, v):
            s = None
            for c in cells4:
                s = u[c] * v[c] if s is None else s + u[c] * v[c]
            return total(s)

        r4 = dict(f4)
        p4 = dict(f4)
        e4 = {c: jnp.zeros((8, 128), F32) for c in cells4}
        rr = inner(r4, r4)
        for _ in range(BOTTOM_ITERS):
            op = around(lambda x, y: p4[x, y], m4)
            q = {}
            for c in cells4:
                u, v = op(*c)
                q[c] = jnp.where(live, (6.0 * q4 + s4[c]) * u - q4 * v, 0.0)
            a = rr / inner(p4, q)
            e4 = {c: e4[c] + a * p4[c] for c in cells4}
            r4 = {c: r4[c] - a * q[c] for c in cells4}
            new = inner(r4, r4)
            ratio = new / rr
            p4 = {c: r4[c] + ratio * p4[c] for c in cells4}
            rr = new
        e = {(x, y): e[x, y] + e4[x // 2, y // 2] for x, y in cells}
        for _ in range(2):
            op = around(lambda x, y: e[x, y], n3)
            nxt = {}
            for c in cells:
                u, v = op(*c)
                nxt[c] = u * KEEP + (e0[c] + tile("w3", *c) * v)
            e = nxt
        for x, y in cells:
            g = x * n3 + y
            R["e3"][8 * g : 8 * g + 8, :] = e[x, y]
        R["e3"][groups * 8 :, :] = jnp.zeros((planes * 128 - groups * 8, 128), F32)
        for p in range(planes):
            R["x3"][p, 0:128, :] = R["e3"][128 * p : 128 * p + 128, :].T

        wide = planes * 128
        slabs3 = n3 + 2
        lane_w = iota((8, wide), 1) >> 3
        row_w = iota((8, wide), 0)
        lo_rows = jnp.where(row_w < 2, n3 - 2 + row_w, -1000)
        mid_rows = jnp.where(row_w < 2, -1000, row_w - 2)
        hi_rows = jnp.where(row_w < 2, row_w, -1000)
        y_below, y_above = jnp.maximum(gy - 1, 0), jnp.minimum(gy + 1, ny - 1)
        z_at = [jnp.maximum(gz - 1, 0), gz, jnp.minimum(gz + 1, nz - 1)]

        def vector(dev):
            return jnp.concatenate([R["x3"][p, pl.ds(dev, 1), :] for p in range(planes)], axis=1)

        for i in range(slabs3):
            partner = jnp.where(gx == 0, i >= n3, i < 2)
            px = jnp.where(partner, 1 - gx, gx)
            xx = jnp.where(gx == 0, i - jnp.where(i >= n3, n3, 0), i - 2 + jnp.where(i < 2, n3, 0))
            lo, mid, hi = (lane_w == xx * n3 + rows for rows in (lo_rows, mid_rows, hi_rows))
            for d in range(3):
                at_y = lambda g: vector(z_at[d] * plane + px * ny + g)
                first = jnp.where(mid, at_y(gy), jnp.where(lo, at_y(y_below), 0.0))
                second = jnp.where(hi, at_y(y_above), 0.0)
                R["lhs"][d, 16 * i : 16 * i + 8, :] = first
                R["lhs"][d, 16 * i + 8 : 16 * i + 16, :] = second
        l, c = iota((wide, 128), 1), iota((wide, 128), 0)
        table = jnp.where((l < B) & ((c & 7) == (l >> SPLIT)) & (c < groups * 8), 1.0, 0.0).astype(BF16)
        v = picked(R["lhs"][...].reshape(3 * slabs3 * 16, wide), table).reshape(3, slabs3, 16, 128)
        v = v[1] + roll(v[2].reshape(slabs3 * 16, 128), B).reshape(slabs3, 16, 128) + roll(
            v[0].reshape(slabs3 * 16, 128), -B).reshape(slabs3, 16, 128)
        u = R["u2"]
        shift = lv2.h - 4
        for i in range(slabs3):
            m = n3 + 4
            u[i, pl.ds(shift, m, stride=2), :] = v[i, 0:m]
            u[i, pl.ds(shift + 1, m, stride=2), :] = v[i, 0:m]

        add_up(lv2)
        relax(lv2, "b", "a", 4)
        relax(lv2, "a", "b", 2)

        def coarse_of(nxt, ref):
            a0 = 1 + gx * (nxt.h - 2)
            return lambda j, m: R[ref][a0 + j, nxt.first - 2 : nxt.first - 2 + m, :]

        prolong(lv1, coarse_of(lv2, "b2"))
        add_up(lv1)
        relax(lv1, "b", "a", 4)
        relax(lv1, "a", "b", 2)
        prolong(lv0, coarse_of(lv1, "b1"))
        add_up(lv0)
        relax(lv0, "b", "a", 4)
        relax(lv0, "a", "b", 2)

        def image(x, sums):
            upper, lower = sums
            a = start_of(lv0) + x
            c, v = beside_of(lv0, R["b0"], a)
            s = R["s0"][a, 8 : 8 + lv0.rows, :]
            ap = (6.0 + s) * c - v
            R["ap"][x] = ap
            c = jnp.where(R["own"][...] > 0.0, c, 0.0)
            return upper + R["f0"][a, 8 : 8 + lv0.rows, :] * c, lower + ap * c

        zero = jnp.zeros((lv0.rows, 128), F32)
        upper, lower = loop(B, image, (zero, zero), lv0.unroll)
        upper, lower = (jnp.sum(v, axis=0, keepdims=True) for v in (upper, lower))
        half = iota((1, 128), 1) < 64
        gather_start("gr", [jnp.where(half, upper, roll(lower, 64))])
        gather_end("gr")
        v = jnp.sum(R["gr"][0, 0:line], axis=0)
        half = iota((8, 128), 1) < 64
        sums = [total(jnp.where(half, v, 0.0)), total(jnp.where(half, 0.0, v))]
        step_length = sums[0] / sums[1]

        def finish(x, c):
            a = start_of(lv0) + x
            p = R["b0"][a, lv0.first : lv0.first + B, :]
            f = R["f0"][a, lv0.first : lv0.first + B, :]
            q = R["ap"][x, lv0.h : lv0.h + B, :]
            sol_ref[x] = R["sgr"][x] + (step_length * p)[:, 0:B]
            res_ref[x] = (f - step_length * q)[:, 0:B]
            return c

        loop(B, finish, 0, 24)
        for name in exchanges:
            if name != "sg":
                sent(name)
        for name in ("gs", "gf", "gr"):
            gather_sent(name)

    return kernel, list(scratch.values())


def solution(mesh):
    sizes = tuple(mesh.shape[a] for a in AXES)

    def body(right_side, start_guess, reaction):
        kernel, scratch = make_kernel(sizes, right_side.shape)
        out = jax.ShapeDtypeStruct(right_side.shape, F32)
        return tuple(
            pl.pallas_call(
                kernel,
                out_shape=(out, out),
                in_specs=[pl.BlockSpec(memory_space=pl.ANY)] * 3,
                out_specs=(pl.BlockSpec(memory_space=pltpu.VMEM),) * 2,
                scratch_shapes=scratch,
                compiler_params=pltpu.CompilerParams(
                    collective_id=0, has_side_effects=True, vmem_limit_bytes=51 * 2**20
                ),
                name="cg_step",
            )(right_side, start_guess, reaction)
        )

    placed = P(*AXES)
    return jax.shard_map(
        body, mesh=mesh, in_specs=(placed,) * 3, out_specs=(placed,) * 2, check_vma=False
    )
```
